64 devices in a mesh: dp: 4 (over x, y), cp: 16 (over z, core).
Axes of the slice: x: 2, y: 2, z: 8, core: 2. Of those that a mesh axis runs over, the one named last changes fastest.
The devices are a block of a 4x4x8 slice.
Arguments:
- x_act: bfloat16 [24576, 1536], P(('dp', 'cp')), parts along dimension 0
- seg_ids: int32 [24576], P(('dp', 'cp')), parts along dimension 0
- w_q: bfloat16 [1536, 12, 128], replicated
- w_k: bfloat16 [1536, 2, 128], replicated
- w_v: bfloat16 [1536, 2, 128], replicated
- w_o: bfloat16 [1536, 12, 128], replicated
- dy_act: bfloat16 [24576, 1536], P(('dp', 'cp')), parts along dimension 0
Outputs:
- output 1: bfloat16 [24576, 1536], P(('dp', 'cp')), parts along dimension 0
- output 2: bfloat16 [24576, 1536], P(('dp', 'cp')), parts along dimension 0
- output 3: float32 [6144, 12, 128], P(('dp', 'cp')), parts along dimension 0
- output 4: float32 [6144, 2, 128], P(('dp', 'cp')), parts along dimension 0
- output 5: float32 [6144, 2, 128], P(('dp', 'cp')), parts along dimension 0
- output 6: float32 [6144, 12, 128], P(('dp', 'cp')), parts along dimension 0
There are 4 independent parts. The reference program is written for one: setup_inputs(seed, part) draws one part's arguments, and reference() takes and returns one part's arrays. A program takes and returns all parts, laid end to end along the dimension named above; an argument that names none is the same for every part.
All inputs are finite; a program needn't handle non-finite values.
Results may differ from the reference program's by a relative error of at most 0.02.
Values are sent between devices in bfloat16 or wider.
A program may use at most 768 MiB of HBM per device.

```python
import jax
import jax.numpy as jnp
from jax import lax

CP_SIZE = 16
TOK_DEV = 384
MODEL_DIM = 1536
Q_HEADS = 12
KV_HEADS = 2
HEAD_DIM = 128

SEQ_LEN = CP_SIZE * TOK_DEV
GROUP_SIZE = Q_HEADS // KV_HEADS
Q_BLOCK = min(TOK_DEV, 128)
N_BLOCKS = SEQ_LEN // Q_BLOCK


def draw_segments(seg_key):
    key_zone, key_kind, key_short = jax.random.split(seg_key, 3)
    positions = jnp.arange(SEQ_LEN)
    zone_start = (jax.random.randint(key_zone, (SEQ_LEN,), 0, 2 * TOK_DEV) == 0) | (positions == 0)
    zone_index = jnp.cumsum(zone_start.astype(jnp.int32))
    parity = jax.random.randint(key_kind, (), 0, 2)
    short_zone = (zone_index + parity) % 2 == 0
    short_start = jax.random.randint(key_short, (SEQ_LEN,), 0, max(TOK_DEV // 8, 2)) == 0
    starts = zone_start | (short_zone & short_start)
    return (jnp.cumsum(starts.astype(jnp.int32)) - 1).astype(jnp.int32)


def setup_inputs(seed: int = 0, part: int = 0) -> dict:
    base_key = jax.random.key(seed)
    part_key = jax.random.fold_in(base_key, part)
    weight_key = jax.random.fold_in(base_key, 1000003)
    key_seg, key_x, key_dy = jax.random.split(part_key, 3)
    key_q, key_k, key_v, key_o = jax.random.split(weight_key, 4)
    in_scale = MODEL_DIM ** -0.5
    out_scale = (Q_HEADS * HEAD_DIM) ** -0.5
    q_shape = (MODEL_DIM, Q_HEADS, HEAD_DIM)
    kv_shape = (MODEL_DIM, KV_HEADS, HEAD_DIM)
    return {
        'x_act': jax.random.normal(key_x, (SEQ_LEN, MODEL_DIM), jnp.float32).astype(jnp.bfloat16),
        'seg_ids': draw_segments(key_seg),
        'w_q': (1.5 * in_scale * jax.random.normal(key_q, q_shape, jnp.float32)).astype(jnp.bfloat16),
        'w_k': (in_scale * jax.random.normal(key_k, kv_shape, jnp.float32)).astype(jnp.bfloat16),
        'w_v': (in_scale * jax.random.normal(key_v, kv_shape, jnp.float32)).astype(jnp.bfloat16),
        'w_o': (out_scale * jax.random.normal(key_o, q_shape, jnp.float32)).astype(jnp.bfloat16),
        'dy_act': jax.random.normal(key_dy, (SEQ_LEN, MODEL_DIM), jnp.float32).astype(jnp.bfloat16),
    }


def product32(einsum_form, left_arg, right_arg):
    return jnp.einsum(einsum_form, left_arg.astype(jnp.float32), right_arg.astype(jnp.float32))


def reference(x_act, seg_ids, w_q, w_k, w_v, w_o, dy_act):
    score_scale = HEAD_DIM ** -0.5
    w_q4 = w_q.reshape(MODEL_DIM, KV_HEADS, GROUP_SIZE, HEAD_DIM)
    w_o4 = w_o.reshape(MODEL_DIM, KV_HEADS, GROUP_SIZE, HEAD_DIM)
    q_all = product32('sm,mkgd->skgd', x_act, w_q4).astype(jnp.bfloat16)
    k_all = product32('sm,mkd->skd', x_act, w_k).astype(jnp.bfloat16)
    v_all = product32('sm,mkd->skd', x_act, w_v).astype(jnp.bfloat16)
    do_all = product32('qm,mkgd->qkgd', dy_act, w_o4).astype(jnp.bfloat16)
    k_wide = k_all.astype(jnp.float32)
    v_wide = v_all.astype(jnp.float32)
    key_pos = jnp.arange(SEQ_LEN)

    def block_step(carry_in, block_in):
        dk_acc, dv_acc = carry_in
        q_blk, do_blk, seg_blk, first_pos = block_in
        q_wide = q_blk.astype(jnp.float32)
        do_wide = do_blk.astype(jnp.float32)
        query_pos = first_pos + jnp.arange(Q_BLOCK)
        allowed = (seg_blk[:, None] == seg_ids[None, :]) & (key_pos[None, :] <= query_pos[:, None])
        scores = jnp.einsum('qkgd,skd->kqgs', q_wide, k_wide) * score_scale
        scores = jnp.where(allowed[None, :, None, :], scores, -jnp.inf)
        attn_prob = jax.nn.softmax(scores, axis=-1)
        prob_half = attn_prob.astype(jnp.bfloat16).astype(jnp.float32)
        out_blk = jnp.einsum('kqgs,skd->kqgd', prob_half, v_wide).astype(jnp.bfloat16)
        row_delta = jnp.einsum('qkgd,kqgd->kqg', do_wide, out_blk.astype(jnp.float32))
        dprobs = jnp.einsum('qkgd,skd->kqgs', do_wide, v_wide)
        dscores = (attn_prob * (dprobs - row_delta[..., None])).astype(jnp.bfloat16).astype(jnp.float32)
        dq_blk = (jnp.einsum('kqgs,skd->kqgd', dscores, k_wide) * score_scale).astype(jnp.bfloat16)
        dk_acc = dk_acc + jnp.einsum('kqgs,qkgd->skd', dscores, q_wide)
        dv_acc = dv_acc + jnp.einsum('kqgs,qkgd->skd', prob_half, do_wide)
        return (dk_acc, dv_acc), (out_blk, dq_blk)

    zeros_kv = jnp.zeros((SEQ_LEN, KV_HEADS, HEAD_DIM), jnp.float32)
    block_inputs = (
        q_all.reshape(N_BLOCKS, Q_BLOCK, KV_HEADS, GROUP_SIZE, HEAD_DIM),
        do_all.reshape(N_BLOCKS, Q_BLOCK, KV_HEADS, GROUP_SIZE, HEAD_DIM),
        seg_ids.reshape(N_BLOCKS, Q_BLOCK),
        jnp.arange(N_BLOCKS) * Q_BLOCK,
    )
    (dk_acc, dv_acc), (out_blocks, dq_blocks) = lax.scan(block_step, (zeros_kv, zeros_kv), block_inputs)
    grad_k = (dk_acc * score_scale).astype(jnp.bfloat16)
    grad_v = dv_acc.astype(jnp.bfloat16)
    x_blocks = x_act.reshape(N_BLOCKS, Q_BLOCK, MODEL_DIM)
    dy_blocks = dy_act.reshape(N_BLOCKS, Q_BLOCK, MODEL_DIM)
    y_out = product32('nkqgd,mkgd->nqm', out_blocks, w_o4).reshape(SEQ_LEN, MODEL_DIM).astype(jnp.bfloat16)
    dx_wide = (product32('nkqgd,mkgd->nqm', dq_blocks, w_q4).reshape(SEQ_LEN, MODEL_DIM)
               + product32('skd,mkd->sm', grad_k, w_k) + product32('skd,mkd->sm', grad_v, w_v))
    dx_out = dx_wide.astype(jnp.bfloat16)
    dw_q = product32('nqm,nkqgd->mkgd', x_blocks, dq_blocks).reshape(MODEL_DIM, Q_HEADS, HEAD_DIM)
    dw_k = product32('sm,skd->mkd', x_act, grad_k)
    dw_v = product32('sm,skd->mkd', x_act, grad_v)
    dw_o = product32('nqm,nkqgd->mkgd', dy_blocks, out_blocks).reshape(MODEL_DIM, Q_HEADS, HEAD_DIM)
    return (y_out, dx_out, dw_q, dw_k, dw_v, dw_o)
```

```python
import functools

import jax
import jax.numpy as jnp
from jax import lax
from jax.experimental import pallas as pl
from jax.experimental.pallas import tpu as pltpu
from jax.sharding import PartitionSpec as P

QT = 128
LOG2E = 1.4426950408889634
NEG_INF = float('-inf')
NT = (((1,), (1,)), ((), ()))
TN = (((0,), (0,)), ((), ()))
NN = (((1,), (0,)), ((), ()))


def dot32(left_arg, right_arg, dims):
    return lax.dot_general(left_arg, right_arg, dims, preferred_element_type=jnp.float32)


def stack_heads(ref, tile, head, group):
    rows = pl.ds(tile * QT, QT)
    return jnp.concatenate(
        [ref[rows, (head * group + member) * 128:(head * group + member + 1) * 128] for member in range(group)], axis=0)


def attention_kernel(kv_heads, group, scale, scal_ref, local_start_ref, seg_all_ref, q_ref, do_ref, kv_ref,
                     o_ref, dq_ref, dkv_ref, start_s, max_s, sum_s, delta_s, acc_s):
    tok = q_ref.shape[0]
    blocks = kv_ref.shape[0]
    tiles = tok // QT
    width = group * QT
    scale2 = scale * LOG2E
    me, first_seg, head_count = scal_ref[0], scal_ref[1], scal_ref[2]

    shard_index = lax.broadcasted_iota(jnp.int32, seg_all_ref.shape, 0)
    earlier = (shard_index < me) & (seg_all_ref[...] < first_seg)
    doc_start = jnp.sum(earlier.astype(jnp.int32))
    first = doc_start // tok
    has_prev = doc_start < me * tok
    tiles_prev = jnp.where(has_prev, (head_count + QT - 1) // QT, 0)
    full_tiles = head_count // QT
    local_start = local_start_ref[...]
    start_s[...] = jnp.where(local_start == 0, doc_start - me * tok, local_start)

    def k_cols(head):
        return slice(head * 128, (head + 1) * 128)

    def v_cols(head):
        return slice((kv_heads + head) * 128, (kv_heads + head + 1) * 128)

    def diag_mask(tile, keys):
        key_pos = lax.broadcasted_iota(jnp.int32, (keys, width), 0)
        query_pos = lax.rem(lax.broadcasted_iota(jnp.int32, (1, width), 1), QT) + tile * QT
        return (key_pos <= query_pos) & (key_pos >= start_s[tile:tile + 1, :])

    def off_mask(tile, blk):
        key_pos = lax.broadcasted_iota(jnp.int32, (tok, width), 0)
        return key_pos >= start_s[tile:tile + 1, :] + (me - blk) * tok

    def off_loops(body):
        for tile in range(tiles):
            @pl.when(tile < tiles_prev)
            def _():
                mask_end = jnp.where(tile < full_tiles, first + 1, me)
                lax.fori_loop(first, mask_end, functools.partial(body, tile, True), 0)
                lax.fori_loop(mask_end, me, functools.partial(body, tile, False), 0)

    def clear_body(blk, carry):
        dkv_ref[blk] = jnp.zeros(dkv_ref.shape[1:], jnp.float32)
        return carry

    lax.fori_loop(0, first, clear_body, 0)
    lax.fori_loop(me + 1, blocks, clear_body, 0)

    for tile in range(tiles):
        keys = QT * (tile + 1)
        allowed = diag_mask(tile, keys)
        for head in range(kv_heads):
            slot = head * tiles + tile
            q_tile = stack_heads(q_ref, tile, head, group)
            k_blk = kv_ref[me, 0:keys, k_cols(head)]
            v_blk = kv_ref[me, 0:keys, v_cols(head)]
            scores = jnp.where(allowed, dot32(k_blk, q_tile, NT) * scale2, NEG_INF)
            new_max = jnp.max(scores, axis=0, keepdims=True)
            weights = jnp.exp2(scores - new_max)
            max_s[slot:slot + 1, :] = new_max
            sum_s[slot:slot + 1, :] = jnp.sum(weights, axis=0, keepdims=True)
            acc_s[slot] = dot32(v_blk, weights.astype(jnp.bfloat16), TN)

    def forward_body(tile, masked, blk, carry):
        for head in range(kv_heads):
            slot = head * tiles + tile
            q_tile = stack_heads(q_ref, tile, head, group)
            k_blk = kv_ref[blk, :, k_cols(head)]
            v_blk = kv_ref[blk, :, v_cols(head)]
            scores = dot32(k_blk, q_tile, NT) * scale2
            if masked:
                scores = jnp.where(off_mask(tile, blk), scores, NEG_INF)
            old_max = max_s[slot:slot + 1, :]
            new_max = jnp.maximum(old_max, jnp.max(scores, axis=0, keepdims=True))
            weights = jnp.exp2(scores - new_max)
            factor = jnp.exp2(old_max - new_max)
            max_s[slot:slot + 1, :] = new_max
            sum_s[slot:slot + 1, :] = sum_s[slot:slot + 1, :] * factor + jnp.sum(weights, axis=0, keepdims=True)
            acc_s[slot] = acc_s[slot] * factor + dot32(v_blk, weights.astype(jnp.bfloat16), TN)
        return carry

    off_loops(forward_body)

    for tile in range(tiles):
        for head in range(kv_heads):
            slot = head * tiles + tile
            total = sum_s[slot:slot + 1, :]
            max_s[slot:slot + 1, :] = max_s[slot:slot + 1, :] + jnp.log2(total)
            out_t = (acc_s[slot] / total).astype(jnp.bfloat16)
            do_t = stack_heads(do_ref, tile, head, group).astype(jnp.float32).T
            delta_s[slot:slot + 1, :] = jnp.sum(do_t * out_t.astype(jnp.float32), axis=0, keepdims=True)
            for member in range(group):
                col = (head * group + member) * 128
                o_ref[tile * QT:(tile + 1) * QT, col:col + 128] = out_t[:, member * QT:(member + 1) * QT].T

    def grads(tile, head, blk, keys, mask):
        slot = head * tiles + tile
        q_tile = stack_heads(q_ref, tile, head, group)
        do_tile = stack_heads(do_ref, tile, head, group)
        k_blk = kv_ref[blk, 0:keys, k_cols(head)]
        v_blk = kv_ref[blk, 0:keys, v_cols(head)]
        scores = dot32(k_blk, q_tile, NT) * scale2
        if mask is not None:
            scores = jnp.where(mask, scores, NEG_INF)
        prob = jnp.exp2(scores - max_s[slot:slot + 1, :])
        dprob = dot32(v_blk, do_tile, NT)
        dscore = (prob * (dprob - delta_s[slot:slot + 1, :])).astype(jnp.bfloat16)
        dv_part = dot32(prob.astype(jnp.bfloat16), do_tile, NN)
        dk_part = dot32(dscore, q_tile, NN)
        dq_part = dot32(k_blk, dscore, TN)
        return dq_part, dk_part, dv_part

    for tile in reversed(range(tiles)):
        keys = QT * (tile + 1)
        allowed = diag_mask(tile, keys)
        for head in range(kv_heads):
            dq_part, dk_part, dv_part = grads(tile, head, me, keys, allowed)
            acc_s[head * tiles + tile] = dq_part
            if tile == tiles - 1:
                dkv_ref[me, 0:keys, k_cols(head)] = dk_part
                dkv_ref[me, 0:keys, v_cols(head)] = dv_part
            else:
                dkv_ref[me, 0:keys, k_cols(head)] = dkv_ref[me, 0:keys, k_cols(head)] + dk_part
                dkv_ref[me, 0:keys, v_cols(head)] = dkv_ref[me, 0:keys, v_cols(head)] + dv_part

    def backward_body(tile, masked, blk, carry):
        mask = off_mask(tile, blk) if masked else None
        for head in range(kv_heads):
            slot = head * tiles + tile
            dq_part, dk_part, dv_part = grads(tile, head, blk, tok, mask)
            acc_s[slot] = acc_s[slot] + dq_part
            if tile == 0:
                dkv_ref[blk, :, k_cols(head)] = dk_part
                dkv_ref[blk, :, v_cols(head)] = dv_part
            else:
                dkv_ref[blk, :, k_cols(head)] = dkv_ref[blk, :, k_cols(head)] + dk_part
                dkv_ref[blk, :, v_cols(head)] = dkv_ref[blk, :, v_cols(head)] + dv_part
        return carry

    off_loops(backward_body)

    for tile in range(tiles):
        for head in range(kv_heads):
            grad_t = (acc_s[head * tiles + tile] * scale).astype(jnp.bfloat16)
            for member in range(group):
                col = (head * group + member) * 128
                dq_ref[tile * QT:(tile + 1) * QT, col:col + 128] = grad_t[:, member * QT:(member + 1) * QT].T


def places(n):
    me = lax.axis_index('cp')
    chips = n // 2
    core = lax.rem(me, 2)
    chip = me // 2

    def at(offset, which):
        return lax.rem(chip + offset + chips, chips) * 2 + which

    return me, chips, core, chip, at


def remote(src, dst, send_sem, recv_sem, target):
    return pltpu.make_async_remote_copy(src_ref=src, dst_ref=dst, send_sem=send_sem, recv_sem=recv_sem,
                                        device_id={'cp': target}, device_id_type=pl.DeviceIdType.MESH)


def greet(targets):
    barrier = pltpu.get_barrier_semaphore()
    for target in targets:
        pl.semaphore_signal(barrier, inc=1, device_id={'cp': target}, device_id_type=pl.DeviceIdType.MESH)
    pl.semaphore_wait(barrier, len(targets))


def gather_kernel(n, kv_ref, seg_ref, x_ref, dy_ref, wq_ref, wo_ref,
                  kv_all_ref, seg_all_ref, q_ref, do_ref, xt_ref, dyt_ref, xtp_ref, dytp_ref,
                  wq_s, wo_s, load_sem, seg_send, seg_recv, ring_send, ring_recv, pair_send, pair_recv,
                  mate_send, mate_recv):
    me, chips, core, chip, at = places(n)
    mate = at(0, 1 - core)
    half = kv_ref.shape[0] // 2
    reach = chips // 2
    load_q = pltpu.make_async_copy(wq_ref, wq_s, load_sem.at[0])
    load_o = pltpu.make_async_copy(wo_ref, wo_s, load_sem.at[1])
    load_q.start()
    load_o.start()
    greet([lax.rem(me + step, n) for step in range(1, n)])

    def rows(sub):
        return pl.ds(sub * half, half)

    def ring_copy(way, sub, hop):
        offset = -(hop - 1) if way == 0 else hop - 1
        owner = at(offset, core)
        src = kv_ref.at[rows(sub)] if hop == 1 else kv_all_ref.at[owner, rows(sub)]
        return remote(src, kv_all_ref.at[owner, rows(sub)], ring_send.at[way, sub, hop - 1], ring_recv.at[way, sub, hop - 1],
                      at(1 if way == 0 else -1, core))

    def pair_copy(way, sub, hop):
        owner = at(-hop if way == 0 else hop, core)
        return remote(kv_all_ref.at[owner, rows(sub)], kv_all_ref.at[owner, rows(sub)],
                      pair_send.at[way, sub, hop - 1], pair_recv.at[way, sub, hop - 1], mate)

    def seg_copy(step):
        return remote(seg_ref, seg_all_ref.at[me], seg_send.at[step - 1], seg_recv.at[step - 1], lax.rem(me + step, n))

    hops = [(way, sub, hop) for hop in range(1, reach + 1) for sub in range(2) for way in range(2)
            if hop < reach or way == sub]
    started = []
    for way, sub, hop in hops:
        if hop == 1:
            started.append(ring_copy(way, sub, hop))
            started[-1].start()
    for step in range(1, n):
        started.append(seg_copy(step))
        started[-1].start()
    started.append(remote(kv_ref, kv_all_ref.at[me], mate_send.at[0], mate_recv.at[0], mate))
    started[-1].start()
    kv_all_ref[me] = kv_ref[...]
    seg_all_ref[me] = seg_ref[...]

    heads = wq_s.shape[0]
    strip = x_ref.shape[1] * 2 // heads

    def project(src_ref, w_s, dst_ref, pair):
        w_pair = jnp.concatenate([w_s[2 * pair], w_s[2 * pair + 1]], axis=1)
        dst_ref[:, pair * 256:(pair + 1) * 256] = dot32(src_ref[...], w_pair, NN).astype(jnp.bfloat16)

    def flip(src_ref, dst_ref, part):
        dst_ref[part * strip:(part + 1) * strip, :] = src_ref[:, part * strip:(part + 1) * strip].T

    work = []
    for part in range(heads // 2):
        work.append(functools.partial(flip, x_ref, xt_ref, part))
        work.append(functools.partial(flip, dy_ref, dyt_ref, part))
    for pair in range(heads // 2):
        work.append(functools.partial(project, x_ref, wq_s, q_ref, pair))
        work.append(functools.partial(project, dy_ref, wo_s, do_ref, pair))
    load_q.wait()
    load_o.wait()
    quota = -(-len(work) // len(hops))
    for index, (way, sub, hop) in enumerate(hops):
        for item in work[index * quota:(index + 1) * quota]:
            item()
        ring_copy(way, sub, hop).wait_recv()
        started.append(pair_copy(way, sub, hop))
        started[-1].start()
        if (way, sub, hop + 1) in hops:
            started.append(ring_copy(way, sub, hop + 1))
            started[-1].start()
    for index, (src, dst) in enumerate(((xt_ref, xtp_ref), (dyt_ref, dytp_ref))):
        started.append(remote(src, dst, mate_send.at[index + 1], mate_recv.at[index + 1], mate))
        started[-1].start()
    for way, sub, hop in hops:
        pair_copy(way, sub, hop).wait_recv()
    for step in range(1, n):
        seg_copy(step).wait_recv()
    remote(kv_ref, kv_all_ref.at[me], mate_send.at[0], mate_recv.at[0], mate).wait_recv()
    remote(xt_ref, xtp_ref, mate_send.at[1], mate_recv.at[1], mate).wait_recv()
    remote(dyt_ref, dytp_ref, mate_send.at[2], mate_recv.at[2], mate).wait_recv()
    for copy in started:
        copy.wait_send()


def reduce_kernel(n, scale, kv_width, dkv_ref, o_ref, dq_ref, xt_ref, dyt_ref, xtp_ref, dytp_ref, wkv_ref, wq_ref, wo_ref,
                  y_ref, dx_ref, dwo_ref, dwq_ref, dwkv_ref,
                  own_s, mate_s, slot1_s, stage1_s, total_s, grad_s, grad_mate_s, o_mate_s, dq_mate_s, slot2_s, stage2_s,
                  wq_s, wo_s, load_sem, block_sem, mate_send, mate_recv, ring_send, ring_recv, extra_send, extra_recv):
    me, chips, core, chip, at = places(n)
    mate = at(0, 1 - core)
    ring = (at(1, core), at(-1, core))
    tok = o_ref.shape[0]
    quarter = tok // 4
    heads, out_rows, head_dim = dwo_ref.shape
    load_q = pltpu.make_async_copy(wq_ref, wq_s, load_sem.at[0])
    load_o = pltpu.make_async_copy(wo_ref, wo_s, load_sem.at[1])
    order = []
    for step in range(1, chips):
        for offset in (-step, step):
            if offset % chips not in order:
                order.append(offset % chips)
    order.append(0)
    own_loads = [pltpu.make_async_copy(dkv_ref.at[at(offset, core)], own_s.at[index], block_sem.at[index])
                 for index, offset in enumerate(order)]
    for load in own_loads:
        load.start()
    load_o.start()
    load_q.start()
    greet([ring[0], ring[1], mate])
    mate_copies = [remote(dkv_ref.at[at(offset, 1 - core)], mate_s.at[index], mate_send.at[index], mate_recv.at[index], mate)
                   for index, offset in enumerate(order)]
    extras = [remote(o_ref, o_mate_s, extra_send.at[0], extra_recv.at[0], mate),
              remote(dq_ref, dq_mate_s, extra_send.at[1], extra_recv.at[1], mate),
              remote(grad_s, grad_mate_s, extra_send.at[2], extra_recv.at[2], mate)]
    for index, copy in enumerate(mate_copies):
        copy.start()
        if index == 3:
            extras[0].start()
            extras[1].start()

    ready = set()

    def need(position):
        if position not in ready:
            ready.add(position)
            own_loads[position].wait()
            mate_copies[position].wait_recv()

    def ring_copy(job, way, sub, step):
        slots, stage = (slot1_s, stage1_s) if job == 0 else (slot2_s, stage2_s)
        src = stage.at[way, sub] if step == 0 else slots.at[way, sub, step - 1]
        return remote(src, slots.at[way, sub, step], ring_send.at[job, way, sub, step], ring_recv.at[job, way, sub, step],
                      ring[way])

    started = []

    def send(job, way, sub, step):
        started.append(ring_copy(job, way, sub, step))
        started[-1].start()

    def contrib1(way, sub, step):
        offset = (-(1 + step) if way == 0 else 1 + step) % chips
        position = order.index(offset)
        need(position)
        span = slice((2 * way + sub) * quarter, (2 * way + sub + 1) * quarter)
        return own_s[position, span, :] + mate_s[position, span, :]

    cut = 7 * head_dim

    def contrib2(way, sub, step):
        offset = -(1 + step) if way == 0 else 1 + step
        first_row = pl.multiple_of(at(offset % chips, core) * out_rows, 32)
        take = pl.ds(first_row, out_rows)
        lhs, lhs_mate = (dyt_ref, dytp_ref) if way == 0 else (xt_ref, xtp_ref)
        rhs, rhs_mate = (o_ref, o_mate_s) if way == 0 else (dq_ref, dq_mate_s)
        if sub == 0:
            return (dot32(lhs[take, :], rhs[:, 0:cut], NN) + dot32(lhs_mate[take, :], rhs_mate[:, 0:cut], NN))
        main = dot32(lhs[take, :], rhs[:, cut:], NN) + dot32(lhs_mate[take, :], rhs_mate[:, cut:], NN)
        cols = slice(way * kv_width, (way + 1) * kv_width)
        side = dot32(xt_ref[take, :], grad_s[:, cols], NN) + dot32(xtp_ref[take, :], grad_mate_s[:, cols], NN)
        return jnp.concatenate([main, side], axis=1)

    strip = 256
    strips = y_ref.shape[1] // strip

    def rows_out(part):
        return slice(part * strip, (part + 1) * strip)

    def times_weight(src_ref, w_s, part):
        total = None
        for pair in range(heads // 2):
            w_pair = jnp.concatenate([w_s[2 * pair, rows_out(part), :], w_s[2 * pair + 1, rows_out(part), :]], axis=1)
            piece = dot32(src_ref[:, pair * 256:(pair + 1) * 256], w_pair, NT)
            total = piece if total is None else total + piece
        return total

    steps = chips - 1
    both = [(sub, way) for sub in range(2) for way in range(2)]
    for sub, way in both:
        stage1_s[way, sub] = contrib1(way, sub, 0)
        send(0, way, sub, 0)
    load_o.wait()
    load_q.wait()
    extras[0].wait_recv()
    extras[1].wait_recv()
    for step in range(steps):
        if step < strips:
            y_ref[:, rows_out(step)] = times_weight(o_ref, wo_s, step).astype(jnp.bfloat16)
        if step == steps - 1:
            for way in range(2):
                stage2_s[way, 0] = contrib2(way, 0, 0)
                send(1, way, 0, 0)
        for sub, way in both:
            part = contrib1(way, sub, step + 1)
            ring_copy(0, way, sub, step).wait_recv()
            if step < steps - 1:
                slot1_s[way, sub, step] = slot1_s[way, sub, step] + part
                send(0, way, sub, step + 1)
            else:
                span = slice((2 * way + sub) * quarter, (2 * way + sub + 1) * quarter)
                total = slot1_s[way, sub, step] + part
                grad_s[span, 0:kv_width] = (total[:, 0:kv_width] * scale).astype(jnp.bfloat16)
                grad_s[span, kv_width:] = total[:, kv_width:].astype(jnp.bfloat16)
    extras[2].start()
    extras[2].wait_recv()
    for way in range(2):
        stage2_s[way, 1] = contrib2(way, 1, 0)
        send(1, way, 1, 0)
    for step in range(steps):
        if step < strips:
            wide = times_weight(dq_ref, wq_s, step) + dot32(grad_s[...], wkv_ref[rows_out(step), :], NT)
            dx_ref[:, rows_out(step)] = wide.astype(jnp.bfloat16)
        for sub, way in both:
            part = contrib2(way, sub, step + 1)
            ring_copy(1, way, sub, step).wait_recv()
            if step < steps - 1:
                slot2_s[way, sub, step] = slot2_s[way, sub, step] + part
                send(1, way, sub, step + 1)
            else:
                total = slot2_s[way, sub, step] + part
                out_ref = dwo_ref if way == 0 else dwq_ref
                base = 0 if sub == 0 else cut // head_dim
                for index in range(cut // head_dim if sub == 0 else heads - cut // head_dim):
                    out_ref[base + index] = total[:, index * head_dim:(index + 1) * head_dim]
                if sub == 1:
                    dwkv_ref[:, way * kv_width:(way + 1) * kv_width] = total[:, heads * head_dim - cut:]
    for copy in started + mate_copies + extras:
        copy.wait_send()


SMEM_SPEC = pl.BlockSpec(memory_space=pltpu.SMEM)
VMEM_SPEC = pl.BlockSpec(memory_space=pltpu.VMEM)
ANY_SPEC = pl.BlockSpec(memory_space=pl.ANY)
VMEM_LIMIT = 60 * 1024 * 1024
REDUCE_LIMIT = 67043328


def solution(mesh):
    group_count = mesh.shape['cp']
    row_spec = P(('dp', 'cp'), None)
    tok_spec = P(('dp', 'cp'))
    weight_spec = P(None, None, None)
    grad_spec = P(('dp', 'cp'), None, None)

    def local_step(x_act, seg_ids, w_q, w_k, w_v, w_o, dy_act):
        tok = x_act.shape[0]
        model_dim, q_heads, head_dim = w_q.shape
        kv_heads = w_k.shape[1]
        group = q_heads // kv_heads
        q_width = q_heads * head_dim
        kv_width = kv_heads * head_dim
        tiles = tok // QT
        scale = head_dim ** -0.5
        me = lax.axis_index('cp')
        bf16 = jnp.bfloat16

        w_kv = jnp.concatenate([w_k.reshape(model_dim, kv_width), w_v.reshape(model_dim, kv_width)], axis=1)
        kv_loc = jnp.dot(x_act, w_kv, preferred_element_type=jnp.float32).astype(bf16)
        local_start = jnp.sum((seg_ids[None, :] < seg_ids[:, None]).astype(jnp.int32), axis=1)
        scalars = jnp.stack([me, seg_ids[0], jnp.sum((seg_ids == seg_ids[0]).astype(jnp.int32))]).astype(jnp.int32)
        local_rows = jnp.tile(local_start.reshape(tiles, 1, QT), (1, group, 1)).reshape(tiles, group * QT)
        wq_heads = w_q.transpose(1, 0, 2)
        wo_heads = w_o.transpose(1, 0, 2)

        slots = kv_heads * tiles
        width = group * QT
        chips = group_count // 2
        reach = chips // 2
        dma = pltpu.SemaphoreType.DMA
        f32 = jnp.float32
        shape = jax.ShapeDtypeStruct
        flat = shape((tok, q_width), bf16)
        flipped = shape((model_dim, tok), bf16)
        kv_all, seg_all, q_loc, do_loc, xt, dyt, xtp, dytp = pl.pallas_call(
            functools.partial(gather_kernel, group_count),
            out_shape=(shape((group_count, tok, 2 * kv_width), bf16), shape((group_count, tok // 128, 128), jnp.int32),
                       flat, flat, flipped, flipped, flipped, flipped),
            in_specs=[VMEM_SPEC] * 4 + [ANY_SPEC] * 2,
            out_specs=(VMEM_SPEC,) * 8,
            scratch_shapes=[pltpu.VMEM((q_heads, model_dim, head_dim), bf16), pltpu.VMEM((q_heads, model_dim, head_dim), bf16),
                            dma((2,)), dma((group_count - 1,)), dma((group_count - 1,)),
                            dma((2, 2, reach)), dma((2, 2, reach)), dma((2, 2, reach)), dma((2, 2, reach)), dma((3,)), dma((3,))],
            compiler_params=pltpu.CompilerParams(collective_id=0, has_side_effects=True, vmem_limit_bytes=VMEM_LIMIT),
            cost_estimate=pl.CostEstimate(flops=8 * tok * model_dim * q_width, bytes_accessed=2**24, transcendentals=0),
            name='gather_keys',
        )(kv_loc, seg_ids.reshape(tok // 128, 128), x_act, dy_act, wq_heads, wo_heads)

        o_loc, dq_loc, dkv_all = pl.pallas_call(
            functools.partial(attention_kernel, kv_heads, group, scale),
            out_shape=(flat, flat, shape((group_count, tok, 2 * kv_width), f32)),
            in_specs=[SMEM_SPEC] + [VMEM_SPEC] * 5,
            out_specs=(VMEM_SPEC,) * 3,
            scratch_shapes=[pltpu.VMEM((tiles, width), jnp.int32), pltpu.VMEM((slots, width), f32), pltpu.VMEM((slots, width), f32),
                            pltpu.VMEM((slots, width), f32), pltpu.VMEM((slots, head_dim, width), f32)],
            compiler_params=pltpu.CompilerParams(vmem_limit_bytes=VMEM_LIMIT),
            cost_estimate=pl.CostEstimate(flops=16 * 14 * tok * tok * q_width, bytes_accessed=2**25, transcendentals=0),
            name='attend',
        )(scalars, local_rows, seg_all, q_loc, do_loc, kv_all)

        out_rows = model_dim // group_count
        blk = (tok, 2 * kv_width)
        cols2 = (q_width + kv_width) // 2
        steps = chips - 1
        head_grad = shape((q_heads, out_rows, head_dim), f32)
        y_out, dx_out, dwo, dwq, dwkv = pl.pallas_call(
            functools.partial(reduce_kernel, group_count, scale, kv_width),
            out_shape=(shape((tok, model_dim), bf16), shape((tok, model_dim), bf16), head_grad, head_grad,
                       shape((out_rows, 2 * kv_width), f32)),
            in_specs=[ANY_SPEC] + [VMEM_SPEC] * 7 + [ANY_SPEC] * 2,
            out_specs=(VMEM_SPEC,) * 5,
            scratch_shapes=[pltpu.VMEM((chips,) + blk, f32), pltpu.VMEM((chips,) + blk, f32),
                            pltpu.VMEM((2, 2, steps, tok // 4, 2 * kv_width), f32), pltpu.VMEM((2, 2, tok // 4, 2 * kv_width), f32),
                            pltpu.VMEM((8, 128), f32), pltpu.VMEM(blk, bf16), pltpu.VMEM(blk, bf16),
                            pltpu.VMEM((tok, q_width), bf16), pltpu.VMEM((tok, q_width), bf16),
                            pltpu.VMEM((2, 2, steps, out_rows, cols2), f32), pltpu.VMEM((2, 2, out_rows, cols2), f32),
                            pltpu.VMEM((q_heads, model_dim, head_dim), bf16), pltpu.VMEM((q_heads, model_dim, head_dim), bf16),
                            dma((2,)), dma((chips,)), dma((chips,)), dma((chips,)),
                            dma((2, 2, 2, steps)), dma((2, 2, 2, steps)), dma((3,)), dma((3,))],
            compiler_params=pltpu.CompilerParams(collective_id=1, has_side_effects=True, vmem_limit_bytes=REDUCE_LIMIT),
            cost_estimate=pl.CostEstimate(flops=16 * tok * model_dim * q_width, bytes_accessed=2**25, transcendentals=0),
            name='reduce_grads',
        )(dkv_all, o_loc, dq_loc, xt, dyt, xtp, dytp, w_kv, wq_heads, wo_heads)
        dwk = dwkv[:, :kv_width].reshape(out_rows, kv_heads, head_dim)
        dwv = dwkv[:, kv_width:].reshape(out_rows, kv_heads, head_dim)
        return y_out, dx_out, dwq.transpose(1, 0, 2), dwk, dwv, dwo.transpose(1, 0, 2)

    return jax.shard_map(local_step, mesh=mesh,
                         in_specs=(row_spec, tok_spec, weight_spec, weight_spec, weight_spec, weight_spec, row_spec),
                         out_specs=(row_spec, row_spec, grad_spec, grad_spec, grad_spec, grad_spec),
                         check_vma=False)
```

```python
import functools

import jax
import jax.numpy as jnp
from jax import lax
from jax.experimental import pallas as pl
from jax.experimental.pallas import tpu as pltpu
from jax.sharding import PartitionSpec as P

QT = 128
LOG2E = 1.4426950408889634
NEG_INF = float('-inf')
NT = (((1,), (1,)), ((), ()))
TN = (((0,), (0,)), ((), ()))
NN = (((1,), (0,)), ((), ()))


def dot32(left_arg, right_arg, dims):
    return lax.dot_general(left_arg, right_arg, dims, preferred_element_type=jnp.float32)


def stack_heads(ref, tile, head, group):
    rows = pl.ds(pl.multiple_of(tile * QT, QT), QT)
    return jnp.concatenate(
        [ref[rows, (head * group + member) * 128:(head * group + member + 1) * 128] for member in range(group)], axis=0)


def attention_kernel(kv_heads, group, scale, seg_ref, seg_all_ref, q_ref, do_ref, dot_ref, kv_ref,
                     o_ref, dq_ref, dkv_ref, start_s, max_s, sum_s, delta_s, acc_s, grad_s, zero_s, out_sem):
    tok = q_ref.shape[0]
    blocks = kv_ref.shape[0]
    tiles = tok // QT
    width = group * QT
    scale2 = scale * LOG2E
    me = lax.axis_index('cp')
    zero_s[...] = jnp.zeros(zero_s.shape, jnp.float32)

    seg_own = seg_ref[...]
    first_seg = jnp.min(seg_own)
    head_count = jnp.sum((seg_own == first_seg).astype(jnp.int32))
    shard_index = lax.broadcasted_iota(jnp.int32, seg_all_ref.shape, 0)
    earlier = (shard_index < me) & (seg_all_ref[...] < first_seg)
    doc_start = jnp.sum(earlier.astype(jnp.int32))
    first = doc_start // tok
    has_prev = doc_start < me * tok
    tiles_prev = jnp.where(has_prev, (head_count + QT - 1) // QT, 0)
    full_tiles = head_count // QT

    def zero_copy(blk):
        return pltpu.make_async_copy(zero_s, dkv_ref.at[blk], out_sem.at[blk])

    def grad_copy(blk):
        return pltpu.make_async_copy(grad_s.at[blk], dkv_ref.at[blk], out_sem.at[blk])

    def clear_body(blk, carry):
        zero_copy(blk).start()
        return carry

    seg_wide = seg_own.astype(jnp.float32)
    columns = [jnp.broadcast_to(seg_wide[part:part + 1, :], (128, 128)).T for part in range(tok // 128)]
    for tile in range(tiles):
        count = sum(jnp.sum((column < seg_wide[tile:tile + 1, :]).astype(jnp.int32), axis=0, keepdims=True)
                    for column in columns)
        row = jnp.where(count == 0, doc_start - me * tok, count)
        start_s[tile] = jnp.concatenate([row] * group, axis=1)

    lax.fori_loop(0, first, clear_body, 0)
    lax.fori_loop(me + 1, blocks, clear_body, 0)

    def k_cols(head):
        return slice(head * 128, (head + 1) * 128)

    def v_cols(head):
        return slice((kv_heads + head) * 128, (kv_heads + head + 1) * 128)

    def diag_mask(tile, keys):
        key_pos = lax.broadcasted_iota(jnp.int32, (keys, width), 0)
        query_pos = lax.rem(lax.broadcasted_iota(jnp.int32, (1, width), 1), QT) + tile * QT
        return (key_pos <= query_pos) & (key_pos >= start_s[tile])

    def off_mask(tile, blk):
        key_pos = lax.broadcasted_iota(jnp.int32, (tok, width), 0)
        return key_pos >= start_s[tile] + (me - blk) * tok

    def over_tiles(body, blk):
        def tile_body(tile, carry):
            masked = (blk == first) | (tile >= full_tiles)
            pl.when(masked)(functools.partial(body, tile, True, blk))
            pl.when(jnp.logical_not(masked))(functools.partial(body, tile, False, blk))
            return carry
        lax.fori_loop(0, tiles_prev, tile_body, 0)

    for tile in range(tiles):
        keys = QT * (tile + 1)
        for head in range(kv_heads):
            slot = head * tiles + tile
            q_tile = stack_heads(q_ref, tile, head, group)
            k_blk = kv_ref[me, 0:keys, k_cols(head)]
            v_blk = kv_ref[me, 0:keys, v_cols(head)]
            scores = jnp.where(diag_mask(tile, keys), dot32(k_blk, q_tile, NT) * scale2, NEG_INF)
            new_max = jnp.max(scores, axis=0, keepdims=True)
            weights = jnp.exp2(scores - new_max)
            max_s[slot] = new_max
            sum_s[slot] = jnp.sum(weights, axis=0, keepdims=True)
            acc_s[slot] = dot32(v_blk, weights.astype(jnp.bfloat16), TN)

    def forward_body(tile, masked, blk):
        for head in range(kv_heads):
            slot = head * tiles + tile
            q_tile = stack_heads(q_ref, tile, head, group)
            k_blk = kv_ref[blk, :, k_cols(head)]
            v_blk = kv_ref[blk, :, v_cols(head)]
            scores = dot32(k_blk, q_tile, NT) * scale2
            if masked:
                scores = jnp.where(off_mask(tile, blk), scores, NEG_INF)
            old_max = max_s[slot]
            new_max = jnp.maximum(old_max, jnp.max(scores, axis=0, keepdims=True))
            weights = jnp.exp2(scores - new_max)
            factor = jnp.exp2(old_max - new_max)
            max_s[slot] = new_max
            sum_s[slot] = sum_s[slot] * factor + jnp.sum(weights, axis=0, keepdims=True)
            acc_s[slot] = acc_s[slot] * factor + dot32(v_blk, weights.astype(jnp.bfloat16), TN)

    def forward_blocks(blk, carry):
        over_tiles(forward_body, blk)
        return carry

    lax.fori_loop(first, me, forward_blocks, 0)

    unit = (lax.broadcasted_iota(jnp.int32, (128, 128), 0)
            == lax.broadcasted_iota(jnp.int32, (128, 128), 1)).astype(jnp.bfloat16)

    def turned(block_t):
        return dot32(unit, block_t, NT).astype(jnp.bfloat16)

    for tile in range(tiles):
        for head in range(kv_heads):
            slot = head * tiles + tile
            total = sum_s[slot]
            max_s[slot] = max_s[slot] + jnp.log2(total)
            out_t = (acc_s[slot] / total).astype(jnp.bfloat16)
            first_col = head * group * 128
            do_t = jnp.concatenate(
                [dot_ref[first_col + member * 128:first_col + (member + 1) * 128, tile * QT:(tile + 1) * QT]
                 for member in range(group)], axis=1)
            delta_s[slot] = jnp.sum(do_t.astype(jnp.float32) * out_t.astype(jnp.float32), axis=0, keepdims=True)
            for member in range(group):
                col = first_col + member * 128
                o_ref[tile * QT:(tile + 1) * QT, col:col + 128] = turned(out_t[:, member * QT:(member + 1) * QT])

    def grads(tile, head, blk, keys, mask_fn):
        slot = head * tiles + tile
        q_tile = stack_heads(q_ref, tile, head, group)
        do_tile = stack_heads(do_ref, tile, head, group)
        k_blk = kv_ref[blk, 0:keys, k_cols(head)]
        v_blk = kv_ref[blk, 0:keys, v_cols(head)]
        scores = dot32(k_blk, q_tile, NT) * scale2
        if mask_fn is not None:
            scores = jnp.where(mask_fn(), scores, NEG_INF)
        prob = jnp.exp2(scores - max_s[slot])
        dprob = dot32(v_blk, do_tile, NT)
        dscore = (prob * (dprob - delta_s[slot])).astype(jnp.bfloat16)
        dv_part = dot32(prob.astype(jnp.bfloat16), do_tile, NN)
        dk_part = dot32(dscore, q_tile, NN)
        dq_part = dot32(k_blk, dscore, TN)
        return dq_part, dk_part, dv_part

    for tile in reversed(range(tiles)):
        keys = QT * (tile + 1)
        for head in range(kv_heads):
            dq_part, dk_part, dv_part = grads(tile, head, me, keys, functools.partial(diag_mask, tile, keys))
            acc_s[head * tiles + tile] = dq_part
            if tile == tiles - 1:
                grad_s[me, 0:keys, k_cols(head)] = dk_part
                grad_s[me, 0:keys, v_cols(head)] = dv_part
            else:
                grad_s[me, 0:keys, k_cols(head)] = grad_s[me, 0:keys, k_cols(head)] + dk_part
                grad_s[me, 0:keys, v_cols(head)] = grad_s[me, 0:keys, v_cols(head)] + dv_part
    grad_copy(me).start()

    def backward_body(tile, masked, blk):
        for head in range(kv_heads):
            slot = head * tiles + tile
            dq_part, dk_part, dv_part = grads(tile, head, blk, tok, functools.partial(off_mask, tile, blk) if masked else None)
            acc_s[slot] = acc_s[slot] + dq_part
            grad_s[blk, :, k_cols(head)] = grad_s[blk, :, k_cols(head)] + dk_part
            grad_s[blk, :, v_cols(head)] = grad_s[blk, :, v_cols(head)] + dv_part

    def backward_blocks(blk, carry):
        grad_s[blk] = jnp.zeros(zero_s.shape, jnp.float32)
        over_tiles(backward_body, blk)
        grad_copy(blk).start()
        return carry

    lax.fori_loop(first, me, backward_blocks, 0)

    for tile in range(tiles):
        for head in range(kv_heads):
            grad_t = (acc_s[head * tiles + tile] * scale).astype(jnp.bfloat16)
            for member in range(group):
                col = (head * group + member) * 128
                dq_ref[tile * QT:(tile + 1) * QT, col:col + 128] = turned(grad_t[:, member * QT:(member + 1) * QT])

    def wait_body(blk, carry):
        zero_copy(blk).wait()
        return carry

    lax.fori_loop(0, blocks, wait_body, 0)


def places(n):
    me = lax.axis_index('cp')
    chips = n // 2
    core = lax.rem(me, 2)
    chip = me // 2

    def at(offset, which):
        return lax.rem(chip + offset + chips, chips) * 2 + which

    return me, chips, core, chip, at


def remote(src, dst, send_sem, recv_sem, target):
    return pltpu.make_async_remote_copy(src_ref=src, dst_ref=dst, send_sem=send_sem, recv_sem=recv_sem,
                                        device_id={'cp': target}, device_id_type=pl.DeviceIdType.MESH)


def greet(targets):
    barrier = pltpu.get_barrier_semaphore()
    for target in targets:
        pl.semaphore_signal(barrier, inc=1, device_id={'cp': target}, device_id_type=pl.DeviceIdType.MESH)
    pl.semaphore_wait(barrier, len(targets))


def gather_kernel(n, seg_ref, x_ref, dy_ref, wkv_ref, wq_ref, wo_ref,
                  kv_all_ref, seg_all_ref, q_ref, do_ref, dot_ref,
                  kv_s, wq_s, wo_s, load_sem, seg_send, seg_recv, ring_send, ring_recv, pair_send, pair_recv,
                  mate_send, mate_recv):
    me, chips, core, chip, at = places(n)
    mate = at(0, 1 - core)
    half = kv_s.shape[0] // 2
    reach = chips // 2
    load_q = pltpu.make_async_copy(wq_ref, wq_s, load_sem.at[0])
    load_o = pltpu.make_async_copy(wo_ref, wo_s, load_sem.at[1])
    load_q.start()
    load_o.start()
    kv_s[...] = dot32(x_ref[...], wkv_ref[...], NN).astype(jnp.bfloat16)
    greet([lax.rem(me + step, n) for step in range(1, n)])

    def rows(sub):
        return pl.ds(sub * half, half)

    def ring_copy(way, sub, hop):
        offset = -(hop - 1) if way == 0 else hop - 1
        owner = at(offset, core)
        src = kv_s.at[rows(sub)] if hop == 1 else kv_all_ref.at[owner, rows(sub)]
        return remote(src, kv_all_ref.at[owner, rows(sub)], ring_send.at[way, sub, hop - 1], ring_recv.at[way, sub, hop - 1],
                      at(1 if way == 0 else -1, core))

    def pair_copy(way, sub, hop):
        owner = at(-hop if way == 0 else hop, core)
        return remote(kv_all_ref.at[owner, rows(sub)], kv_all_ref.at[owner, rows(sub)],
                      pair_send.at[way, sub, hop - 1], pair_recv.at[way, sub, hop - 1], mate)

    def seg_copy(step):
        return remote(seg_ref, seg_all_ref.at[me], seg_send.at[step - 1], seg_recv.at[step - 1], lax.rem(me + step, n))

    hops = [(way, sub, hop) for hop in range(1, reach + 1) for sub in range(2) for way in range(2)
            if hop < reach or way == sub]
    started = []
    for way, sub, hop in hops:
        if hop == 1:
            started.append(ring_copy(way, sub, hop))
            started[-1].start()
    for step in range(1, n):
        started.append(seg_copy(step))
        started[-1].start()
    started.append(remote(kv_s, kv_all_ref.at[me], mate_send.at[0], mate_recv.at[0], mate))
    started[-1].start()
    kv_all_ref[me] = kv_s[...]
    seg_all_ref[me] = seg_ref[...]

    heads = wq_s.shape[0]
    strip = x_ref.shape[1] * 2 // heads

    def project(src_ref, w_s, dst_ref, pair):
        w_pair = jnp.concatenate([w_s[2 * pair], w_s[2 * pair + 1]], axis=1)
        dst_ref[:, pair * 256:(pair + 1) * 256] = dot32(src_ref[...], w_pair, NN).astype(jnp.bfloat16)

    def flip(src_ref, dst_ref, part):
        dst_ref[part * strip:(part + 1) * strip, :] = src_ref[:, part * strip:(part + 1) * strip].T

    work = []
    for pair in range(heads // 2):
        work.append(functools.partial(project, dy_ref, wo_s, do_ref, pair))
        work.append(functools.partial(project, x_ref, wq_s, q_ref, pair))
        work.append(functools.partial(flip, do_ref, dot_ref, pair))
    load_q.wait()
    load_o.wait()
    quota = -(-len(work) // len(hops))
    for index, (way, sub, hop) in enumerate(hops):
        for item in work[index * quota:(index + 1) * quota]:
            item()
        ring_copy(way, sub, hop).wait_recv()
        started.append(pair_copy(way, sub, hop))
        started[-1].start()
        if (way, sub, hop + 1) in hops:
            started.append(ring_copy(way, sub, hop + 1))
            started[-1].start()
    for way, sub, hop in hops:
        pair_copy(way, sub, hop).wait_recv()
    for step in range(1, n):
        seg_copy(step).wait_recv()
    remote(kv_s, kv_all_ref.at[me], mate_send.at[0], mate_recv.at[0], mate).wait_recv()
    for copy in started:
        copy.wait_send()


def reduce_kernel(n, scale, kv_width, dkv_ref, o_hbm, dq_hbm, x_hbm, dy_hbm, wkv_hbm, wq_ref, wo_ref,
                  y_ref, dx_ref, dwo_ref, dwq_ref, dwkv_ref,
                  o_ref, dq_ref, x_ref, dy_ref, wkv_ref, xt_ref, dyt_ref, xtp_ref, dytp_ref,
                  own_s, mate_s, slot1_s, stage1_s, grad_s, grad_mate_s, o_mate_s, dq_mate_s, slot2_s, stage2_s,
                  wq_s, wo_s, load_sem, block_sem, mate_send, mate_recv, ring_send, ring_recv, extra_send, extra_recv):
    me, chips, core, chip, at = places(n)
    mate = at(0, 1 - core)
    ring = (at(1, core), at(-1, core))
    tok = o_ref.shape[0]
    quarter = tok // 4
    heads, out_rows, head_dim = dwo_ref.shape
    loads = [pltpu.make_async_copy(src, dst, load_sem.at[index]) for index, (src, dst) in enumerate(
        ((o_hbm, o_ref), (dq_hbm, dq_ref), (x_hbm, x_ref), (dy_hbm, dy_ref), (wo_ref, wo_s), (wq_ref, wq_s),
         (wkv_hbm, wkv_ref)))]
    order = []
    for step in range(1, chips):
        for offset in (-step, step):
            if offset % chips not in order:
                order.append(offset % chips)
    order.append(0)
    own_loads = [pltpu.make_async_copy(dkv_ref.at[at(offset, core)], own_s.at[index], block_sem.at[index])
                 for index, offset in enumerate(order)]
    for load in own_loads:
        load.start()
    for load in loads:
        load.start()
    greet([ring[0], ring[1], mate])
    mate_copies = [remote(dkv_ref.at[at(offset, 1 - core)], mate_s.at[index], mate_send.at[index], mate_recv.at[index], mate)
                   for index, offset in enumerate(order)]
    extras = [remote(o_hbm, o_mate_s, extra_send.at[0], extra_recv.at[0], mate),
              remote(dq_hbm, dq_mate_s, extra_send.at[1], extra_recv.at[1], mate),
              remote(grad_s, grad_mate_s, extra_send.at[2], extra_recv.at[2], mate),
              remote(xt_ref, xtp_ref, extra_send.at[3], extra_recv.at[3], mate),
              remote(dyt_ref, dytp_ref, extra_send.at[4], extra_recv.at[4], mate)]
    for index, copy in enumerate(mate_copies):
        copy.start()
        if index == 3:
            extras[0].start()
            extras[1].start()

    ready = set()

    def need(position):
        if position not in ready:
            ready.add(position)
            own_loads[position].wait()
            mate_copies[position].wait_recv()

    def ring_copy(job, way, sub, step):
        slots, stage = (slot1_s, stage1_s) if job == 0 else (slot2_s, stage2_s)
        src = stage.at[way, sub] if step == 0 else slots.at[way, sub, step - 1]
        return remote(src, slots.at[way, sub, step], ring_send.at[job, way, sub, step], ring_recv.at[job, way, sub, step],
                      ring[way])

    started = []

    def send(job, way, sub, step):
        started.append(ring_copy(job, way, sub, step))
        started[-1].start()

    def contrib1(way, sub, step):
        offset = (-(1 + step) if way == 0 else 1 + step) % chips
        position = order.index(offset)
        need(position)
        span = slice((2 * way + sub) * quarter, (2 * way + sub + 1) * quarter)
        return own_s[position, span, :] + mate_s[position, span, :]

    cut = 7 * head_dim

    def contrib2(way, sub, step):
        offset = -(1 + step) if way == 0 else 1 + step
        first_row = pl.multiple_of(at(offset % chips, core) * out_rows, 32)
        take = pl.ds(first_row, out_rows)
        lhs, lhs_mate = (dyt_ref, dytp_ref) if way == 0 else (xt_ref, xtp_ref)
        rhs, rhs_mate = (o_ref, o_mate_s) if way == 0 else (dq_ref, dq_mate_s)
        if sub == 0:
            return (dot32(lhs[take, :], rhs[:, 0:cut], NN) + dot32(lhs_mate[take, :], rhs_mate[:, 0:cut], NN))
        main = dot32(lhs[take, :], rhs[:, cut:], NN) + dot32(lhs_mate[take, :], rhs_mate[:, cut:], NN)
        cols = slice(way * kv_width, (way + 1) * kv_width)
        side = dot32(xt_ref[take, :], grad_s[:, cols], NN) + dot32(xtp_ref[take, :], grad_mate_s[:, cols], NN)
        return jnp.concatenate([main, side], axis=1)

    strip = 256
    strips = y_ref.shape[1] // strip

    def rows_out(part):
        return pl.ds(pl.multiple_of(part * strip, strip), strip)

    def times_weight(src_ref, w_s, part):
        total = None
        for pair in range(heads // 2):
            w_pair = jnp.concatenate([w_s[2 * pair, rows_out(part), :], w_s[2 * pair + 1, rows_out(part), :]], axis=1)
            piece = dot32(src_ref[:, pair * 256:(pair + 1) * 256], w_pair, NT)
            total = piece if total is None else total + piece
        return total

    def y_strip(part, carry):
        y_ref[:, rows_out(part)] = times_weight(o_ref, wo_s, part).astype(jnp.bfloat16)
        return carry

    def flip_strip(part, carry):
        xt_ref[rows_out(part), :] = x_ref[:, rows_out(part)].T
        dyt_ref[rows_out(part), :] = dy_ref[:, rows_out(part)].T
        return carry

    def dx_strip(part, carry):
        wide = times_weight(dq_ref, wq_s, part) + dot32(grad_s[...], wkv_ref[rows_out(part), :], NT)
        dx_ref[:, rows_out(part)] = wide.astype(jnp.bfloat16)
        return carry

    steps = chips - 1
    both = [(sub, way) for sub in range(2) for way in range(2)]
    for sub, way in both:
        stage1_s[way, sub] = contrib1(way, sub, 0)
        send(0, way, sub, 0)
    for load in loads:
        load.wait()
    for step in range(steps):
        if step == 0:
            lax.fori_loop(0, strips, y_strip, 0)
        if step == 1:
            lax.fori_loop(0, strips, flip_strip, 0)
        if step == 4:
            extras[3].start()
            extras[4].start()
        if step == steps - 1:
            for index in (0, 1, 3, 4):
                extras[index].wait_recv()
            for way in range(2):
                stage2_s[way, 0] = contrib2(way, 0, 0)
                send(1, way, 0, 0)
        for sub, way in both:
            part = contrib1(way, sub, step + 1)
            ring_copy(0, way, sub, step).wait_recv()
            if step < steps - 1:
                slot1_s[way, sub, step] = slot1_s[way, sub, step] + part
                send(0, way, sub, step + 1)
            else:
                span = slice((2 * way + sub) * quarter, (2 * way + sub + 1) * quarter)
                total = slot1_s[way, sub, step] + part
                grad_s[span, 0:kv_width] = (total[:, 0:kv_width] * scale).astype(jnp.bfloat16)
                grad_s[span, kv_width:] = total[:, kv_width:].astype(jnp.bfloat16)
    extras[2].start()
    extras[2].wait_recv()
    for way in range(2):
        stage2_s[way, 1] = contrib2(way, 1, 0)
        send(1, way, 1, 0)
    for step in range(steps):
        if step == 0:
            lax.fori_loop(0, strips, dx_strip, 0)
        for sub, way in both:
            part = contrib2(way, sub, step + 1)
            ring_copy(1, way, sub, step).wait_recv()
            if step < steps - 1:
                slot2_s[way, sub, step] = slot2_s[way, sub, step] + part
                send(1, way, sub, step + 1)
            else:
                total = slot2_s[way, sub, step] + part
                out_ref = dwo_ref if way == 0 else dwq_ref
                base = 0 if sub == 0 else cut // head_dim
                for index in range(cut // head_dim if sub == 0 else heads - cut // head_dim):
                    out_ref[base + index] = total[:, index * head_dim:(index + 1) * head_dim]
                if sub == 1:
                    dwkv_ref[:, way * kv_width:(way + 1) * kv_width] = total[:, heads * head_dim - cut:]
    for copy in started + mate_copies + extras:
        copy.wait_send()


VMEM_SPEC = pl.BlockSpec(memory_space=pltpu.VMEM)
ANY_SPEC = pl.BlockSpec(memory_space=pl.ANY)
VMEM_LIMIT = 60 * 1024 * 1024
REDUCE_LIMIT = 67043328


def solution(mesh):
    group_count = mesh.shape['cp']
    row_spec = P(('dp', 'cp'), None)
    tok_spec = P(('dp', 'cp'))
    weight_spec = P(None, None, None)
    grad_spec = P(('dp', 'cp'), None, None)

    def local_step(x_act, seg_ids, w_q, w_k, w_v, w_o, dy_act):
        tok = x_act.shape[0]
        model_dim, q_heads, head_dim = w_q.shape
        kv_heads = w_k.shape[1]
        group = q_heads // kv_heads
        q_width = q_heads * head_dim
        kv_width = kv_heads * head_dim
        tiles = tok // QT
        scale = head_dim ** -0.5
        bf16 = jnp.bfloat16

        w_kv = jnp.concatenate([w_k.reshape(model_dim, kv_width), w_v.reshape(model_dim, kv_width)], axis=1)
        seg_rows = seg_ids.reshape(tok // 128, 128)
        wq_heads = w_q.transpose(1, 0, 2)
        wo_heads = w_o.transpose(1, 0, 2)

        slots = kv_heads * tiles
        width = group * QT
        chips = group_count // 2
        reach = chips // 2
        dma = pltpu.SemaphoreType.DMA
        f32 = jnp.float32
        shape = jax.ShapeDtypeStruct
        flat = shape((tok, q_width), bf16)
        kv_all, seg_all, q_loc, do_loc, do_turned = pl.pallas_call(
            functools.partial(gather_kernel, group_count),
            out_shape=(shape((group_count, tok, 2 * kv_width), bf16), shape((group_count, tok // 128, 128), jnp.int32),
                       flat, flat, shape((q_width, tok), bf16)),
            in_specs=[VMEM_SPEC] * 4 + [ANY_SPEC] * 2,
            out_specs=(VMEM_SPEC,) * 5,
            scratch_shapes=[pltpu.VMEM((tok, 2 * kv_width), bf16), pltpu.VMEM((q_heads, model_dim, head_dim), bf16), pltpu.VMEM((q_heads, model_dim, head_dim), bf16),
                            dma((2,)), dma((group_count - 1,)), dma((group_count - 1,)),
                            dma((2, 2, reach)), dma((2, 2, reach)), dma((2, 2, reach)), dma((2, 2, reach)), dma((1,)), dma((1,))],
            compiler_params=pltpu.CompilerParams(collective_id=0, has_side_effects=True, vmem_limit_bytes=VMEM_LIMIT),
            cost_estimate=pl.CostEstimate(flops=8 * tok * model_dim * q_width, bytes_accessed=2**24, transcendentals=0),
            name='gather_keys',
        )(seg_rows, x_act, dy_act, w_kv, wq_heads, wo_heads)

        o_loc, dq_loc, dkv_all = pl.pallas_call(
            functools.partial(attention_kernel, kv_heads, group, scale),
            out_shape=(flat, flat, shape((group_count, tok, 2 * kv_width), f32)),
            in_specs=[VMEM_SPEC] * 6,
            out_specs=(VMEM_SPEC, VMEM_SPEC, ANY_SPEC),
            scratch_shapes=[pltpu.VMEM((tiles, 1, width), jnp.int32), pltpu.VMEM((slots, 1, width), f32),
                            pltpu.VMEM((slots, 1, width), f32), pltpu.VMEM((slots, 1, width), f32),
                            pltpu.VMEM((slots, head_dim, width), f32), pltpu.VMEM((group_count, tok, 2 * kv_width), f32),
                            pltpu.VMEM((tok, 2 * kv_width), f32), dma((group_count,))],
            compiler_params=pltpu.CompilerParams(vmem_limit_bytes=VMEM_LIMIT),
            cost_estimate=pl.CostEstimate(flops=16 * 14 * tok * tok * q_width, bytes_accessed=2**25, transcendentals=0),
            name='attend',
        )(seg_rows, seg_all, q_loc, do_loc, do_turned, kv_all)

        out_rows = model_dim // group_count
        blk = (tok, 2 * kv_width)
        cols2 = (q_width + kv_width) // 2
        steps = chips - 1
        head_grad = shape((q_heads, out_rows, head_dim), f32)
        y_out, dx_out, dwo, dwq, dwkv = pl.pallas_call(
            functools.partial(reduce_kernel, group_count, scale, kv_width),
            out_shape=(shape((tok, model_dim), bf16), shape((tok, model_dim), bf16), head_grad, head_grad,
                       shape((out_rows, 2 * kv_width), f32)),
            in_specs=[ANY_SPEC] * 8,
            out_specs=(VMEM_SPEC,) * 5,
            scratch_shapes=[pltpu.VMEM((tok, q_width), bf16), pltpu.VMEM((tok, q_width), bf16),
                            pltpu.VMEM((tok, model_dim), bf16), pltpu.VMEM((tok, model_dim), bf16),
                            pltpu.VMEM((model_dim, 2 * kv_width), bf16),
                            pltpu.VMEM((model_dim, tok), bf16), pltpu.VMEM((model_dim, tok), bf16),
                            pltpu.VMEM((model_dim, tok), bf16), pltpu.VMEM((model_dim, tok), bf16),
                            pltpu.VMEM((chips,) + blk, f32), pltpu.VMEM((chips,) + blk, f32),
                            pltpu.VMEM((2, 2, steps, tok // 4, 2 * kv_width), f32), pltpu.VMEM((2, 2, tok // 4, 2 * kv_width), f32),
                            pltpu.VMEM(blk, bf16), pltpu.VMEM(blk, bf16),
                            pltpu.VMEM((tok, q_width), bf16), pltpu.VMEM((tok, q_width), bf16),
                            pltpu.VMEM((2, 2, steps, out_rows, cols2), f32), pltpu.VMEM((2, 2, out_rows, cols2), f32),
                            pltpu.VMEM((q_heads, model_dim, head_dim), bf16), pltpu.VMEM((q_heads, model_dim, head_dim), bf16),
                            dma((7,)), dma((chips,)), dma((chips,)), dma((chips,)),
                            dma((2, 2, 2, steps)), dma((2, 2, 2, steps)), dma((5,)), dma((5,))],
            compiler_params=pltpu.CompilerParams(collective_id=1, has_side_effects=True, vmem_limit_bytes=REDUCE_LIMIT),
            cost_estimate=pl.CostEstimate(flops=16 * tok * model_dim * q_width, bytes_accessed=2**25, transcendentals=0),
            name='reduce_grads',
        )(dkv_all, o_loc, dq_loc, x_act, dy_act, w_kv, wq_heads, wo_heads)
        dwk = dwkv[:, :kv_width].reshape(out_rows, kv_heads, head_dim)
        dwv = dwkv[:, kv_width:].reshape(out_rows, kv_heads, head_dim)
        return y_out, dx_out, dwq.transpose(1, 0, 2), dwk, dwv, dwo.transpose(1, 0, 2)

    return jax.shard_map(local_step, mesh=mesh,
                         in_specs=(row_spec, tok_spec, weight_spec, weight_spec, weight_spec, weight_spec, row_spec),
                         out_specs=(row_spec, row_spec, grad_spec, grad_spec, grad_spec, grad_spec),
                         check_vma=False)
```

```python
import functools

import jax
import jax.numpy as jnp
from jax import lax
from jax.experimental import pallas as pl
from jax.experimental.pallas import tpu as pltpu
from jax.sharding import PartitionSpec as P

QT = 128
LOG2E = 1.4426950408889634
NEG_INF = float('-inf')
NT = (((1,), (1,)), ((), ()))
TN = (((0,), (0,)), ((), ()))
NN = (((1,), (0,)), ((), ()))


def dot32(left_arg, right_arg, dims):
    return lax.dot_general(left_arg, right_arg, dims, preferred_element_type=jnp.float32)


def stack_heads(ref, tile, head, group):
    rows = pl.ds(pl.multiple_of(tile * QT, QT), QT)
    return jnp.concatenate(
        [ref[rows, (head * group + member) * 128:(head * group + member + 1) * 128] for member in range(group)], axis=0)


def member_rows(ref, tile, head, group, chunk):
    rows = pl.ds(pl.multiple_of(tile * QT, QT), QT)
    first = (head * group + 2 * chunk) * 128
    return jnp.concatenate([ref[rows, first:first + 128], ref[rows, first + 128:first + 256]], axis=0)


def forward_update(kv_heads, group, scale2, tile, q_ref, kv_ref, blk, stats, mask_row, keys=None, diag=False):
    keys = kv_ref.shape[1] if keys is None else keys
    chains = [(head, chunk) for chunk in range(group // 2) for head in range(kv_heads)]
    k_blks = [kv_ref[blk, 0:keys, head * 128:(head + 1) * 128] for head in range(kv_heads)]
    v_turned = [kv_ref[blk, 0:keys, (kv_heads + head) * 128:(kv_heads + head + 1) * 128].T for head in range(kv_heads)]
    old = [None if diag else (stats[head][0][tile], stats[head][1][tile]) for head in range(kv_heads)]
    new_rows = [([], []) for head in range(kv_heads)]

    def score(chain):
        head, chunk = chain
        return dot32(k_blks[head], member_rows(q_ref, tile, head, group, chunk), NT) * scale2

    pending = [score(chain) for chain in chains[:2]]
    for index, (head, chunk) in enumerate(chains):
        scores = pending.pop(0)
        if index + 2 < len(chains):
            pending.append(score(chains[index + 2]))
        cols = slice(chunk * 256, (chunk + 1) * 256)
        if mask_row is not None:
            key_pos = lax.broadcasted_iota(jnp.int32, (keys, 256), 0)
            allowed = key_pos >= mask_row[:, cols]
            if diag:
                query_pos = lax.rem(lax.broadcasted_iota(jnp.int32, (1, 256), 1), QT) + tile * QT
                allowed = allowed & (key_pos <= query_pos)
            scores = jnp.where(allowed, scores, NEG_INF)
        new_max = jnp.max(scores, axis=0, keepdims=True)
        if not diag:
            old_max = old[head][0][:, cols]
            new_max = jnp.maximum(old_max, new_max)
        weights = jnp.exp2(scores - new_max)
        total = jnp.sum(weights, axis=0, keepdims=True)
        part = dot32(v_turned[head], weights.astype(jnp.bfloat16), NN)
        acc = stats[head][2]
        if diag:
            acc[tile, :, cols] = part
        else:
            factor = jnp.exp2(old_max - new_max)
            total = old[head][1][:, cols] * factor + total
            acc[tile, :, cols] = acc[tile, :, cols] * factor + part
        new_rows[head][0].append(new_max)
        new_rows[head][1].append(total)
    for head in range(kv_heads):
        stats[head][0][tile] = jnp.concatenate(new_rows[head][0], axis=1)
        stats[head][1][tile] = jnp.concatenate(new_rows[head][1], axis=1)


def attention_kernel(kv_heads, group, scale, seg_ref, seg_all_ref, q_ref, do_ref, dot_ref, kv_ref, start_s,
                     max0_ref, max1_ref, sum0_ref, sum1_ref, acc0_ref, acc1_ref,
                     o_ref, dq_ref, dkv_ref, max0_s, max1_s, sum0_s, sum1_s, delta_s, acc0_s, acc1_s,
                     grad_s, zero_s, out_sem):
    tok = q_ref.shape[0]
    blocks = kv_ref.shape[0]
    tiles = tok // QT
    width = group * QT
    scale2 = scale * LOG2E
    max_s, sum_s, acc_s = (max0_s, max1_s), (sum0_s, sum1_s), (acc0_s, acc1_s)
    stats = [(max_s[head], sum_s[head], acc_s[head]) for head in range(kv_heads)]
    me = lax.axis_index('cp')
    near_first = jnp.maximum(2 * (me // 2 - (blocks // 4 - 1)), 0)
    for kept_ref, kept_s in ((max0_ref, max0_s), (max1_ref, max1_s), (sum0_ref, sum0_s), (sum1_ref, sum1_s),
                             (acc0_ref, acc0_s), (acc1_ref, acc1_s)):
        kept_s[...] = kept_ref[...]
    zero_s[...] = jnp.zeros(zero_s.shape, jnp.float32)

    seg_own = seg_ref[...]
    first_seg = jnp.min(seg_own)
    head_count = jnp.sum((seg_own == first_seg).astype(jnp.int32))
    shard_index = lax.broadcasted_iota(jnp.int32, seg_all_ref.shape, 0)
    earlier = (shard_index < me) & (seg_all_ref[...] < first_seg)
    doc_start = jnp.sum(earlier.astype(jnp.int32))
    first = doc_start // tok
    has_prev = doc_start < me * tok
    tiles_prev = jnp.where(has_prev, (head_count + QT - 1) // QT, 0)
    full_tiles = head_count // QT

    def zero_copy(blk):
        return pltpu.make_async_copy(zero_s, dkv_ref.at[blk], out_sem.at[blk])

    def grad_copy(blk):
        return pltpu.make_async_copy(grad_s.at[blk], dkv_ref.at[blk], out_sem.at[blk])

    def clear_body(blk, carry):
        zero_copy(blk).start()
        return carry

    lax.fori_loop(0, first, clear_body, 0)
    lax.fori_loop(me + 1, blocks, clear_body, 0)

    def k_cols(head):
        return slice(head * 128, (head + 1) * 128)

    def v_cols(head):
        return slice((kv_heads + head) * 128, (kv_heads + head + 1) * 128)

    def diag_mask(tile, keys):
        key_pos = lax.broadcasted_iota(jnp.int32, (keys, width), 0)
        query_pos = lax.rem(lax.broadcasted_iota(jnp.int32, (1, width), 1), QT) + tile * QT
        return (key_pos <= query_pos) & (key_pos >= start_s[tile])

    def off_mask(tile, blk):
        key_pos = lax.broadcasted_iota(jnp.int32, (tok, width), 0)
        return key_pos >= start_s[tile] + (me - blk) * tok

    def over_tiles(body, blk):
        def tile_body(tile, carry):
            masked = (blk == first) | (tile >= full_tiles)
            pl.when(masked)(functools.partial(body, tile, True, blk))
            pl.when(jnp.logical_not(masked))(functools.partial(body, tile, False, blk))
            return carry
        lax.fori_loop(0, tiles_prev, tile_body, 0)

    def forward_body(tile, masked, blk):
        row = start_s[tile] + (me - blk) * tok if masked else None
        forward_update(kv_heads, group, scale2, tile, q_ref, kv_ref, blk, stats, row)

    def forward_blocks(blk, carry):
        over_tiles(forward_body, blk)
        return carry

    lax.fori_loop(first, jnp.maximum(first, near_first), forward_blocks, 0)

    unit = (lax.broadcasted_iota(jnp.int32, (128, 128), 0)
            == lax.broadcasted_iota(jnp.int32, (128, 128), 1)).astype(jnp.bfloat16)

    def turned(block_t):
        return dot32(unit, block_t, NT).astype(jnp.bfloat16)

    for tile in range(tiles):
        for head in range(kv_heads):
            slot = head * tiles + tile
            total = sum_s[head][tile]
            max_s[head][tile] = max_s[head][tile] + jnp.log2(total)
            out_t = (acc_s[head][tile] / total).astype(jnp.bfloat16)
            first_col = head * group * 128
            do_t = jnp.concatenate(
                [dot_ref[first_col + member * 128:first_col + (member + 1) * 128, tile * QT:(tile + 1) * QT]
                 for member in range(group)], axis=1)
            delta_s[slot] = jnp.sum(do_t.astype(jnp.float32) * out_t.astype(jnp.float32), axis=0, keepdims=True)
            for member in range(group):
                col = first_col + member * 128
                o_ref[tile * QT:(tile + 1) * QT, col:col + 128] = turned(out_t[:, member * QT:(member + 1) * QT])

    def grads(tile, head, blk, keys, mask_fn):
        slot = head * tiles + tile
        q_tile = stack_heads(q_ref, tile, head, group)
        do_tile = stack_heads(do_ref, tile, head, group)
        k_blk = kv_ref[blk, 0:keys, k_cols(head)]
        v_blk = kv_ref[blk, 0:keys, v_cols(head)]
        scores = dot32(k_blk, q_tile, NT) * scale2
        if mask_fn is not None:
            scores = jnp.where(mask_fn(), scores, NEG_INF)
        prob = jnp.exp2(scores - max_s[head][tile])
        dprob = dot32(v_blk, do_tile, NT)
        dscore = (prob * (dprob - delta_s[slot])).astype(jnp.bfloat16)
        dv_part = dot32(prob.astype(jnp.bfloat16), do_tile, NN)
        dk_part = dot32(dscore, q_tile, NN)
        dq_part = dot32(k_blk, dscore, TN)
        return dq_part, dk_part, dv_part

    for tile in reversed(range(tiles)):
        keys = QT * (tile + 1)
        for head in range(kv_heads):
            dq_part, dk_part, dv_part = grads(tile, head, me, keys, functools.partial(diag_mask, tile, keys))
            acc_s[head][tile] = dq_part
            if tile == tiles - 1:
                grad_s[me, 0:keys, k_cols(head)] = dk_part
                grad_s[me, 0:keys, v_cols(head)] = dv_part
            else:
                grad_s[me, 0:keys, k_cols(head)] = grad_s[me, 0:keys, k_cols(head)] + dk_part
                grad_s[me, 0:keys, v_cols(head)] = grad_s[me, 0:keys, v_cols(head)] + dv_part
    grad_copy(me).start()

    def backward_body(tile, masked, blk):
        for head in range(kv_heads):
            slot = head * tiles + tile
            dq_part, dk_part, dv_part = grads(tile, head, blk, tok, functools.partial(off_mask, tile, blk) if masked else None)
            acc_s[head][tile] = acc_s[head][tile] + dq_part
            grad_s[blk, :, k_cols(head)] = grad_s[blk, :, k_cols(head)] + dk_part
            grad_s[blk, :, v_cols(head)] = grad_s[blk, :, v_cols(head)] + dv_part

    def backward_blocks(blk, carry):
        grad_s[blk] = jnp.zeros(zero_s.shape, jnp.float32)
        over_tiles(backward_body, blk)
        grad_copy(blk).start()
        return carry

    lax.fori_loop(first, me, backward_blocks, 0)

    for tile in range(tiles):
        for head in range(kv_heads):
            grad_t = (acc_s[head][tile] * scale).astype(jnp.bfloat16)
            for member in range(group):
                col = (head * group + member) * 128
                dq_ref[tile * QT:(tile + 1) * QT, col:col + 128] = turned(grad_t[:, member * QT:(member + 1) * QT])

    def wait_body(blk, carry):
        zero_copy(blk).wait()
        return carry

    lax.fori_loop(0, blocks, wait_body, 0)


def places(n):
    me = lax.axis_index('cp')
    chips = n // 2
    core = lax.rem(me, 2)
    chip = me // 2

    def at(offset, which):
        return lax.rem(chip + offset + chips, chips) * 2 + which

    return me, chips, core, chip, at


def remote(src, dst, send_sem, recv_sem, target):
    return pltpu.make_async_remote_copy(src_ref=src, dst_ref=dst, send_sem=send_sem, recv_sem=recv_sem,
                                        device_id={'cp': target}, device_id_type=pl.DeviceIdType.MESH)


def greet(targets):
    barrier = pltpu.get_barrier_semaphore()
    for target in targets:
        pl.semaphore_signal(barrier, inc=1, device_id={'cp': target}, device_id_type=pl.DeviceIdType.MESH)
    pl.semaphore_wait(barrier, len(targets))


def gather_kernel(n, kv_heads, group, scale2, seg_ref, x_ref, dy_ref, wkv_ref, wq_ref, wo_ref,
                  kv_all_ref, seg_all_ref, q_ref, do_ref, dot_ref, start_ref,
                  max0_ref, max1_ref, sum0_ref, sum1_ref, acc0_ref, acc1_ref,
                  kv_s, wq_s, wo_s, load_sem, seg_send, seg_recv, ring_send, ring_recv, pair_send, pair_recv,
                  mate_send, mate_recv):
    me, chips, core, chip, at = places(n)
    mate = at(0, 1 - core)
    tok = kv_s.shape[0]
    tiles = tok // QT
    half = tok // 2
    reach = chips // 2
    stats = [(max0_ref, sum0_ref, acc0_ref), (max1_ref, sum1_ref, acc1_ref)]
    load_q = pltpu.make_async_copy(wq_ref, wq_s, load_sem.at[0])
    load_o = pltpu.make_async_copy(wo_ref, wo_s, load_sem.at[1])
    load_q.start()
    load_o.start()
    kv_own = dot32(x_ref[...], wkv_ref[...], NN).astype(jnp.bfloat16)
    kv_s[...] = kv_own
    kv_all_ref[me] = kv_own
    seg_all_ref[me] = seg_ref[...]
    greet([lax.rem(me + step, n) for step in range(1, n)])

    def rows(sub):
        return pl.ds(sub * half, half)

    def ring_copy(way, sub, hop):
        offset = 1 - hop if way == 0 else hop - 1
        spot = kv_all_ref.at[at(offset, core), rows(sub)]
        return remote(spot, spot, ring_send.at[way, sub, hop - 1], ring_recv.at[way, sub, hop - 1],
                      at(1 if way == 0 else -1, core))

    def pair_copy(way, sub, hop):
        spot = kv_all_ref.at[at(-hop if way == 0 else hop, core), rows(sub)]
        return remote(spot, spot, pair_send.at[way, sub, hop - 1], pair_recv.at[way, sub, hop - 1], mate)

    def seg_copy(step):
        return remote(seg_ref, seg_all_ref.at[me], seg_send.at[step - 1], seg_recv.at[step - 1], lax.rem(me + step, n))

    def own_copy():
        return remote(kv_s, kv_all_ref.at[me], mate_send.at[0], mate_recv.at[0], mate)

    both = [(way, sub) for sub in range(2) for way in range(2)]
    for way, sub in both:
        ring_copy(way, sub, 1).start()
    own_copy().start()
    for step in range(1, n):
        seg_copy(step).start()

    pairs = wq_s.shape[0] // 2

    def project(src_ref, w_s, dst_ref, pair):
        w_pair = jnp.concatenate([w_s[2 * pair], w_s[2 * pair + 1]], axis=1)
        cols = pl.ds(pl.multiple_of(pair * 256, 256), 256)
        value = dot32(src_ref[...], w_pair, NN).astype(jnp.bfloat16)
        dst_ref[:, cols] = value
        return value

    def query_pair(pair, carry):
        project(x_ref, wq_s, q_ref, pair)
        return carry

    load_q.wait()
    lax.fori_loop(0, pairs, query_pair, 0)

    for step in range(1, n):
        seg_copy(step).wait_recv()
    seg_own = seg_ref[...]
    first_seg = jnp.min(seg_own)
    shard_index = lax.broadcasted_iota(jnp.int32, seg_all_ref.shape, 0)
    earlier = (shard_index < me) & (seg_all_ref[...] < first_seg)
    doc_start = jnp.sum(earlier.astype(jnp.int32))
    seg_wide = seg_own.astype(jnp.float32)
    columns = [jnp.broadcast_to(seg_wide[part:part + 1, :], (128, 128)).T for part in range(tok // 128)]
    for tile in range(tiles):
        count = sum(jnp.sum((column < seg_wide[tile:tile + 1, :]).astype(jnp.int32), axis=0, keepdims=True)
                    for column in columns)
        row = jnp.where(count == 0, doc_start - me * tok, count)
        start_ref[tile] = jnp.concatenate([row] * group, axis=1)

    for tile in range(tiles):
        forward_update(kv_heads, group, scale2, tile, q_ref, kv_all_ref, me, stats, start_ref[tile], QT * (tile + 1), True)
    load_o.wait()

    def round_body(step, carry):
        for sub in range(2):
            for way in range(2):
                live = (step < reach - 1) if way != sub else (step < reach)

                @pl.when(live)
                def _():
                    ring_copy(way, sub, step + 1).wait_recv()
                    pair_copy(way, sub, step + 1).start()

                @pl.when((step + 1 < reach - 1) if way != sub else (step + 1 < reach))
                def _():
                    ring_copy(way, sub, step + 2).start()

            if sub == 0:
                @pl.when(step == 0)
                def _():
                    own_copy().wait_recv()

                @pl.when(step > 0)
                def _():
                    pair_copy(0, 0, step).wait_recv()
                    pair_copy(0, 1, step).wait_recv()

            @pl.when(2 * step + sub < pairs)
            def _():
                pair = 2 * step + sub
                value = project(dy_ref, wo_s, do_ref, pair)
                dot_ref[pl.ds(pl.multiple_of(pair * 256, 256), 256), :] = value.T

            near = (chip >= step) & ((step > 0) | ((core == 1) & (sub == 0)))

            @pl.when(near)
            def _():
                blk = 2 * (chip - step) + sub

                def tile_body(tile, inner):
                    forward_update(kv_heads, group, scale2, tile, q_ref, kv_all_ref, blk, stats,
                                   start_ref[tile] + (me - blk) * tok)
                    return inner

                lax.fori_loop(0, tiles, tile_body, 0)
        return carry

    lax.fori_loop(0, reach, round_body, 0)
    for way, sub in both:
        for hop in range(1, reach + 1):
            if hop < reach or way == sub:
                if way == 1 or hop == reach:
                    pair_copy(way, sub, hop).wait_recv()
                pair_copy(way, sub, hop).wait_send()
                ring_copy(way, sub, hop).wait_send()
    own_copy().wait_send()
    for step in range(1, n):
        seg_copy(step).wait_send()


def reduce_kernel(n, scale, kv_width, dkv_ref, o_hbm, dq_hbm, x_hbm, dy_hbm, wkv_hbm, wq_ref, wo_ref,
                  y_ref, dx_ref, dwo_ref, dwq_ref, dwkv_ref,
                  o_ref, dq_ref, x_ref, dy_ref, wkv_ref, xt_ref, dyt_ref, xtp_ref, dytp_ref,
                  own_s, mate_s, slot1_s, stage1_s, grad_s, grad_mate_s, o_mate_s, dq_mate_s, slot2_s, stage2_s,
                  wq_s, wo_s, load_sem, block_sem, mate_send, mate_recv, ring_send, ring_recv, extra_send, extra_recv):
    me, chips, core, chip, at = places(n)
    mate = at(0, 1 - core)
    ring = (at(1, core), at(-1, core))
    tok = o_ref.shape[0]
    quarter = tok // 4
    heads, out_rows, head_dim = dwo_ref.shape
    loads = [pltpu.make_async_copy(src, dst, load_sem.at[index]) for index, (src, dst) in enumerate(
        ((o_hbm, o_ref), (dq_hbm, dq_ref), (x_hbm, x_ref), (dy_hbm, dy_ref), (wo_ref, wo_s), (wq_ref, wq_s),
         (wkv_hbm, wkv_ref)))]
    order = []
    for step in range(1, chips):
        for offset in (-step, step):
            if offset % chips not in order:
                order.append(offset % chips)
    order.append(0)
    own_loads = [pltpu.make_async_copy(dkv_ref.at[at(offset, core)], own_s.at[index], block_sem.at[index])
                 for index, offset in enumerate(order)]
    for load in own_loads:
        load.start()
    for load in loads:
        load.start()
    greet([ring[0], ring[1], mate])
    mate_copies = [remote(dkv_ref.at[at(offset, 1 - core)], mate_s.at[index], mate_send.at[index], mate_recv.at[index], mate)
                   for index, offset in enumerate(order)]
    extras = [remote(o_hbm, o_mate_s, extra_send.at[0], extra_recv.at[0], mate),
              remote(dq_hbm, dq_mate_s, extra_send.at[1], extra_recv.at[1], mate),
              remote(grad_s, grad_mate_s, extra_send.at[2], extra_recv.at[2], mate),
              remote(xt_ref, xtp_ref, extra_send.at[3], extra_recv.at[3], mate),
              remote(dyt_ref, dytp_ref, extra_send.at[4], extra_recv.at[4], mate)]
    for index, copy in enumerate(mate_copies):
        copy.start()
        if index == 3:
            extras[0].start()
            extras[1].start()

    ready = set()

    def need(position):
        if position not in ready:
            ready.add(position)
            own_loads[position].wait()
            mate_copies[position].wait_recv()

    def ring_copy(job, way, sub, step):
        slots, stage = (slot1_s, stage1_s) if job == 0 else (slot2_s, stage2_s)
        src = stage.at[way, sub] if step == 0 else slots.at[way, sub, step - 1]
        return remote(src, slots.at[way, sub, step], ring_send.at[job, way, sub, step], ring_recv.at[job, way, sub, step],
                      ring[way])

    started = []

    def send(job, way, sub, step):
        started.append(ring_copy(job, way, sub, step))
        started[-1].start()

    def contrib1(way, sub, step):
        offset = (-(1 + step) if way == 0 else 1 + step) % chips
        position = order.index(offset)
        need(position)
        span = slice((2 * way + sub) * quarter, (2 * way + sub + 1) * quarter)
        return own_s[position, span, :] + mate_s[position, span, :]

    cut = 7 * head_dim

    def contrib2(way, sub, step):
        offset = -(1 + step) if way == 0 else 1 + step
        first_row = pl.multiple_of(at(offset % chips, core) * out_rows, 32)
        take = pl.ds(first_row, out_rows)
        lhs, lhs_mate = (dyt_ref, dytp_ref) if way == 0 else (xt_ref, xtp_ref)
        rhs, rhs_mate = (o_ref, o_mate_s) if way == 0 else (dq_ref, dq_mate_s)
        if sub == 0:
            return (dot32(lhs[take, :], rhs[:, 0:cut], NN) + dot32(lhs_mate[take, :], rhs_mate[:, 0:cut], NN))
        main = dot32(lhs[take, :], rhs[:, cut:], NN) + dot32(lhs_mate[take, :], rhs_mate[:, cut:], NN)
        cols = slice(way * kv_width, (way + 1) * kv_width)
        side = dot32(xt_ref[take, :], grad_s[:, cols], NN) + dot32(xtp_ref[take, :], grad_mate_s[:, cols], NN)
        return jnp.concatenate([main, side], axis=1)

    strip = 256
    strips = y_ref.shape[1] // strip

    def rows_out(part):
        return pl.ds(pl.multiple_of(part * strip, strip), strip)

    def times_weight(src_ref, w_s, part):
        total = None
        for pair in range(heads // 2):
            w_pair = jnp.concatenate([w_s[2 * pair, rows_out(part), :], w_s[2 * pair + 1, rows_out(part), :]], axis=1)
            piece = dot32(src_ref[:, pair * 256:(pair + 1) * 256], w_pair, NT)
            total = piece if total is None else total + piece
        return total

    def y_strip(part, carry):
        y_ref[:, rows_out(part)] = times_weight(o_ref, wo_s, part).astype(jnp.bfloat16)
        return carry

    def flip_strip(part, carry):
        xt_ref[rows_out(part), :] = x_ref[:, rows_out(part)].T
        dyt_ref[rows_out(part), :] = dy_ref[:, rows_out(part)].T
        return carry

    def dx_strip(part, carry):
        wide = times_weight(dq_ref, wq_s, part) + dot32(grad_s[...], wkv_ref[rows_out(part), :], NT)
        dx_ref[:, rows_out(part)] = wide.astype(jnp.bfloat16)
        return carry

    steps = chips - 1
    both = [(sub, way) for sub in range(2) for way in range(2)]
    for sub, way in both:
        stage1_s[way, sub] = contrib1(way, sub, 0)
        send(0, way, sub, 0)
    for load in loads:
        load.wait()
    for step in range(steps):
        if step == 0:
            lax.fori_loop(0, strips, y_strip, 0)
        if step == 1:
            lax.fori_loop(0, strips, flip_strip, 0)
        if step == 4:
            extras[3].start()
            extras[4].start()
        if step == steps - 1:
            for index in (0, 1, 3, 4):
                extras[index].wait_recv()
            for way in range(2):
                stage2_s[way, 0] = contrib2(way, 0, 0)
                send(1, way, 0, 0)
        for sub, way in both:
            part = contrib1(way, sub, step + 1)
            ring_copy(0, way, sub, step).wait_recv()
            if step < steps - 1:
                slot1_s[way, sub, step] = slot1_s[way, sub, step] + part
                send(0, way, sub, step + 1)
            else:
                span = slice((2 * way + sub) * quarter, (2 * way + sub + 1) * quarter)
                total = slot1_s[way, sub, step] + part
                grad_s[span, 0:kv_width] = (total[:, 0:kv_width] * scale).astype(jnp.bfloat16)
                grad_s[span, kv_width:] = total[:, kv_width:].astype(jnp.bfloat16)
    extras[2].start()
    extras[2].wait_recv()
    for way in range(2):
        stage2_s[way, 1] = contrib2(way, 1, 0)
        send(1, way, 1, 0)
    for step in range(steps):
        if step == 0:
            lax.fori_loop(0, strips, dx_strip, 0)
        for sub, way in both:
            part = contrib2(way, sub, step + 1)
            ring_copy(1, way, sub, step).wait_recv()
            if step < steps - 1:
                slot2_s[way, sub, step] = slot2_s[way, sub, step] + part
                send(1, way, sub, step + 1)
            else:
                total = slot2_s[way, sub, step] + part
                out_ref = dwo_ref if way == 0 else dwq_ref
                base = 0 if sub == 0 else cut // head_dim
                for index in range(cut // head_dim if sub == 0 else heads - cut // head_dim):
                    out_ref[base + index] = total[:, index * head_dim:(index + 1) * head_dim]
                if sub == 1:
                    dwkv_ref[:, way * kv_width:(way + 1) * kv_width] = total[:, heads * head_dim - cut:]
    for copy in started + mate_copies + extras:
        copy.wait_send()


VMEM_SPEC = pl.BlockSpec(memory_space=pltpu.VMEM)
ANY_SPEC = pl.BlockSpec(memory_space=pl.ANY)
VMEM_LIMIT = 60 * 1024 * 1024
REDUCE_LIMIT = 67043328


def solution(mesh):
    group_count = mesh.shape['cp']
    row_spec = P(('dp', 'cp'), None)
    tok_spec = P(('dp', 'cp'))
    weight_spec = P(None, None, None)
    grad_spec = P(('dp', 'cp'), None, None)

    def local_step(x_act, seg_ids, w_q, w_k, w_v, w_o, dy_act):
        tok = x_act.shape[0]
        model_dim, q_heads, head_dim = w_q.shape
        kv_heads = w_k.shape[1]
        group = q_heads // kv_heads
        q_width = q_heads * head_dim
        kv_width = kv_heads * head_dim
        tiles = tok // QT
        scale = head_dim ** -0.5
        bf16 = jnp.bfloat16

        w_kv = jnp.concatenate([w_k.reshape(model_dim, kv_width), w_v.reshape(model_dim, kv_width)], axis=1)
        seg_rows = seg_ids.reshape(tok // 128, 128)
        wq_heads = w_q.transpose(1, 0, 2)
        wo_heads = w_o.transpose(1, 0, 2)

        slots = kv_heads * tiles
        width = group * QT
        chips = group_count // 2
        reach = chips // 2
        dma = pltpu.SemaphoreType.DMA
        f32 = jnp.float32
        shape = jax.ShapeDtypeStruct
        flat = shape((tok, q_width), bf16)
        row32 = shape((tiles, 1, width), f32)
        wide32 = shape((tiles, head_dim, width), f32)
        kv_all, seg_all, q_loc, do_loc, do_turned, *kept = pl.pallas_call(
            functools.partial(gather_kernel, group_count, kv_heads, group, scale * LOG2E),
            out_shape=(shape((group_count, tok, 2 * kv_width), bf16), shape((group_count, tok // 128, 128), jnp.int32),
                       flat, flat, shape((q_width, tok), bf16), shape((tiles, 1, width), jnp.int32),
                       row32, row32, row32, row32, wide32, wide32),
            in_specs=[VMEM_SPEC] * 4 + [ANY_SPEC] * 2,
            out_specs=(VMEM_SPEC,) * 12,
            scratch_shapes=[pltpu.VMEM((tok, 2 * kv_width), bf16), pltpu.VMEM((q_heads, model_dim, head_dim), bf16),
                            pltpu.VMEM((q_heads, model_dim, head_dim), bf16),
                            dma((2,)), dma((group_count - 1,)), dma((group_count - 1,)),
                            dma((2, 2, reach)), dma((2, 2, reach)), dma((2, 2, reach)), dma((2, 2, reach)), dma((1,)), dma((1,))],
            compiler_params=pltpu.CompilerParams(collective_id=0, has_side_effects=True, vmem_limit_bytes=VMEM_LIMIT),
            cost_estimate=pl.CostEstimate(flops=8 * tok * model_dim * q_width, bytes_accessed=2**24, transcendentals=0),
            name='gather_keys',
        )(seg_rows, x_act, dy_act, w_kv, wq_heads, wo_heads)

        o_loc, dq_loc, dkv_all = pl.pallas_call(
            functools.partial(attention_kernel, kv_heads, group, scale),
            out_shape=(flat, flat, shape((group_count, tok, 2 * kv_width), f32)),
            in_specs=[VMEM_SPEC] * 13,
            out_specs=(VMEM_SPEC, VMEM_SPEC, ANY_SPEC),
            scratch_shapes=[pltpu.VMEM((tiles, 1, width), f32)] * 4
                           + [pltpu.VMEM((slots, 1, width), f32)] + [pltpu.VMEM((tiles, head_dim, width), f32)] * 2
                           + [pltpu.VMEM((group_count, tok, 2 * kv_width), f32),
                            pltpu.VMEM((tok, 2 * kv_width), f32), dma((group_count,))],
            compiler_params=pltpu.CompilerParams(vmem_limit_bytes=VMEM_LIMIT),
            cost_estimate=pl.CostEstimate(flops=16 * 14 * tok * tok * q_width, bytes_accessed=2**25, transcendentals=0),
            name='attend',
        )(seg_rows, seg_all, q_loc, do_loc, do_turned, kv_all, *kept)

        out_rows = model_dim // group_count
        blk = (tok, 2 * kv_width)
        cols2 = (q_width + kv_width) // 2
        steps = chips - 1
        head_grad = shape((q_heads, out_rows, head_dim), f32)
        y_out, dx_out, dwo, dwq, dwkv = pl.pallas_call(
            functools.partial(reduce_kernel, group_count, scale, kv_width),
            out_shape=(shape((tok, model_dim), bf16), shape((tok, model_dim), bf16), head_grad, head_grad,
                       shape((out_rows, 2 * kv_width), f32)),
            in_specs=[ANY_SPEC] * 8,
            out_specs=(VMEM_SPEC,) * 5,
            scratch_shapes=[pltpu.VMEM((tok, q_width), bf16), pltpu.VMEM((tok, q_width), bf16),
                            pltpu.VMEM((tok, model_dim), bf16), pltpu.VMEM((tok, model_dim), bf16),
                            pltpu.VMEM((model_dim, 2 * kv_width), bf16),
                            pltpu.VMEM((model_dim, tok), bf16), pltpu.VMEM((model_dim, tok), bf16),
                            pltpu.VMEM((model_dim, tok), bf16), pltpu.VMEM((model_dim, tok), bf16),
                            pltpu.VMEM((chips,) + blk, f32), pltpu.VMEM((chips,) + blk, f32),
                            pltpu.VMEM((2, 2, steps, tok // 4, 2 * kv_width), f32), pltpu.VMEM((2, 2, tok // 4, 2 * kv_width), f32),
                            pltpu.VMEM(blk, bf16), pltpu.VMEM(blk, bf16),
                            pltpu.VMEM((tok, q_width), bf16), pltpu.VMEM((tok, q_width), bf16),
                            pltpu.VMEM((2, 2, steps, out_rows, cols2), f32), pltpu.VMEM((2, 2, out_rows, cols2), f32),
                            pltpu.VMEM((q_heads, model_dim, head_dim), bf16), pltpu.VMEM((q_heads, model_dim, head_dim), bf16),
                            dma((7,)), dma((chips,)), dma((chips,)), dma((chips,)),
                            dma((2, 2, 2, steps)), dma((2, 2, 2, steps)), dma((5,)), dma((5,))],
            compiler_params=pltpu.CompilerParams(collective_id=1, has_side_effects=True, vmem_limit_bytes=REDUCE_LIMIT),
            cost_estimate=pl.CostEstimate(flops=16 * tok * model_dim * q_width, bytes_accessed=2**25, transcendentals=0),
            name='reduce_grads',
        )(dkv_all, o_loc, dq_loc, x_act, dy_act, w_kv, wq_heads, wo_heads)
        dwk = dwkv[:, :kv_width].reshape(out_rows, kv_heads, head_dim)
        dwv = dwkv[:, kv_width:].reshape(out_rows, kv_heads, head_dim)
        return y_out, dx_out, dwq.transpose(1, 0, 2), dwk, dwv, dwo.transpose(1, 0, 2)

    return jax.shard_map(local_step, mesh=mesh,
                         in_specs=(row_spec, tok_spec, weight_spec, weight_spec, weight_spec, weight_spec, row_spec),
                         out_specs=(row_spec, row_spec, grad_spec, grad_spec, grad_spec, grad_spec),
                         check_vma=False)
```

```python
import functools

import jax
import jax.numpy as jnp
from jax import lax
from jax.experimental import pallas as pl
from jax.experimental.pallas import tpu as pltpu
from jax.sharding import PartitionSpec as P

QT = 128
SLICES = 6
LOG2E = 1.4426950408889634
NEG_INF = float('-inf')
NT = (((1,), (1,)), ((), ()))
TN = (((0,), (0,)), ((), ()))
NN = (((1,), (0,)), ((), ()))


def dot32(left_arg, right_arg, dims):
    return lax.dot_general(left_arg, right_arg, dims, preferred_element_type=jnp.float32)


def stack_heads(ref, tile, head, group):
    rows = pl.ds(pl.multiple_of(tile * QT, QT), QT)
    return jnp.concatenate(
        [ref[rows, (head * group + member) * 128:(head * group + member + 1) * 128] for member in range(group)], axis=0)


def member_rows(ref, tile, head, group, chunk):
    rows = pl.ds(pl.multiple_of(tile * QT, QT), QT)
    first = (head * group + 2 * chunk) * 128
    return jnp.concatenate([ref[rows, first:first + 128], ref[rows, first + 128:first + 256]], axis=0)


def forward_update(kv_heads, group, scale2, tile, q_ref, kv_ref, blk, stats, mask_row, keys=None, diag=False):
    keys = kv_ref.shape[1] if keys is None else keys
    chains = [(head, chunk) for chunk in range(group // 2) for head in range(kv_heads)]
    k_blks = [kv_ref[blk, 0:keys, head * 128:(head + 1) * 128] for head in range(kv_heads)]
    v_turned = [kv_ref[blk, 0:keys, (kv_heads + head) * 128:(kv_heads + head + 1) * 128].T for head in range(kv_heads)]
    old = [None if diag else (stats[head][0][tile], stats[head][1][tile]) for head in range(kv_heads)]
    new_rows = [([], []) for head in range(kv_heads)]

    def score(chain):
        head, chunk = chain
        return dot32(k_blks[head], member_rows(q_ref, tile, head, group, chunk), NT) * scale2

    pending = [score(chain) for chain in chains[:2]]
    for index, (head, chunk) in enumerate(chains):
        scores = pending.pop(0)
        if index + 2 < len(chains):
            pending.append(score(chains[index + 2]))
        cols = slice(chunk * 256, (chunk + 1) * 256)
        if mask_row is not None:
            key_pos = lax.broadcasted_iota(jnp.int32, (keys, 256), 0)
            allowed = key_pos >= mask_row[:, cols]
            if diag:
                query_pos = lax.rem(lax.broadcasted_iota(jnp.int32, (1, 256), 1), QT) + tile * QT
                allowed = allowed & (key_pos <= query_pos)
            scores = jnp.where(allowed, scores, NEG_INF)
        new_max = jnp.max(scores, axis=0, keepdims=True)
        if not diag:
            old_max = old[head][0][:, cols]
            new_max = jnp.maximum(old_max, new_max)
        weights = jnp.exp2(scores - new_max)
        total = jnp.sum(weights, axis=0, keepdims=True)
        part = dot32(v_turned[head], weights.astype(jnp.bfloat16), NN)
        acc = stats[head][2]
        if diag:
            acc[tile, :, cols] = part
        else:
            factor = jnp.exp2(old_max - new_max)
            total = old[head][1][:, cols] * factor + total
            acc[tile, :, cols] = acc[tile, :, cols] * factor + part
        new_rows[head][0].append(new_max)
        new_rows[head][1].append(total)
    for head in range(kv_heads):
        stats[head][0][tile] = jnp.concatenate(new_rows[head][0], axis=1)
        stats[head][1][tile] = jnp.concatenate(new_rows[head][1], axis=1)


def attention_kernel(kv_heads, group, scale, seg_ref, seg_all_ref, q_ref, do_ref, dot_ref, kv_ref, start_s,
                     max0_ref, max1_ref, sum0_ref, sum1_ref, acc0_ref, acc1_ref,
                     o_ref, dq_ref, dkv_ref, max0_s, max1_s, sum0_s, sum1_s, delta_s, acc0_s, acc1_s,
                     grad_s, zero_s, out_sem):
    tok = q_ref.shape[0]
    blocks = kv_ref.shape[0]
    tiles = tok // QT
    width = group * QT
    scale2 = scale * LOG2E
    max_s, sum_s, acc_s = (max0_s, max1_s), (sum0_s, sum1_s), (acc0_s, acc1_s)
    stats = [(max_s[head], sum_s[head], acc_s[head]) for head in range(kv_heads)]
    me = lax.axis_index('cp')
    near_first = jnp.maximum(2 * (me // 2 - (blocks // 4 - 1)), 0)
    for kept_ref, kept_s in ((max0_ref, max0_s), (max1_ref, max1_s), (sum0_ref, sum0_s), (sum1_ref, sum1_s),
                             (acc0_ref, acc0_s), (acc1_ref, acc1_s)):
        kept_s[...] = kept_ref[...]
    zero_s[...] = jnp.zeros(zero_s.shape, jnp.float32)

    seg_own = seg_ref[...]
    first_seg = jnp.min(seg_own)
    head_count = jnp.sum((seg_own == first_seg).astype(jnp.int32))
    shard_index = lax.broadcasted_iota(jnp.int32, seg_all_ref.shape, 0)
    earlier = (shard_index < me) & (seg_all_ref[...] < first_seg)
    doc_start = jnp.sum(earlier.astype(jnp.int32))
    first = doc_start // tok
    has_prev = doc_start < me * tok
    tiles_prev = jnp.where(has_prev, (head_count + QT - 1) // QT, 0)
    full_tiles = head_count // QT

    def zero_copy(blk):
        return pltpu.make_async_copy(zero_s, dkv_ref.at[blk], out_sem.at[blk])

    def grad_copy(blk):
        return pltpu.make_async_copy(grad_s.at[blk], dkv_ref.at[blk], out_sem.at[blk])

    def clear_body(blk, carry):
        zero_copy(blk).start()
        return carry

    lax.fori_loop(0, first, clear_body, 0)
    lax.fori_loop(me + 1, blocks, clear_body, 0)

    def k_cols(head):
        return slice(head * 128, (head + 1) * 128)

    def v_cols(head):
        return slice((kv_heads + head) * 128, (kv_heads + head + 1) * 128)

    def diag_mask(tile, keys):
        key_pos = lax.broadcasted_iota(jnp.int32, (keys, width), 0)
        query_pos = lax.rem(lax.broadcasted_iota(jnp.int32, (1, width), 1), QT) + tile * QT
        return (key_pos <= query_pos) & (key_pos >= start_s[tile])

    def off_mask(tile, blk):
        key_pos = lax.broadcasted_iota(jnp.int32, (tok, width), 0)
        return key_pos >= start_s[tile] + (me - blk) * tok

    def over_tiles(body, blk):
        def tile_body(tile, carry):
            masked = (blk == first) | (tile >= full_tiles)
            pl.when(masked)(functools.partial(body, tile, True, blk))
            pl.when(jnp.logical_not(masked))(functools.partial(body, tile, False, blk))
            return carry
        lax.fori_loop(0, tiles_prev, tile_body, 0)

    def forward_body(tile, masked, blk):
        row = start_s[tile] + (me - blk) * tok if masked else None
        forward_update(kv_heads, group, scale2, tile, q_ref, kv_ref, blk, stats, row)

    def forward_blocks(blk, carry):
        over_tiles(forward_body, blk)
        return carry

    lax.fori_loop(first, jnp.maximum(first, near_first), forward_blocks, 0)

    unit = (lax.broadcasted_iota(jnp.int32, (128, 128), 0)
            == lax.broadcasted_iota(jnp.int32, (128, 128), 1)).astype(jnp.bfloat16)

    def turned(block_t):
        return dot32(unit, block_t, NT).astype(jnp.bfloat16)

    for tile in range(tiles):
        for head in range(kv_heads):
            slot = head * tiles + tile
            total = sum_s[head][tile]
            max_s[head][tile] = max_s[head][tile] + jnp.log2(total)
            out_t = (acc_s[head][tile] / total).astype(jnp.bfloat16)
            first_col = head * group * 128
            do_t = jnp.concatenate(
                [dot_ref[first_col + member * 128:first_col + (member + 1) * 128, tile * QT:(tile + 1) * QT]
                 for member in range(group)], axis=1)
            delta_s[slot] = jnp.sum(do_t.astype(jnp.float32) * out_t.astype(jnp.float32), axis=0, keepdims=True)
            for member in range(group):
                col = first_col + member * 128
                o_ref[tile * QT:(tile + 1) * QT, col:col + 128] = turned(out_t[:, member * QT:(member + 1) * QT])

    def grads(tile, head, blk, keys, mask_fn):
        slot = head * tiles + tile
        q_tile = stack_heads(q_ref, tile, head, group)
        do_tile = stack_heads(do_ref, tile, head, group)
        k_blk = kv_ref[blk, 0:keys, k_cols(head)]
        v_blk = kv_ref[blk, 0:keys, v_cols(head)]
        scores = dot32(k_blk, q_tile, NT) * scale2
        if mask_fn is not None:
            scores = jnp.where(mask_fn(), scores, NEG_INF)
        prob = jnp.exp2(scores - max_s[head][tile])
        dprob = dot32(v_blk, do_tile, NT)
        dscore = (prob * (dprob - delta_s[slot])).astype(jnp.bfloat16)
        dv_part = dot32(prob.astype(jnp.bfloat16), do_tile, NN)
        dk_part = dot32(dscore, q_tile, NN)
        dq_part = dot32(k_blk, dscore, TN)
        return dq_part, dk_part, dv_part

    for tile in reversed(range(tiles)):
        keys = QT * (tile + 1)
        for head in range(kv_heads):
            dq_part, dk_part, dv_part = grads(tile, head, me, keys, functools.partial(diag_mask, tile, keys))
            acc_s[head][tile] = dq_part
            if tile == tiles - 1:
                grad_s[me, 0:keys, k_cols(head)] = dk_part
                grad_s[me, 0:keys, v_cols(head)] = dv_part
            else:
                grad_s[me, 0:keys, k_cols(head)] = grad_s[me, 0:keys, k_cols(head)] + dk_part
                grad_s[me, 0:keys, v_cols(head)] = grad_s[me, 0:keys, v_cols(head)] + dv_part
    grad_copy(me).start()

    def backward_body(tile, masked, blk):
        for head in range(kv_heads):
            slot = head * tiles + tile
            dq_part, dk_part, dv_part = grads(tile, head, blk, tok, functools.partial(off_mask, tile, blk) if masked else None)
            acc_s[head][tile] = acc_s[head][tile] + dq_part
            grad_s[blk, :, k_cols(head)] = grad_s[blk, :, k_cols(head)] + dk_part
            grad_s[blk, :, v_cols(head)] = grad_s[blk, :, v_cols(head)] + dv_part

    def backward_blocks(blk, carry):
        grad_s[blk] = jnp.zeros(zero_s.shape, jnp.float32)
        over_tiles(backward_body, blk)
        grad_copy(blk).start()
        return carry

    lax.fori_loop(first, me, backward_blocks, 0)

    for tile in range(tiles):
        for head in range(kv_heads):
            grad_t = (acc_s[head][tile] * scale).astype(jnp.bfloat16)
            for member in range(group):
                col = (head * group + member) * 128
                dq_ref[tile * QT:(tile + 1) * QT, col:col + 128] = turned(grad_t[:, member * QT:(member + 1) * QT])

    def wait_body(blk, carry):
        zero_copy(blk).wait()
        return carry

    lax.fori_loop(0, blocks, wait_body, 0)


def places(n):
    me = lax.axis_index('cp')
    chips = n // 2
    core = lax.rem(me, 2)
    chip = me // 2

    def at(offset, which):
        return lax.rem(chip + offset + chips, chips) * 2 + which

    return me, chips, core, chip, at


def remote(src, dst, send_sem, recv_sem, target):
    return pltpu.make_async_remote_copy(src_ref=src, dst_ref=dst, send_sem=send_sem, recv_sem=recv_sem,
                                        device_id={'cp': target}, device_id_type=pl.DeviceIdType.MESH)


def greet(targets):
    barrier = pltpu.get_barrier_semaphore()
    for target in targets:
        pl.semaphore_signal(barrier, inc=1, device_id={'cp': target}, device_id_type=pl.DeviceIdType.MESH)
    pl.semaphore_wait(barrier, len(targets))


def gather_kernel(n, kv_heads, group, scale2, seg_ref, x_ref, dy_ref, wkv_ref, wq_ref, wo_ref,
                  kv_all_ref, seg_all_ref, q_ref, do_ref, dot_ref, start_ref,
                  max0_ref, max1_ref, sum0_ref, sum1_ref, acc0_ref, acc1_ref,
                  kv_s, wq_s, wo_s, load_sem, seg_send, seg_recv, ring_send, ring_recv, pair_send, pair_recv,
                  mate_send, mate_recv):
    me, chips, core, chip, at = places(n)
    mate = at(0, 1 - core)
    tok = kv_s.shape[0]
    tiles = tok // QT
    slice_rows = tok // SLICES
    reach = chips // 2
    stats = [(max0_ref, sum0_ref, acc0_ref), (max1_ref, sum1_ref, acc1_ref)]
    load_q = pltpu.make_async_copy(wq_ref, wq_s, load_sem.at[0])
    load_o = pltpu.make_async_copy(wo_ref, wo_s, load_sem.at[1])
    load_q.start()
    load_o.start()
    kv_own = dot32(x_ref[...], wkv_ref[...], NN).astype(jnp.bfloat16)
    kv_s[...] = kv_own
    kv_all_ref[me] = kv_own
    seg_all_ref[me] = seg_ref[...]
    greet([lax.rem(me + step, n) for step in range(1, n)])

    def rows(sub):
        return pl.ds(pl.multiple_of(sub * slice_rows, slice_rows), slice_rows)

    def ring_copy(way, sub, hop):
        offset = 1 - hop if way == 0 else hop - 1
        spot = kv_all_ref.at[at(offset, core), rows(sub)]
        return remote(spot, spot, ring_send.at[way, sub, hop - 1], ring_recv.at[way, sub, hop - 1],
                      at(1 if way == 0 else -1, core))

    def pair_copy(way, sub, hop):
        spot = kv_all_ref.at[at(-hop if way == 0 else hop, core), rows(sub)]
        return remote(spot, spot, pair_send.at[way, sub, hop - 1], pair_recv.at[way, sub, hop - 1], mate)

    def seg_copy(step):
        return remote(seg_ref, seg_all_ref.at[me], seg_send.at[step - 1], seg_recv.at[step - 1], lax.rem(me + step, n))

    def own_copy():
        return remote(kv_s, kv_all_ref.at[me], mate_send.at[0], mate_recv.at[0], mate)

    for sub in range(SLICES):
        for way in range(2):
            ring_copy(way, sub, 1).start()
    own_copy().start()
    for step in range(1, n):
        seg_copy(step).start()

    pairs = wq_s.shape[0] // 2

    def project(src_ref, w_s, dst_ref, pair):
        w_pair = jnp.concatenate([w_s[2 * pair], w_s[2 * pair + 1]], axis=1)
        cols = pl.ds(pl.multiple_of(pair * 256, 256), 256)
        value = dot32(src_ref[...], w_pair, NN).astype(jnp.bfloat16)
        dst_ref[:, cols] = value
        return value

    def query_pair(pair, carry):
        project(x_ref, wq_s, q_ref, pair)
        return carry

    load_q.wait()
    lax.fori_loop(0, pairs, query_pair, 0)

    for step in range(1, n):
        seg_copy(step).wait_recv()
    seg_own = seg_ref[...]
    first_seg = jnp.min(seg_own)
    shard_index = lax.broadcasted_iota(jnp.int32, seg_all_ref.shape, 0)
    earlier = (shard_index < me) & (seg_all_ref[...] < first_seg)
    doc_start = jnp.sum(earlier.astype(jnp.int32))
    seg_wide = seg_own.astype(jnp.float32)
    columns = [jnp.broadcast_to(seg_wide[part:part + 1, :], (128, 128)).T for part in range(tok // 128)]
    for tile in range(tiles):
        count = sum(jnp.sum((column < seg_wide[tile:tile + 1, :]).astype(jnp.int32), axis=0, keepdims=True)
                    for column in columns)
        row = jnp.where(count == 0, doc_start - me * tok, count)
        start_ref[tile] = jnp.concatenate([row] * group, axis=1)

    for tile in range(tiles):
        forward_update(kv_heads, group, scale2, tile, q_ref, kv_all_ref, me, stats, start_ref[tile], QT * (tile + 1), True)
    load_o.wait()

    def tick_body(tick, carry):
        step, sub = tick // SLICES, lax.rem(tick, SLICES)
        for way in range(2):
            last = (sub < SLICES // 2) if way == 0 else (sub >= SLICES // 2)

            @pl.when((step < reach - 1) | last)
            def _():
                ring_copy(way, sub, step + 1).wait_recv()
                pair_copy(way, sub, step + 1).start()

            @pl.when((step < reach - 2) | ((step == reach - 2) & last))
            def _():
                ring_copy(way, sub, step + 2).start()

        @pl.when((step == 0) & (sub == 0))
        def _():
            own_copy().wait_recv()

        @pl.when((step > 0) & (sub == 0))
        def _():
            for piece in range(SLICES):
                pair_copy(0, piece, step).wait_recv()

        @pl.when(lax.rem(tick, reach) == 0)
        def _():
            pair = tick // reach
            value = project(dy_ref, wo_s, do_ref, pair)
            dot_ref[pl.ds(pl.multiple_of(pair * 256, 256), 256), :] = value.T

        side = sub // tiles
        near = (chip >= step) & ((step > 0) | ((core == 1) & (side == 0)))

        @pl.when(near)
        def _():
            blk = 2 * (chip - step) + side
            tile = lax.rem(sub, tiles)
            forward_update(kv_heads, group, scale2, tile, q_ref, kv_all_ref, blk, stats, start_ref[tile] + (me - blk) * tok)

        return carry

    lax.fori_loop(0, reach * SLICES, tick_body, 0)
    for way in range(2):
        for sub in range(SLICES):
            for hop in range(1, reach + 1):
                if hop < reach or (sub < SLICES // 2) == (way == 0):
                    if way == 1 or hop == reach:
                        pair_copy(way, sub, hop).wait_recv()
                    pair_copy(way, sub, hop).wait_send()
                    ring_copy(way, sub, hop).wait_send()
    own_copy().wait_send()
    for step in range(1, n):
        seg_copy(step).wait_send()


def reduce_kernel(n, scale, kv_width, dkv_ref, o_hbm, dq_hbm, x_hbm, dy_hbm, wkv_hbm, wq_ref, wo_ref,
                  y_ref, dx_ref, dwo_ref, dwq_ref, dwk_ref, dwv_ref,
                  o_ref, dq_ref, x_ref, dy_ref, wkv_ref, xt_ref, dyt_ref, xtp_ref, dytp_ref,
                  own_s, mate_s, slot1_s, stage1_s, grad_s, grad_mate_s, o_mate_s, dq_mate_s, slot2_s, stage2_s,
                  wq_s, wo_s, load_sem, block_sem, mate_send, mate_recv, ring_send, ring_recv, extra_send, extra_recv):
    me, chips, core, chip, at = places(n)
    mate = at(0, 1 - core)
    ring = (at(1, core), at(-1, core))
    tok = o_ref.shape[0]
    quarter = tok // 4
    heads, out_rows, head_dim = dwo_ref.shape
    loads = [pltpu.make_async_copy(src, dst, load_sem.at[index]) for index, (src, dst) in enumerate(
        ((o_hbm, o_ref), (dq_hbm, dq_ref), (x_hbm, x_ref), (dy_hbm, dy_ref), (wo_ref, wo_s), (wq_ref, wq_s),
         (wkv_hbm, wkv_ref)))]
    order = []
    for step in range(1, chips):
        for offset in (-step, step):
            if offset % chips not in order:
                order.append(offset % chips)
    order.append(0)
    own_loads = [pltpu.make_async_copy(dkv_ref.at[at(offset, core)], own_s.at[index], block_sem.at[index])
                 for index, offset in enumerate(order)]
    for load in own_loads:
        load.start()
    for load in loads:
        load.start()
    greet([ring[0], ring[1], mate])
    mate_copies = [remote(dkv_ref.at[at(offset, 1 - core)], mate_s.at[index], mate_send.at[index], mate_recv.at[index], mate)
                   for index, offset in enumerate(order)]
    extras = [remote(o_hbm, o_mate_s, extra_send.at[0], extra_recv.at[0], mate),
              remote(dq_hbm, dq_mate_s, extra_send.at[1], extra_recv.at[1], mate),
              remote(grad_s, grad_mate_s, extra_send.at[2], extra_recv.at[2], mate),
              remote(xt_ref, xtp_ref, extra_send.at[3], extra_recv.at[3], mate),
              remote(dyt_ref, dytp_ref, extra_send.at[4], extra_recv.at[4], mate)]
    for index, copy in enumerate(mate_copies):
        copy.start()
        if index == 3:
            extras[0].start()
            extras[1].start()

    ready = set()

    def need(position):
        if position not in ready:
            ready.add(position)
            own_loads[position].wait()
            mate_copies[position].wait_recv()

    def ring_copy(job, way, sub, step):
        slots, stage = (slot1_s, stage1_s) if job == 0 else (slot2_s, stage2_s)
        src = stage.at[way, sub] if step == 0 else slots.at[way, sub, step - 1]
        return remote(src, slots.at[way, sub, step], ring_send.at[job, way, sub, step], ring_recv.at[job, way, sub, step],
                      ring[way])

    started = []

    def send(job, way, sub, step):
        started.append(ring_copy(job, way, sub, step))
        started[-1].start()

    def contrib1(way, sub, step):
        offset = (-(1 + step) if way == 0 else 1 + step) % chips
        position = order.index(offset)
        need(position)
        span = slice((2 * way + sub) * quarter, (2 * way + sub + 1) * quarter)
        return own_s[position, span, :] + mate_s[position, span, :]

    cut = 7 * head_dim

    def contrib2(way, sub, step):
        offset = -(1 + step) if way == 0 else 1 + step
        first_row = pl.multiple_of(at(offset % chips, core) * out_rows, 32)
        take = pl.ds(first_row, out_rows)
        lhs, lhs_mate = (dyt_ref, dytp_ref) if way == 0 else (xt_ref, xtp_ref)
        rhs, rhs_mate = (o_ref, o_mate_s) if way == 0 else (dq_ref, dq_mate_s)
        if sub == 0:
            return (dot32(lhs[take, :], rhs[:, 0:cut], NN) + dot32(lhs_mate[take, :], rhs_mate[:, 0:cut], NN))
        main = dot32(lhs[take, :], rhs[:, cut:], NN) + dot32(lhs_mate[take, :], rhs_mate[:, cut:], NN)
        cols = slice(way * kv_width, (way + 1) * kv_width)
        side = dot32(xt_ref[take, :], grad_s[:, cols], NN) + dot32(xtp_ref[take, :], grad_mate_s[:, cols], NN)
        return jnp.concatenate([main, side], axis=1)

    strip = 256
    strips = y_ref.shape[1] // strip

    def rows_out(part):
        return pl.ds(pl.multiple_of(part * strip, strip), strip)

    def times_weight(src_ref, w_s, part):
        total = None
        for pair in range(heads // 2):
            w_pair = jnp.concatenate([w_s[2 * pair, rows_out(part), :], w_s[2 * pair + 1, rows_out(part), :]], axis=1)
            piece = dot32(src_ref[:, pair * 256:(pair + 1) * 256], w_pair, NT)
            total = piece if total is None else total + piece
        return total

    def y_strip(part, carry):
        y_ref[:, rows_out(part)] = times_weight(o_ref, wo_s, part).astype(jnp.bfloat16)
        return carry

    def flip_strip(part, carry):
        xt_ref[rows_out(part), :] = x_ref[:, rows_out(part)].T
        dyt_ref[rows_out(part), :] = dy_ref[:, rows_out(part)].T
        return carry

    def dx_strip(part, carry):
        wide = times_weight(dq_ref, wq_s, part) + dot32(grad_s[...], wkv_ref[rows_out(part), :], NT)
        dx_ref[:, rows_out(part)] = wide.astype(jnp.bfloat16)
        return carry

    steps = chips - 1
    both = [(sub, way) for sub in range(2) for way in range(2)]
    for sub, way in both:
        stage1_s[way, sub] = contrib1(way, sub, 0)
        send(0, way, sub, 0)
    for load in loads:
        load.wait()
    for step in range(steps):
        if step == 0:
            lax.fori_loop(0, strips, y_strip, 0)
        if step == 1:
            lax.fori_loop(0, strips, flip_strip, 0)
        if step == 4:
            extras[3].start()
            extras[4].start()
        if step == steps - 1:
            for index in (0, 1, 3, 4):
                extras[index].wait_recv()
            for way in range(2):
                stage2_s[way, 0] = contrib2(way, 0, 0)
                send(1, way, 0, 0)
        for sub, way in both:
            part = contrib1(way, sub, step + 1)
            ring_copy(0, way, sub, step).wait_recv()
            if step < steps - 1:
                slot1_s[way, sub, step] = slot1_s[way, sub, step] + part
                send(0, way, sub, step + 1)
            else:
                span = slice((2 * way + sub) * quarter, (2 * way + sub + 1) * quarter)
                total = slot1_s[way, sub, step] + part
                grad_s[span, 0:kv_width] = (total[:, 0:kv_width] * scale).astype(jnp.bfloat16)
                grad_s[span, kv_width:] = total[:, kv_width:].astype(jnp.bfloat16)
    extras[2].start()
    extras[2].wait_recv()
    for way in range(2):
        stage2_s[way, 1] = contrib2(way, 1, 0)
        send(1, way, 1, 0)
    for step in range(steps):
        if step == 0:
            lax.fori_loop(0, strips, dx_strip, 0)
        for sub, way in both:
            part = contrib2(way, sub, step + 1)
            ring_copy(1, way, sub, step).wait_recv()
            if step < steps - 1:
                slot2_s[way, sub, step] = slot2_s[way, sub, step] + part
                send(1, way, sub, step + 1)
            else:
                total = slot2_s[way, sub, step] + part
                out_ref = dwo_ref if way == 0 else dwq_ref
                base = 0 if sub == 0 else cut // head_dim
                for index in range(cut // head_dim if sub == 0 else heads - cut // head_dim):
                    out_ref[base + index] = total[:, index * head_dim:(index + 1) * head_dim]
                if sub == 1:
                    side_ref = dwk_ref if way == 0 else dwv_ref
                    for index in range(kv_width // head_dim):
                        base = heads * head_dim - cut + index * head_dim
                        side_ref[:, index, :] = total[:, base:base + head_dim]
    for copy in started + mate_copies + extras:
        copy.wait_send()


VMEM_SPEC = pl.BlockSpec(memory_space=pltpu.VMEM)
ANY_SPEC = pl.BlockSpec(memory_space=pl.ANY)
VMEM_LIMIT = 60 * 1024 * 1024
REDUCE_LIMIT = 67043328


def solution(mesh):
    group_count = mesh.shape['cp']
    row_spec = P(('dp', 'cp'), None)
    tok_spec = P(('dp', 'cp'))
    weight_spec = P(None, None, None)
    grad_spec = P(('dp', 'cp'), None, None)

    def local_step(x_act, seg_ids, w_q, w_k, w_v, w_o, dy_act):
        tok = x_act.shape[0]
        model_dim, q_heads, head_dim = w_q.shape
        kv_heads = w_k.shape[1]
        group = q_heads // kv_heads
        q_width = q_heads * head_dim
        kv_width = kv_heads * head_dim
        tiles = tok // QT
        scale = head_dim ** -0.5
        bf16 = jnp.bfloat16

        w_kv = jnp.concatenate([w_k.reshape(model_dim, kv_width), w_v.reshape(model_dim, kv_width)], axis=1)
        seg_rows = seg_ids.reshape(tok // 128, 128)
        wq_heads = w_q.transpose(1, 0, 2)
        wo_heads = w_o.transpose(1, 0, 2)

        slots = kv_heads * tiles
        width = group * QT
        chips = group_count // 2
        reach = chips // 2
        dma = pltpu.SemaphoreType.DMA
        f32 = jnp.float32
        shape = jax.ShapeDtypeStruct
        flat = shape((tok, q_width), bf16)
        row32 = shape((tiles, 1, width), f32)
        wide32 = shape((tiles, head_dim, width), f32)
        kv_all, seg_all, q_loc, do_loc, do_turned, *kept = pl.pallas_call(
            functools.partial(gather_kernel, group_count, kv_heads, group, scale * LOG2E),
            out_shape=(shape((group_count, tok, 2 * kv_width), bf16), shape((group_count, tok // 128, 128), jnp.int32),
                       flat, flat, shape((q_width, tok), bf16), shape((tiles, 1, width), jnp.int32),
                       row32, row32, row32, row32, wide32, wide32),
            in_specs=[VMEM_SPEC] * 4 + [ANY_SPEC] * 2,
            out_specs=(VMEM_SPEC,) * 12,
            scratch_shapes=[pltpu.VMEM((tok, 2 * kv_width), bf16), pltpu.VMEM((q_heads, model_dim, head_dim), bf16),
                            pltpu.VMEM((q_heads, model_dim, head_dim), bf16),
                            dma((2,)), dma((group_count - 1,)), dma((group_count - 1,)),
                            dma((2, SLICES, reach)), dma((2, SLICES, reach)), dma((2, SLICES, reach)), dma((2, SLICES, reach)), dma((1,)), dma((1,))],
            compiler_params=pltpu.CompilerParams(collective_id=0, has_side_effects=True, vmem_limit_bytes=VMEM_LIMIT),
            cost_estimate=pl.CostEstimate(flops=8 * tok * model_dim * q_width, bytes_accessed=2**24, transcendentals=0),
            name='gather_keys',
        )(seg_rows, x_act, dy_act, w_kv, wq_heads, wo_heads)

        o_loc, dq_loc, dkv_all = pl.pallas_call(
            functools.partial(attention_kernel, kv_heads, group, scale),
            out_shape=(flat, flat, shape((group_count, tok, 2 * kv_width), f32)),
            in_specs=[VMEM_SPEC] * 13,
            out_specs=(VMEM_SPEC, VMEM_SPEC, ANY_SPEC),
            scratch_shapes=[pltpu.VMEM((tiles, 1, width), f32)] * 4
                           + [pltpu.VMEM((slots, 1, width), f32)] + [pltpu.VMEM((tiles, head_dim, width), f32)] * 2
                           + [pltpu.VMEM((group_count, tok, 2 * kv_width), f32),
                            pltpu.VMEM((tok, 2 * kv_width), f32), dma((group_count,))],
            compiler_params=pltpu.CompilerParams(vmem_limit_bytes=VMEM_LIMIT),
            cost_estimate=pl.CostEstimate(flops=16 * 14 * tok * tok * q_width, bytes_accessed=2**25, transcendentals=0),
            name='attend',
        )(seg_rows, seg_all, q_loc, do_loc, do_turned, kv_all, *kept)

        out_rows = model_dim // group_count
        blk = (tok, 2 * kv_width)
        cols2 = (q_width + kv_width) // 2
        steps = chips - 1
        head_grad = shape((q_heads, out_rows, head_dim), f32)
        y_out, dx_out, dwo, dwq, dwk, dwv = pl.pallas_call(
            functools.partial(reduce_kernel, group_count, scale, kv_width),
            out_shape=(shape((tok, model_dim), bf16), shape((tok, model_dim), bf16), head_grad, head_grad,
                       shape((out_rows, kv_heads, head_dim), f32), shape((out_rows, kv_heads, head_dim), f32)),
            in_specs=[ANY_SPEC] * 8,
            out_specs=(VMEM_SPEC,) * 6,
            scratch_shapes=[pltpu.VMEM((tok, q_width), bf16), pltpu.VMEM((tok, q_width), bf16),
                            pltpu.VMEM((tok, model_dim), bf16), pltpu.VMEM((tok, model_dim), bf16),
                            pltpu.VMEM((model_dim, 2 * kv_width), bf16),
                            pltpu.VMEM((model_dim, tok), bf16), pltpu.VMEM((model_dim, tok), bf16),
                            pltpu.VMEM((model_dim, tok), bf16), pltpu.VMEM((model_dim, tok), bf16),
                            pltpu.VMEM((chips,) + blk, f32), pltpu.VMEM((chips,) + blk, f32),
                            pltpu.VMEM((2, 2, steps, tok // 4, 2 * kv_width), f32), pltpu.VMEM((2, 2, tok // 4, 2 * kv_width), f32),
                            pltpu.VMEM(blk, bf16), pltpu.VMEM(blk, bf16),
                            pltpu.VMEM((tok, q_width), bf16), pltpu.VMEM((tok, q_width), bf16),
                            pltpu.VMEM((2, 2, steps, out_rows, cols2), f32), pltpu.VMEM((2, 2, out_rows, cols2), f32),
                            pltpu.VMEM((q_heads, model_dim, head_dim), bf16), pltpu.VMEM((q_heads, model_dim, head_dim), bf16),
                            dma((7,)), dma((chips,)), dma((chips,)), dma((chips,)),
                            dma((2, 2, 2, steps)), dma((2, 2, 2, steps)), dma((5,)), dma((5,))],
            compiler_params=pltpu.CompilerParams(collective_id=1, has_side_effects=True, vmem_limit_bytes=REDUCE_LIMIT),
            cost_estimate=pl.CostEstimate(flops=16 * tok * model_dim * q_width, bytes_accessed=2**25, transcendentals=0),
            name='reduce_grads',
        )(dkv_all, o_loc, dq_loc, x_act, dy_act, w_kv, wq_heads, wo_heads)
        return y_out, dx_out, dwq.transpose(1, 0, 2), dwk, dwv, dwo.transpose(1, 0, 2)

    return jax.shard_map(local_step, mesh=mesh,
                         in_specs=(row_spec, tok_spec, weight_spec, weight_spec, weight_spec, weight_spec, row_spec),
                         out_specs=(row_spec, row_spec, grad_spec, grad_spec, grad_spec, grad_spec),
                         check_vma=False)
```

```python
import functools

import jax
import jax.numpy as jnp
from jax import lax
from jax.experimental import pallas as pl
from jax.experimental.pallas import tpu as pltpu
from jax.sharding import PartitionSpec as P

QT = 128
SLICES = 6
LOG2E = 1.4426950408889634
NEG_INF = float('-inf')
NT = (((1,), (1,)), ((), ()))
TN = (((0,), (0,)), ((), ()))
NN = (((1,), (0,)), ((), ()))


def dot32(left_arg, right_arg, dims):
    return lax.dot_general(left_arg, right_arg, dims, preferred_element_type=jnp.float32)


def stack_heads(ref, tile, head, group):
    rows = pl.ds(pl.multiple_of(tile * QT, QT), QT)
    return jnp.concatenate(
        [ref[rows, (head * group + member) * 128:(head * group + member + 1) * 128] for member in range(group)], axis=0)


def member_rows(ref, tile, head, group, chunk):
    rows = pl.ds(pl.multiple_of(tile * QT, QT), QT)
    first = (head * group + 2 * chunk) * 128
    return jnp.concatenate([ref[rows, first:first + 128], ref[rows, first + 128:first + 256]], axis=0)


def forward_update(kv_heads, group, scale2, tile, q_ref, kv_ref, blk, stats, mask_row, keys=None, diag=False):
    keys = kv_ref.shape[1] if keys is None else keys
    chains = [(head, chunk) for chunk in range(group // 2) for head in range(kv_heads)]
    k_blks = [kv_ref[blk, 0:keys, head * 128:(head + 1) * 128] for head in range(kv_heads)]
    v_turned = [kv_ref[blk, 0:keys, (kv_heads + head) * 128:(kv_heads + head + 1) * 128].T for head in range(kv_heads)]
    old = [None if diag else (stats[head][0][tile], stats[head][1][tile]) for head in range(kv_heads)]
    new_rows = [([], []) for head in range(kv_heads)]

    def score(chain):
        head, chunk = chain
        return dot32(k_blks[head], member_rows(q_ref, tile, head, group, chunk), NT)

    pending = [score(chain) for chain in chains[:6]]
    for index, (head, chunk) in enumerate(chains):
        scores = pending.pop(0)
        if index + 6 < len(chains):
            pending.append(score(chains[index + 6]))
        cols = slice(chunk * 256, (chunk + 1) * 256)
        if mask_row is not None:
            key_pos = lax.broadcasted_iota(jnp.int32, (keys, 256), 0)
            allowed = key_pos >= mask_row[:, cols]
            if diag:
                query_pos = lax.rem(lax.broadcasted_iota(jnp.int32, (1, 256), 1), QT) + tile * QT
                allowed = allowed & (key_pos <= query_pos)
            scores = jnp.where(allowed, scores, NEG_INF)
        new_max = jnp.max(scores, axis=0, keepdims=True) * scale2
        if not diag:
            old_max = old[head][0][:, cols]
            new_max = jnp.maximum(old_max, new_max)
        weights = jnp.exp2(scores * scale2 - new_max)
        total = jnp.sum(weights, axis=0, keepdims=True)
        part = dot32(v_turned[head], weights.astype(jnp.bfloat16), NN)
        acc = stats[head][2]
        if diag:
            acc[tile, :, cols] = part
        else:
            factor = jnp.exp2(old_max - new_max)
            total = old[head][1][:, cols] * factor + total
            acc[tile, :, cols] = acc[tile, :, cols] * factor + part
        new_rows[head][0].append(new_max)
        new_rows[head][1].append(total)
    for head in range(kv_heads):
        stats[head][0][tile] = jnp.concatenate(new_rows[head][0], axis=1)
        stats[head][1][tile] = jnp.concatenate(new_rows[head][1], axis=1)


def attention_kernel(kv_heads, group, scale, seg_ref, seg_all_ref, q_ref, do_ref, dot_ref, kv_hbm, start_s,
                     max0_ref, max1_ref, sum0_ref, sum1_ref, acc0_ref, acc1_ref,
                     o_ref, dq_ref, dkv_ref, max0_s, max1_s, sum0_s, sum1_s, delta_s, acc0_s, acc1_s,
                     grad_s, zero_s, out_sem,
                     kv_ref, in_sem):
    tok = q_ref.shape[0]
    blocks = kv_ref.shape[0]
    tiles = tok // QT
    width = group * QT
    scale2 = scale * LOG2E
    max_s, sum_s, acc_s = (max0_s, max1_s), (sum0_s, sum1_s), (acc0_s, acc1_s)
    stats = [(max_s[head], sum_s[head], acc_s[head]) for head in range(kv_heads)]
    me = lax.axis_index('cp')
    near_first = jnp.maximum(2 * (me // 2 - (blocks // 4 - 1)), 0)
    for kept_ref, kept_s in ((max0_ref, max0_s), (max1_ref, max1_s), (sum0_ref, sum0_s), (sum1_ref, sum1_s),
                             (acc0_ref, acc0_s), (acc1_ref, acc1_s)):
        kept_s[...] = kept_ref[...]
    zero_s[...] = jnp.zeros(zero_s.shape, jnp.float32)

    seg_own = seg_ref[...]
    first_seg = jnp.min(seg_own)
    head_count = jnp.sum((seg_own == first_seg).astype(jnp.int32))
    shard_index = lax.broadcasted_iota(jnp.int32, seg_all_ref.shape, 0)
    earlier = (shard_index < me) & (seg_all_ref[...] < first_seg)
    doc_start = jnp.sum(earlier.astype(jnp.int32))
    first = doc_start // tok
    has_prev = doc_start < me * tok
    tiles_prev = jnp.where(has_prev, (head_count + QT - 1) // QT, 0)
    full_tiles = head_count // QT

    def key_copy(blk):
        return pltpu.make_async_copy(kv_hbm.at[blk], kv_ref.at[blk], in_sem.at[blk])

    def key_body(blk, carry):
        key_copy(blk).start()
        return carry

    lax.fori_loop(first, me + 1, key_body, 0)

    def zero_copy(blk):
        return pltpu.make_async_copy(zero_s, dkv_ref.at[blk], out_sem.at[blk])

    def grad_copy(blk):
        return pltpu.make_async_copy(grad_s.at[blk], dkv_ref.at[blk], out_sem.at[blk])

    def clear_body(blk, carry):
        zero_copy(blk).start()
        return carry

    lax.fori_loop(0, first, clear_body, 0)
    lax.fori_loop(me + 1, blocks, clear_body, 0)

    def k_cols(head):
        return slice(head * 128, (head + 1) * 128)

    def v_cols(head):
        return slice((kv_heads + head) * 128, (kv_heads + head + 1) * 128)

    def diag_mask(tile, keys):
        key_pos = lax.broadcasted_iota(jnp.int32, (keys, width), 0)
        query_pos = lax.rem(lax.broadcasted_iota(jnp.int32, (1, width), 1), QT) + tile * QT
        return (key_pos <= query_pos) & (key_pos >= start_s[tile])

    def off_mask(tile, blk):
        key_pos = lax.broadcasted_iota(jnp.int32, (tok, width), 0)
        return key_pos >= start_s[tile] + (me - blk) * tok

    def over_tiles(body, blk):
        def tile_body(tile, carry):
            masked = (blk == first) | (tile >= full_tiles)
            pl.when(masked)(functools.partial(body, tile, True, blk))
            pl.when(jnp.logical_not(masked))(functools.partial(body, tile, False, blk))
            return carry
        lax.fori_loop(0, tiles_prev, tile_body, 0)

    def forward_body(tile, masked, blk):
        row = start_s[tile] + (me - blk) * tok if masked else None
        forward_update(kv_heads, group, scale2, tile, q_ref, kv_ref, blk, stats, row)

    def forward_blocks(blk, carry):
        key_copy(blk).wait()
        over_tiles(forward_body, blk)
        return carry

    lax.fori_loop(first, jnp.maximum(first, near_first), forward_blocks, 0)

    unit = (lax.broadcasted_iota(jnp.int32, (128, 128), 0)
            == lax.broadcasted_iota(jnp.int32, (128, 128), 1)).astype(jnp.bfloat16)

    def turned(block_t):
        return dot32(unit, block_t, NT).astype(jnp.bfloat16)

    for tile in range(tiles):
        for head in range(kv_heads):
            slot = head * tiles + tile
            total = sum_s[head][tile]
            max_s[head][tile] = max_s[head][tile] + jnp.log2(total)
            out_t = (acc_s[head][tile] / total).astype(jnp.bfloat16)
            first_col = head * group * 128
            do_t = jnp.concatenate(
                [dot_ref[first_col + member * 128:first_col + (member + 1) * 128, tile * QT:(tile + 1) * QT]
                 for member in range(group)], axis=1)
            delta_s[slot] = jnp.sum(do_t.astype(jnp.float32) * out_t.astype(jnp.float32), axis=0, keepdims=True)
            for member in range(group):
                col = first_col + member * 128
                o_ref[tile * QT:(tile + 1) * QT, col:col + 128] = turned(out_t[:, member * QT:(member + 1) * QT])

    def grads(tile, head, blk, keys, mask_fn):
        slot = head * tiles + tile
        q_tile = stack_heads(q_ref, tile, head, group)
        do_tile = stack_heads(do_ref, tile, head, group)
        k_blk = kv_ref[blk, 0:keys, k_cols(head)]
        v_blk = kv_ref[blk, 0:keys, v_cols(head)]
        scores = dot32(k_blk, q_tile, NT) * scale2
        if mask_fn is not None:
            scores = jnp.where(mask_fn(), scores, NEG_INF)
        prob = jnp.exp2(scores - max_s[head][tile])
        dprob = dot32(v_blk, do_tile, NT)
        dscore = (prob * (dprob - delta_s[slot])).astype(jnp.bfloat16)
        dv_part = dot32(prob.astype(jnp.bfloat16), do_tile, NN)
        dk_part = dot32(dscore, q_tile, NN)
        dq_part = dot32(k_blk, dscore, TN)
        return dq_part, dk_part, dv_part

    key_copy(me).wait()
    for tile in reversed(range(tiles)):
        keys = QT * (tile + 1)
        for head in range(kv_heads):
            dq_part, dk_part, dv_part = grads(tile, head, me, keys, functools.partial(diag_mask, tile, keys))
            acc_s[head][tile] = dq_part
            if tile == tiles - 1:
                grad_s[me, 0:keys, k_cols(head)] = dk_part
                grad_s[me, 0:keys, v_cols(head)] = dv_part
            else:
                grad_s[me, 0:keys, k_cols(head)] = grad_s[me, 0:keys, k_cols(head)] + dk_part
                grad_s[me, 0:keys, v_cols(head)] = grad_s[me, 0:keys, v_cols(head)] + dv_part
    grad_copy(me).start()

    def backward_body(tile, masked, blk):
        for head in range(kv_heads):
            slot = head * tiles + tile
            dq_part, dk_part, dv_part = grads(tile, head, blk, tok, functools.partial(off_mask, tile, blk) if masked else None)
            acc_s[head][tile] = acc_s[head][tile] + dq_part
            grad_s[blk, :, k_cols(head)] = grad_s[blk, :, k_cols(head)] + dk_part
            grad_s[blk, :, v_cols(head)] = grad_s[blk, :, v_cols(head)] + dv_part

    def backward_blocks(blk, carry):
        pl.when(blk >= near_first)(lambda: key_copy(blk).wait())
        grad_s[blk] = jnp.zeros(zero_s.shape, jnp.float32)
        over_tiles(backward_body, blk)
        grad_copy(blk).start()
        return carry

    lax.fori_loop(first, me, backward_blocks, 0)

    for tile in range(tiles):
        for head in range(kv_heads):
            grad_t = (acc_s[head][tile] * scale).astype(jnp.bfloat16)
            for member in range(group):
                col = (head * group + member) * 128
                dq_ref[tile * QT:(tile + 1) * QT, col:col + 128] = turned(grad_t[:, member * QT:(member + 1) * QT])

    def wait_body(blk, carry):
        zero_copy(blk).wait()
        return carry

    lax.fori_loop(0, blocks, wait_body, 0)


def places(n):
    me = lax.axis_index('cp')
    chips = n // 2
    core = lax.rem(me, 2)
    chip = me // 2

    def at(offset, which):
        return lax.rem(chip + offset + chips, chips) * 2 + which

    return me, chips, core, chip, at


def remote(src, dst, send_sem, recv_sem, target):
    return pltpu.make_async_remote_copy(src_ref=src, dst_ref=dst, send_sem=send_sem, recv_sem=recv_sem,
                                        device_id={'cp': target}, device_id_type=pl.DeviceIdType.MESH)


def greet(targets):
    barrier = pltpu.get_barrier_semaphore()
    for target in targets:
        pl.semaphore_signal(barrier, inc=1, device_id={'cp': target}, device_id_type=pl.DeviceIdType.MESH)
    pl.semaphore_wait(barrier, len(targets))


def gather_kernel(n, kv_heads, group, scale2, seg_ref, x_ref, dy_ref, wkv_ref, wq_ref, wo_ref,
                  kv_out, seg_all_ref, q_out, do_out, dot_out, start_ref,
                  max0_ref, max1_ref, sum0_ref, sum1_ref, acc0_ref, acc1_ref,
                  kv_all_ref, q_ref, do_ref, dot_ref, flat_sem, block_sem, kv_s, wq_s, wo_s, load_sem, seg_send, seg_recv, ring_send, ring_recv, pair_send, pair_recv,
                  mate_send, mate_recv):
    me, chips, core, chip, at = places(n)
    mate = at(0, 1 - core)
    tok = kv_s.shape[0]
    tiles = tok // QT
    slice_rows = tok // SLICES
    reach = chips // 2
    stats = [(max0_ref, sum0_ref, acc0_ref), (max1_ref, sum1_ref, acc1_ref)]
    load_q = pltpu.make_async_copy(wq_ref, wq_s, load_sem.at[0])
    load_o = pltpu.make_async_copy(wo_ref, wo_s, load_sem.at[1])
    load_q.start()
    load_o.start()
    kv_own = dot32(x_ref[...], wkv_ref[...], NN).astype(jnp.bfloat16)
    kv_s[...] = kv_own
    kv_all_ref[me] = kv_own
    seg_all_ref[me] = seg_ref[...]
    greet([lax.rem(me + step, n) for step in range(1, n)])

    flat_outs = [pltpu.make_async_copy(src, dst, flat_sem.at[index]) for index, (src, dst) in enumerate(
        ((q_ref, q_out), (do_ref, do_out), (dot_ref, dot_out)))]

    def block_out(blk):
        return pltpu.make_async_copy(kv_all_ref.at[blk], kv_out.at[blk], block_sem.at[blk])

    def rows(sub):
        return pl.ds(pl.multiple_of(sub * slice_rows, slice_rows), slice_rows)

    def ring_copy(way, sub, hop):
        offset = 1 - hop if way == 0 else hop - 1
        spot = kv_all_ref.at[at(offset, core), rows(sub)]
        return remote(spot, spot, ring_send.at[way, sub, hop - 1], ring_recv.at[way, sub, hop - 1],
                      at(1 if way == 0 else -1, core))

    def pair_copy(way, sub, hop):
        spot = kv_all_ref.at[at(-hop if way == 0 else hop, core), rows(sub)]
        return remote(spot, spot, pair_send.at[way, sub, hop - 1], pair_recv.at[way, sub, hop - 1], mate)

    def seg_copy(step):
        return remote(seg_ref, seg_all_ref.at[me], seg_send.at[step - 1], seg_recv.at[step - 1], lax.rem(me + step, n))

    def own_copy():
        return remote(kv_s, kv_all_ref.at[me], mate_send.at[0], mate_recv.at[0], mate)

    for sub in range(SLICES):
        for way in range(2):
            ring_copy(way, sub, 1).start()
    own_copy().start()
    for step in range(1, n):
        seg_copy(step).start()

    pairs = wq_s.shape[0] // 2

    def project(src_ref, w_s, dst_ref, pair):
        w_pair = jnp.concatenate([w_s[2 * pair], w_s[2 * pair + 1]], axis=1)
        cols = pl.ds(pl.multiple_of(pair * 256, 256), 256)
        value = dot32(src_ref[...], w_pair, NN).astype(jnp.bfloat16)
        dst_ref[:, cols] = value
        return value

    def query_pair(pair, carry):
        project(x_ref, wq_s, q_ref, pair)
        return carry

    load_q.wait()
    lax.fori_loop(0, pairs, query_pair, 0)

    for step in range(1, n):
        seg_copy(step).wait_recv()
    seg_own = seg_ref[...]
    first_seg = jnp.min(seg_own)
    shard_index = lax.broadcasted_iota(jnp.int32, seg_all_ref.shape, 0)
    earlier = (shard_index < me) & (seg_all_ref[...] < first_seg)
    doc_start = jnp.sum(earlier.astype(jnp.int32))
    seg_wide = seg_own.astype(jnp.float32)
    columns = [jnp.broadcast_to(seg_wide[part:part + 1, :], (128, 128)).T for part in range(tok // 128)]
    for tile in range(tiles):
        count = sum(jnp.sum((column < seg_wide[tile:tile + 1, :]).astype(jnp.int32), axis=0, keepdims=True)
                    for column in columns)
        row = jnp.where(count == 0, doc_start - me * tok, count)
        start_ref[tile] = jnp.concatenate([row] * group, axis=1)

    for tile in range(tiles):
        forward_update(kv_heads, group, scale2, tile, q_ref, kv_all_ref, me, stats, start_ref[tile], QT * (tile + 1), True)
    load_o.wait()
    flat_outs[0].start()

    def tick_body(tick, carry):
        step, sub = tick // SLICES, lax.rem(tick, SLICES)
        for way in range(2):
            last = (sub < SLICES // 2) if way == 0 else (sub >= SLICES // 2)

            @pl.when((step < reach - 1) | last)
            def _():
                ring_copy(way, sub, step + 1).wait_recv()
                pair_copy(way, sub, step + 1).start()

            @pl.when((step < reach - 2) | ((step == reach - 2) & last))
            def _():
                ring_copy(way, sub, step + 2).start()

        @pl.when((step == 0) & (sub == 0))
        def _():
            own_copy().wait_recv()

        @pl.when((step > 0) & (sub == 0))
        def _():
            for piece in range(SLICES):
                pair_copy(0, piece, step).wait_recv()

        @pl.when(sub == 0)
        def _():
            for which in range(2):
                block_out(at(-step, which)).start()

        @pl.when(lax.rem(tick, reach) == 0)
        def _():
            pair = tick // reach
            value = project(dy_ref, wo_s, do_ref, pair)
            dot_ref[pl.ds(pl.multiple_of(pair * 256, 256), 256), :] = value.T

        side = sub // tiles
        near = (chip >= step) & ((step > 0) | ((core == 1) & (side == 0)))

        @pl.when(near)
        def _():
            blk = 2 * (chip - step) + side
            tile = lax.rem(sub, tiles)
            forward_update(kv_heads, group, scale2, tile, q_ref, kv_all_ref, blk, stats, start_ref[tile] + (me - blk) * tok)

        return carry

    lax.fori_loop(0, reach * SLICES, tick_body, 0)
    flat_outs[1].start()
    flat_outs[2].start()
    for way in range(2):
        for sub in range(SLICES):
            for hop in range(1, reach + 1):
                if hop < reach or (sub < SLICES // 2) == (way == 0):
                    if way == 1 or hop == reach:
                        pair_copy(way, sub, hop).wait_recv()
                    pair_copy(way, sub, hop).wait_send()
                    ring_copy(way, sub, hop).wait_send()
    for offset in range(1, chips - reach + 1):
        for which in range(2):
            block_out(at(offset, which)).start()
    own_copy().wait_send()
    for step in range(1, n):
        seg_copy(step).wait_send()
    for copy in flat_outs:
        copy.wait()
    for blk in range(n):
        block_out(blk).wait()


def reduce_kernel(n, scale, kv_width, dkv_ref, o_hbm, dq_hbm, x_hbm, dy_hbm, wkv_hbm, wq_ref, wo_ref,
                  y_ref, dx_ref, dwo_ref, dwq_ref, dwk_ref, dwv_ref,
                  o_ref, dq_ref, x_ref, dy_ref, wkv_ref, xt_ref, dyt_ref, xtp_ref, dytp_ref,
                  own_s, mate_s, slot1_s, stage1_s, grad_s, grad_mate_s, o_mate_s, dq_mate_s, slot2_s, stage2_s,
                  wq_s, wo_s, load_sem, block_sem, mate_send, mate_recv, ring_send, ring_recv, extra_send, extra_recv):
    me, chips, core, chip, at = places(n)
    mate = at(0, 1 - core)
    ring = (at(1, core), at(-1, core))
    tok = o_ref.shape[0]
    quarter = tok // 4
    heads, out_rows, head_dim = dwo_ref.shape
    loads = [pltpu.make_async_copy(src, dst, load_sem.at[index]) for index, (src, dst) in enumerate(
        ((o_hbm, o_ref), (dq_hbm, dq_ref), (x_hbm, x_ref), (dy_hbm, dy_ref), (wo_ref, wo_s), (wq_ref, wq_s),
         (wkv_hbm, wkv_ref)))]
    order = []
    for step in range(1, chips):
        for offset in (-step, step):
            if offset % chips not in order:
                order.append(offset % chips)
    order.append(0)
    own_loads = [pltpu.make_async_copy(dkv_ref.at[at(offset, core)], own_s.at[index], block_sem.at[index])
                 for index, offset in enumerate(order)]
    for load in own_loads:
        load.start()
    for load in loads:
        load.start()
    greet([ring[0], ring[1], mate])
    mate_copies = [remote(dkv_ref.at[at(offset, 1 - core)], mate_s.at[index], mate_send.at[index], mate_recv.at[index], mate)
                   for index, offset in enumerate(order)]
    extras = [remote(o_hbm, o_mate_s, extra_send.at[0], extra_recv.at[0], mate),
              remote(dq_hbm, dq_mate_s, extra_send.at[1], extra_recv.at[1], mate),
              remote(grad_s, grad_mate_s, extra_send.at[2], extra_recv.at[2], mate),
              remote(xt_ref, xtp_ref, extra_send.at[3], extra_recv.at[3], mate),
              remote(dyt_ref, dytp_ref, extra_send.at[4], extra_recv.at[4], mate)]
    for index, copy in enumerate(mate_copies):
        copy.start()
        if index == 3:
            extras[0].start()
            extras[1].start()

    ready = set()

    def need(position):
        if position not in ready:
            ready.add(position)
            own_loads[position].wait()
            mate_copies[position].wait_recv()

    def ring_copy(job, way, sub, step):
        slots, stage = (slot1_s, stage1_s) if job == 0 else (slot2_s, stage2_s)
        src = stage.at[way, sub] if step == 0 else slots.at[way, sub, step - 1]
        return remote(src, slots.at[way, sub, step], ring_send.at[job, way, sub, step], ring_recv.at[job, way, sub, step],
                      ring[way])

    started = []

    def send(job, way, sub, step):
        started.append(ring_copy(job, way, sub, step))
        started[-1].start()

    def contrib1(way, sub, step):
        offset = (-(1 + step) if way == 0 else 1 + step) % chips
        position = order.index(offset)
        need(position)
        span = slice((2 * way + sub) * quarter, (2 * way + sub + 1) * quarter)
        return own_s[position, span, :] + mate_s[position, span, :]

    cut = 7 * head_dim

    def contrib2(way, sub, step):
        offset = -(1 + step) if way == 0 else 1 + step
        first_row = pl.multiple_of(at(offset % chips, core) * out_rows, 32)
        take = pl.ds(first_row, out_rows)
        lhs, lhs_mate = (dyt_ref, dytp_ref) if way == 0 else (xt_ref, xtp_ref)
        rhs, rhs_mate = (o_ref, o_mate_s) if way == 0 else (dq_ref, dq_mate_s)
        if sub == 0:
            return (dot32(lhs[take, :], rhs[:, 0:cut], NN) + dot32(lhs_mate[take, :], rhs_mate[:, 0:cut], NN))
        main = dot32(lhs[take, :], rhs[:, cut:], NN) + dot32(lhs_mate[take, :], rhs_mate[:, cut:], NN)
        cols = slice(way * kv_width, (way + 1) * kv_width)
        side = dot32(xt_ref[take, :], grad_s[:, cols], NN) + dot32(xtp_ref[take, :], grad_mate_s[:, cols], NN)
        return jnp.concatenate([main, side], axis=1)

    strip = 256
    strips = y_ref.shape[1] // strip

    def rows_out(part):
        return pl.ds(pl.multiple_of(part * strip, strip), strip)

    def times_weight(src_ref, w_s, part):
        total = None
        for pair in range(heads // 2):
            w_pair = jnp.concatenate([w_s[2 * pair, rows_out(part), :], w_s[2 * pair + 1, rows_out(part), :]], axis=1)
            piece = dot32(src_ref[:, pair * 256:(pair + 1) * 256], w_pair, NT)
            total = piece if total is None else total + piece
        return total

    def y_strip(part, carry):
        y_ref[:, rows_out(part)] = times_weight(o_ref, wo_s, part).astype(jnp.bfloat16)
        return carry

    def flip_strip(part, carry):
        xt_ref[rows_out(part), :] = x_ref[:, rows_out(part)].T
        dyt_ref[rows_out(part), :] = dy_ref[:, rows_out(part)].T
        return carry

    def dx_strip(part, carry):
        wide = times_weight(dq_ref, wq_s, part) + dot32(grad_s[...], wkv_ref[rows_out(part), :], NT)
        dx_ref[:, rows_out(part)] = wide.astype(jnp.bfloat16)
        return carry

    steps = chips - 1
    both = [(sub, way) for sub in range(2) for way in range(2)]
    for sub, way in both:
        stage1_s[way, sub] = contrib1(way, sub, 0)
        send(0, way, sub, 0)
    for load in loads:
        load.wait()
    for step in range(steps):
        if step == 0:
            lax.fori_loop(0, strips, y_strip, 0)
        if step == 1:
            lax.fori_loop(0, strips, flip_strip, 0)
        if step == 4:
            extras[3].start()
            extras[4].start()
        if step == steps - 1:
            for index in (0, 1, 3, 4):
                extras[index].wait_recv()
            for way in range(2):
                stage2_s[way, 0] = contrib2(way, 0, 0)
                send(1, way, 0, 0)
        for sub, way in both:
            part = contrib1(way, sub, step + 1)
            ring_copy(0, way, sub, step).wait_recv()
            if step < steps - 1:
                slot1_s[way, sub, step] = slot1_s[way, sub, step] + part
                send(0, way, sub, step + 1)
            else:
                span = slice((2 * way + sub) * quarter, (2 * way + sub + 1) * quarter)
                total = slot1_s[way, sub, step] + part
                grad_s[span, 0:kv_width] = (total[:, 0:kv_width] * scale).astype(jnp.bfloat16)
                grad_s[span, kv_width:] = total[:, kv_width:].astype(jnp.bfloat16)
    extras[2].start()
    extras[2].wait_recv()
    for way in range(2):
        stage2_s[way, 1] = contrib2(way, 1, 0)
        send(1, way, 1, 0)
    for step in range(steps):
        if step == 0:
            lax.fori_loop(0, strips, dx_strip, 0)
        for sub, way in both:
            part = contrib2(way, sub, step + 1)
            ring_copy(1, way, sub, step).wait_recv()
            if step < steps - 1:
                slot2_s[way, sub, step] = slot2_s[way, sub, step] + part
                send(1, way, sub, step + 1)
            else:
                total = slot2_s[way, sub, step] + part
                out_ref = dwo_ref if way == 0 else dwq_ref
                base = 0 if sub == 0 else cut // head_dim
                for index in range(cut // head_dim if sub == 0 else heads - cut // head_dim):
                    out_ref[base + index] = total[:, index * head_dim:(index + 1) * head_dim]
                if sub == 1:
                    side_ref = dwk_ref if way == 0 else dwv_ref
                    for index in range(kv_width // head_dim):
                        base = heads * head_dim - cut + index * head_dim
                        side_ref[:, index, :] = total[:, base:base + head_dim]
    for copy in started + mate_copies + extras:
        copy.wait_send()


VMEM_SPEC = pl.BlockSpec(memory_space=pltpu.VMEM)
ANY_SPEC = pl.BlockSpec(memory_space=pl.ANY)
VMEM_LIMIT = 60 * 1024 * 1024
REDUCE_LIMIT = 67043328


def solution(mesh):
    group_count = mesh.shape['cp']
    row_spec = P(('dp', 'cp'), None)
    tok_spec = P(('dp', 'cp'))
    weight_spec = P(None, None, None)
    grad_spec = P(('dp', 'cp'), None, None)

    def local_step(x_act, seg_ids, w_q, w_k, w_v, w_o, dy_act):
        tok = x_act.shape[0]
        model_dim, q_heads, head_dim = w_q.shape
        kv_heads = w_k.shape[1]
        group = q_heads // kv_heads
        q_width = q_heads * head_dim
        kv_width = kv_heads * head_dim
        tiles = tok // QT
        scale = head_dim ** -0.5
        bf16 = jnp.bfloat16

        w_kv = jnp.concatenate([w_k.reshape(model_dim, kv_width), w_v.reshape(model_dim, kv_width)], axis=1)
        seg_rows = seg_ids.reshape(tok // 128, 128)
        wq_heads = w_q.transpose(1, 0, 2)
        wo_heads = w_o.transpose(1, 0, 2)

        slots = kv_heads * tiles
        width = group * QT
        chips = group_count // 2
        reach = chips // 2
        dma = pltpu.SemaphoreType.DMA
        f32 = jnp.float32
        shape = jax.ShapeDtypeStruct
        flat = shape((tok, q_width), bf16)
        row32 = shape((tiles, 1, width), f32)
        wide32 = shape((tiles, head_dim, width), f32)
        kv_all, seg_all, q_loc, do_loc, do_turned, *kept = pl.pallas_call(
            functools.partial(gather_kernel, group_count, kv_heads, group, scale * LOG2E),
            out_shape=(shape((group_count, tok, 2 * kv_width), bf16), shape((group_count, tok // 128, 128), jnp.int32),
                       flat, flat, shape((q_width, tok), bf16), shape((tiles, 1, width), jnp.int32),
                       row32, row32, row32, row32, wide32, wide32),
            in_specs=[VMEM_SPEC] * 4 + [ANY_SPEC] * 2,
            out_specs=(ANY_SPEC, VMEM_SPEC) + (ANY_SPEC,) * 3 + (VMEM_SPEC,) * 7,
            scratch_shapes=[pltpu.VMEM((group_count, tok, 2 * kv_width), bf16), pltpu.VMEM((tok, q_width), bf16),
                            pltpu.VMEM((tok, q_width), bf16), pltpu.VMEM((q_width, tok), bf16),
                            dma((3,)), dma((group_count,)), pltpu.VMEM((tok, 2 * kv_width), bf16), pltpu.VMEM((q_heads, model_dim, head_dim), bf16),
                            pltpu.VMEM((q_heads, model_dim, head_dim), bf16),
                            dma((2,)), dma((group_count - 1,)), dma((group_count - 1,)),
                            dma((2, SLICES, reach)), dma((2, SLICES, reach)), dma((2, SLICES, reach)), dma((2, SLICES, reach)), dma((1,)), dma((1,))],
            compiler_params=pltpu.CompilerParams(collective_id=0, has_side_effects=True, vmem_limit_bytes=VMEM_LIMIT),
            cost_estimate=pl.CostEstimate(flops=8 * tok * model_dim * q_width, bytes_accessed=2**24, transcendentals=0),
            name='gather_keys',
        )(seg_rows, x_act, dy_act, w_kv, wq_heads, wo_heads)

        o_loc, dq_loc, dkv_all = pl.pallas_call(
            functools.partial(attention_kernel, kv_heads, group, scale),
            out_shape=(flat, flat, shape((group_count, tok, 2 * kv_width), f32)),
            in_specs=[VMEM_SPEC] * 5 + [ANY_SPEC] + [VMEM_SPEC] * 7,
            out_specs=(VMEM_SPEC, VMEM_SPEC, ANY_SPEC),
            scratch_shapes=[pltpu.VMEM((tiles, 1, width), f32)] * 4
                           + [pltpu.VMEM((slots, 1, width), f32)] + [pltpu.VMEM((tiles, head_dim, width), f32)] * 2
                           + [pltpu.VMEM((group_count, tok, 2 * kv_width), f32),
                            pltpu.VMEM((tok, 2 * kv_width), f32), dma((group_count,)),
                            pltpu.VMEM((group_count, tok, 2 * kv_width), bf16), dma((group_count,))],
            compiler_params=pltpu.CompilerParams(vmem_limit_bytes=VMEM_LIMIT),
            cost_estimate=pl.CostEstimate(flops=16 * 14 * tok * tok * q_width, bytes_accessed=2**25, transcendentals=0),
            name='attend',
        )(seg_rows, seg_all, q_loc, do_loc, do_turned, kv_all, *kept)

        out_rows = model_dim // group_count
        blk = (tok, 2 * kv_width)
        cols2 = (q_width + kv_width) // 2
        steps = chips - 1
        head_grad = shape((q_heads, out_rows, head_dim), f32)
        y_out, dx_out, dwo, dwq, dwk, dwv = pl.pallas_call(
            functools.partial(reduce_kernel, group_count, scale, kv_width),
            out_shape=(shape((tok, model_dim), bf16), shape((tok, model_dim), bf16), head_grad, head_grad,
                       shape((out_rows, kv_heads, head_dim), f32), shape((out_rows, kv_heads, head_dim), f32)),
            in_specs=[ANY_SPEC] * 8,
            out_specs=(VMEM_SPEC,) * 6,
            scratch_shapes=[pltpu.VMEM((tok, q_width), bf16), pltpu.VMEM((tok, q_width), bf16),
                            pltpu.VMEM((tok, model_dim), bf16), pltpu.VMEM((tok, model_dim), bf16),
                            pltpu.VMEM((model_dim, 2 * kv_width), bf16),
                            pltpu.VMEM((model_dim, tok), bf16), pltpu.VMEM((model_dim, tok), bf16),
                            pltpu.VMEM((model_dim, tok), bf16), pltpu.VMEM((model_dim, tok), bf16),
                            pltpu.VMEM((chips,) + blk, f32), pltpu.VMEM((chips,) + blk, f32),
                            pltpu.VMEM((2, 2, steps, tok // 4, 2 * kv_width), f32), pltpu.VMEM((2, 2, tok // 4, 2 * kv_width), f32),
                            pltpu.VMEM(blk, bf16), pltpu.VMEM(blk, bf16),
                            pltpu.VMEM((tok, q_width), bf16), pltpu.VMEM((tok, q_width), bf16),
                            pltpu.VMEM((2, 2, steps, out_rows, cols2), f32), pltpu.VMEM((2, 2, out_rows, cols2), f32),
                            pltpu.VMEM((q_heads, model_dim, head_dim), bf16), pltpu.VMEM((q_heads, model_dim, head_dim), bf16),
                            dma((7,)), dma((chips,)), dma((chips,)), dma((chips,)),
                            dma((2, 2, 2, steps)), dma((2, 2, 2, steps)), dma((5,)), dma((5,))],
            compiler_params=pltpu.CompilerParams(collective_id=1, has_side_effects=True, vmem_limit_bytes=REDUCE_LIMIT),
            cost_estimate=pl.CostEstimate(flops=16 * tok * model_dim * q_width, bytes_accessed=2**25, transcendentals=0),
            name='reduce_grads',
        )(dkv_all, o_loc, dq_loc, x_act, dy_act, w_kv, wq_heads, wo_heads)
        return y_out, dx_out, dwq.transpose(1, 0, 2), dwk, dwv, dwo.transpose(1, 0, 2)

    return jax.shard_map(local_step, mesh=mesh,
                         in_specs=(row_spec, tok_spec, weight_spec, weight_spec, weight_spec, weight_spec, row_spec),
                         out_specs=(row_spec, row_spec, grad_spec, grad_spec, grad_spec, grad_spec),
                         check_vma=False)
```

```python
import functools

import jax
import jax.numpy as jnp
from jax import lax
from jax.experimental import pallas as pl
from jax.experimental.pallas import tpu as pltpu
from jax.sharding import PartitionSpec as P

QT = 128
SLICES = 3
LOG2E = 1.4426950408889634
NEG_INF = float('-inf')
NT = (((1,), (1,)), ((), ()))
TN = (((0,), (0,)), ((), ()))
NN = (((1,), (0,)), ((), ()))


def dot32(left_arg, right_arg, dims):
    return lax.dot_general(left_arg, right_arg, dims, preferred_element_type=jnp.float32)


def stack_heads(ref, tile, head, group):
    rows = pl.ds(pl.multiple_of(tile * QT, QT), QT)
    return jnp.concatenate(
        [ref[rows, (head * group + member) * 128:(head * group + member + 1) * 128] for member in range(group)], axis=0)


def member_rows(ref, tile, head, group, chunk):
    rows = pl.ds(pl.multiple_of(tile * QT, QT), QT)
    first = (head * group + 2 * chunk) * 128
    return jnp.concatenate([ref[rows, first:first + 128], ref[rows, first + 128:first + 256]], axis=0)


def forward_update(kv_heads, group, scale2, tile, q_ref, kv_ref, blk, stats, mask_row, keys=None, diag=False):
    keys = kv_ref.shape[1] if keys is None else keys
    chains = [(head, chunk) for chunk in range(group // 2) for head in range(kv_heads)]
    k_blks = [kv_ref[blk, 0:keys, head * 128:(head + 1) * 128] for head in range(kv_heads)]
    v_turned = [kv_ref[blk, 0:keys, (kv_heads + head) * 128:(kv_heads + head + 1) * 128].T for head in range(kv_heads)]
    old = [None if diag else (stats[head][0][tile], stats[head][1][tile]) for head in range(kv_heads)]
    new_rows = [([], []) for head in range(kv_heads)]

    def score(chain):
        head, chunk = chain
        return dot32(k_blks[head], member_rows(q_ref, tile, head, group, chunk), NT)

    pending = [score(chain) for chain in chains[:6]]
    for index, (head, chunk) in enumerate(chains):
        scores = pending.pop(0)
        if index + 6 < len(chains):
            pending.append(score(chains[index + 6]))
        cols = slice(chunk * 256, (chunk + 1) * 256)
        if mask_row is not None:
            key_pos = lax.broadcasted_iota(jnp.int32, (keys, 256), 0)
            allowed = key_pos >= mask_row[:, cols]
            if diag:
                query_pos = lax.rem(lax.broadcasted_iota(jnp.int32, (1, 256), 1), QT) + tile * QT
                allowed = allowed & (key_pos <= query_pos)
            scores = jnp.where(allowed, scores, NEG_INF)
        new_max = jnp.max(scores, axis=0, keepdims=True) * scale2
        if not diag:
            old_max = old[head][0][:, cols]
            new_max = jnp.maximum(old_max, new_max)
        weights = jnp.exp2(scores * scale2 - new_max)
        total = jnp.sum(weights, axis=0, keepdims=True)
        part = dot32(v_turned[head], weights.astype(jnp.bfloat16), NN)
        acc = stats[head][2]
        if diag:
            acc[tile, :, cols] = part
        else:
            factor = jnp.exp2(old_max - new_max)
            total = old[head][1][:, cols] * factor + total
            acc[tile, :, cols] = acc[tile, :, cols] * factor + part
        new_rows[head][0].append(new_max)
        new_rows[head][1].append(total)
    for head in range(kv_heads):
        stats[head][0][tile] = jnp.concatenate(new_rows[head][0], axis=1)
        stats[head][1][tile] = jnp.concatenate(new_rows[head][1], axis=1)


def attention_kernel(kv_heads, group, scale, seg_ref, seg_all_ref, q_ref, do_ref, dot_ref, kv_hbm, start_s,
                     max0_ref, max1_ref, sum0_ref, sum1_ref, acc0_ref, acc1_ref,
                     o_ref, dq_ref, dkv_ref, max0_s, max1_s, sum0_s, sum1_s, delta_s, acc0_s, acc1_s,
                     grad_s, zero_s, out_sem,
                     kv_ref, in_sem):
    tok = q_ref.shape[0]
    blocks = kv_ref.shape[0]
    tiles = tok // QT
    width = group * QT
    scale2 = scale * LOG2E
    max_s, sum_s, acc_s = (max0_s, max1_s), (sum0_s, sum1_s), (acc0_s, acc1_s)
    stats = [(max_s[head], sum_s[head], acc_s[head]) for head in range(kv_heads)]
    me = lax.axis_index('cp')
    near_first = jnp.maximum(2 * (me // 2 - (blocks // 4 - 1)), 0)
    for kept_ref, kept_s in ((max0_ref, max0_s), (max1_ref, max1_s), (sum0_ref, sum0_s), (sum1_ref, sum1_s),
                             (acc0_ref, acc0_s), (acc1_ref, acc1_s)):
        kept_s[...] = kept_ref[...]
    zero_s[...] = jnp.zeros(zero_s.shape, jnp.float32)

    seg_own = seg_ref[...]
    first_seg = jnp.min(seg_own)
    head_count = jnp.sum((seg_own == first_seg).astype(jnp.int32))
    shard_index = lax.broadcasted_iota(jnp.int32, seg_all_ref.shape, 0)
    earlier = (shard_index < me) & (seg_all_ref[...] < first_seg)
    doc_start = jnp.sum(earlier.astype(jnp.int32))
    first = doc_start // tok
    has_prev = doc_start < me * tok
    tiles_prev = jnp.where(has_prev, (head_count + QT - 1) // QT, 0)
    full_tiles = head_count // QT

    def key_copy(blk):
        return pltpu.make_async_copy(kv_hbm.at[blk], kv_ref.at[blk], in_sem.at[blk])

    def key_body(blk, carry):
        key_copy(blk).start()
        return carry

    lax.fori_loop(first, me + 1, key_body, 0)

    def zero_copy(blk):
        return pltpu.make_async_copy(zero_s, dkv_ref.at[blk], out_sem.at[blk])

    def grad_copy(blk):
        return pltpu.make_async_copy(grad_s.at[blk], dkv_ref.at[blk], out_sem.at[blk])

    def clear_body(blk, carry):
        zero_copy(blk).start()
        return carry

    lax.fori_loop(0, first, clear_body, 0)
    lax.fori_loop(me + 1, blocks, clear_body, 0)

    def k_cols(head):
        return slice(head * 128, (head + 1) * 128)

    def v_cols(head):
        return slice((kv_heads + head) * 128, (kv_heads + head + 1) * 128)

    def diag_mask(tile, keys):
        key_pos = lax.broadcasted_iota(jnp.int32, (keys, width), 0)
        query_pos = lax.rem(lax.broadcasted_iota(jnp.int32, (1, width), 1), QT) + tile * QT
        return (key_pos <= query_pos) & (key_pos >= start_s[tile])

    def off_mask(tile, blk):
        key_pos = lax.broadcasted_iota(jnp.int32, (tok, width), 0)
        return key_pos >= start_s[tile] + (me - blk) * tok

    def over_tiles(body, blk):
        def tile_body(tile, carry):
            masked = (blk == first) | (tile >= full_tiles)
            pl.when(masked)(functools.partial(body, tile, True, blk))
            pl.when(jnp.logical_not(masked))(functools.partial(body, tile, False, blk))
            return carry
        lax.fori_loop(0, tiles_prev, tile_body, 0)

    def forward_body(tile, masked, blk):
        row = start_s[tile] + (me - blk) * tok if masked else None
        forward_update(kv_heads, group, scale2, tile, q_ref, kv_ref, blk, stats, row)

    def forward_blocks(blk, carry):
        key_copy(blk).wait()
        over_tiles(forward_body, blk)
        return carry

    lax.fori_loop(first, jnp.maximum(first, near_first), forward_blocks, 0)

    unit = (lax.broadcasted_iota(jnp.int32, (128, 128), 0)
            == lax.broadcasted_iota(jnp.int32, (128, 128), 1)).astype(jnp.bfloat16)

    def turned(block_t):
        return dot32(unit, block_t, NT).astype(jnp.bfloat16)

    for tile in range(tiles):
        for head in range(kv_heads):
            slot = head * tiles + tile
            total = sum_s[head][tile]
            max_s[head][tile] = max_s[head][tile] + jnp.log2(total)
            out_t = (acc_s[head][tile] / total).astype(jnp.bfloat16)
            first_col = head * group * 128
            do_t = jnp.concatenate(
                [dot_ref[first_col + member * 128:first_col + (member + 1) * 128, tile * QT:(tile + 1) * QT]
                 for member in range(group)], axis=1)
            delta_s[slot] = jnp.sum(do_t.astype(jnp.float32) * out_t.astype(jnp.float32), axis=0, keepdims=True)
            for member in range(group):
                col = first_col + member * 128
                o_ref[tile * QT:(tile + 1) * QT, col:col + 128] = turned(out_t[:, member * QT:(member + 1) * QT])

    def grads(tile, head, blk, keys, mask_fn):
        slot = head * tiles + tile
        q_tile = stack_heads(q_ref, tile, head, group)
        do_tile = stack_heads(do_ref, tile, head, group)
        k_blk = kv_ref[blk, 0:keys, k_cols(head)]
        v_blk = kv_ref[blk, 0:keys, v_cols(head)]
        scores = dot32(k_blk, q_tile, NT) * scale2
        if mask_fn is not None:
            scores = jnp.where(mask_fn(), scores, NEG_INF)
        prob = jnp.exp2(scores - max_s[head][tile])
        dprob = dot32(v_blk, do_tile, NT)
        dscore = (prob * (dprob - delta_s[slot])).astype(jnp.bfloat16)
        dv_part = dot32(prob.astype(jnp.bfloat16), do_tile, NN)
        dk_part = dot32(dscore, q_tile, NN)
        dq_part = dot32(k_blk, dscore, TN)
        return dq_part, dk_part, dv_part

    key_copy(me).wait()
    for tile in reversed(range(tiles)):
        keys = QT * (tile + 1)
        for head in range(kv_heads):
            dq_part, dk_part, dv_part = grads(tile, head, me, keys, functools.partial(diag_mask, tile, keys))
            acc_s[head][tile] = dq_part
            if tile == tiles - 1:
                grad_s[me, 0:keys, k_cols(head)] = dk_part
                grad_s[me, 0:keys, v_cols(head)] = dv_part
            else:
                grad_s[me, 0:keys, k_cols(head)] = grad_s[me, 0:keys, k_cols(head)] + dk_part
                grad_s[me, 0:keys, v_cols(head)] = grad_s[me, 0:keys, v_cols(head)] + dv_part
    grad_copy(me).start()

    def backward_body(tile, masked, blk):
        for head in range(kv_heads):
            slot = head * tiles + tile
            dq_part, dk_part, dv_part = grads(tile, head, blk, tok, functools.partial(off_mask, tile, blk) if masked else None)
            acc_s[head][tile] = acc_s[head][tile] + dq_part
            grad_s[blk, :, k_cols(head)] = grad_s[blk, :, k_cols(head)] + dk_part
            grad_s[blk, :, v_cols(head)] = grad_s[blk, :, v_cols(head)] + dv_part

    def backward_blocks(blk, carry):
        pl.when(blk >= near_first)(lambda: key_copy(blk).wait())
        grad_s[blk] = jnp.zeros(zero_s.shape, jnp.float32)
        over_tiles(backward_body, blk)
        grad_copy(blk).start()
        return carry

    lax.fori_loop(first, me, backward_blocks, 0)

    for tile in range(tiles):
        for head in range(kv_heads):
            grad_t = (acc_s[head][tile] * scale).astype(jnp.bfloat16)
            for member in range(group):
                col = (head * group + member) * 128
                dq_ref[tile * QT:(tile + 1) * QT, col:col + 128] = turned(grad_t[:, member * QT:(member + 1) * QT])

    def wait_body(blk, carry):
        zero_copy(blk).wait()
        return carry

    lax.fori_loop(0, blocks, wait_body, 0)


def places(n):
    me = lax.axis_index('cp')
    chips = n // 2
    core = lax.rem(me, 2)
    chip = me // 2

    def at(offset, which):
        return lax.rem(chip + offset + chips, chips) * 2 + which

    return me, chips, core, chip, at


def remote(src, dst, send_sem, recv_sem, target):
    return pltpu.make_async_remote_copy(src_ref=src, dst_ref=dst, send_sem=send_sem, recv_sem=recv_sem,
                                        device_id={'cp': target}, device_id_type=pl.DeviceIdType.MESH)


def greet(targets):
    barrier = pltpu.get_barrier_semaphore()
    for target in targets:
        pl.semaphore_signal(barrier, inc=1, device_id={'cp': target}, device_id_type=pl.DeviceIdType.MESH)
    pl.semaphore_wait(barrier, len(targets))


def gather_kernel(n, kv_heads, group, scale2, seg_ref, x_ref, dy_ref, wkv_ref, wq_ref, wo_ref,
                  kv_out, wkv_out, seg_all_ref, q_out, do_out, dot_out, start_ref,
                  max0_ref, max1_ref, sum0_ref, sum1_ref, acc0_ref, acc1_ref,
                  kv_all_ref, q_ref, do_ref, dot_ref, flat_sem, block_sem, kv_s, wq_s, wo_s, load_sem, seg_send, seg_recv, ring_send, ring_recv, pair_send, pair_recv,
                  mate_send, mate_recv):
    me, chips, core, chip, at = places(n)
    mate = at(0, 1 - core)
    tok = kv_s.shape[0]
    tiles = tok // QT
    slice_rows = tok // SLICES
    reach = chips // 2
    stats = [(max0_ref, sum0_ref, acc0_ref), (max1_ref, sum1_ref, acc1_ref)]
    load_q = pltpu.make_async_copy(wq_ref, wq_s, load_sem.at[0])
    load_o = pltpu.make_async_copy(wo_ref, wo_s, load_sem.at[1])
    load_q.start()
    load_o.start()
    kv_own = dot32(x_ref[...], wkv_ref[...], NN).astype(jnp.bfloat16)
    kv_s[...] = kv_own
    kv_all_ref[me] = kv_own
    seg_all_ref[me] = seg_ref[...]
    greet([lax.rem(me + step, n) for step in range(1, n)])

    flat_outs = [pltpu.make_async_copy(src, dst, flat_sem.at[index]) for index, (src, dst) in enumerate(
        ((q_ref, q_out), (do_ref, do_out), (dot_ref, dot_out), (wkv_ref, wkv_out)))]

    def block_out(blk):
        return pltpu.make_async_copy(kv_all_ref.at[blk], kv_out.at[blk], block_sem.at[blk])

    def rows(sub):
        return pl.ds(pl.multiple_of(sub * slice_rows, slice_rows), slice_rows)

    def ring_copy(way, sub, hop):
        offset = 1 - hop if way == 0 else hop - 1
        spot = kv_all_ref.at[at(offset, core), rows(sub)]
        return remote(spot, spot, ring_send.at[way, sub, hop - 1], ring_recv.at[way, sub, hop - 1],
                      at(1 if way == 0 else -1, core))

    def pair_copy(way, sub, hop):
        spot = kv_all_ref.at[at(-hop if way == 0 else hop, core), rows(sub)]
        return remote(spot, spot, pair_send.at[way, sub, hop - 1], pair_recv.at[way, sub, hop - 1], mate)

    def seg_copy(step):
        return remote(seg_ref, seg_all_ref.at[me], seg_send.at[step - 1], seg_recv.at[step - 1], lax.rem(me + step, n))

    def own_copy():
        return remote(kv_s, kv_all_ref.at[me], mate_send.at[0], mate_recv.at[0], mate)

    for sub in range(SLICES):
        for way in range(2):
            ring_copy(way, sub, 1).start()
    own_copy().start()
    for step in range(1, n):
        seg_copy(step).start()

    pairs = wq_s.shape[0] // 2

    def project(src_ref, w_s, dst_ref, pair):
        w_pair = jnp.concatenate([w_s[2 * pair], w_s[2 * pair + 1]], axis=1)
        cols = pl.ds(pl.multiple_of(pair * 256, 256), 256)
        value = dot32(src_ref[...], w_pair, NN).astype(jnp.bfloat16)
        dst_ref[:, cols] = value
        return value

    def query_pair(pair, carry):
        project(x_ref, wq_s, q_ref, pair)
        return carry

    load_q.wait()
    lax.fori_loop(0, pairs, query_pair, 0)

    for step in range(1, n):
        seg_copy(step).wait_recv()
    seg_own = seg_ref[...]
    first_seg = jnp.min(seg_own)
    shard_index = lax.broadcasted_iota(jnp.int32, seg_all_ref.shape, 0)
    earlier = (shard_index < me) & (seg_all_ref[...] < first_seg)
    doc_start = jnp.sum(earlier.astype(jnp.int32))
    seg_wide = seg_own.astype(jnp.float32)
    columns = [jnp.broadcast_to(seg_wide[part:part + 1, :], (128, 128)).T for part in range(tok // 128)]
    for tile in range(tiles):
        count = sum(jnp.sum((column < seg_wide[tile:tile + 1, :]).astype(jnp.int32), axis=0, keepdims=True)
                    for column in columns)
        row = jnp.where(count == 0, doc_start - me * tok, count)
        start_ref[tile] = jnp.concatenate([row] * group, axis=1)

    for tile in range(tiles):
        forward_update(kv_heads, group, scale2, tile, q_ref, kv_all_ref, me, stats, start_ref[tile], QT * (tile + 1), True)
    load_o.wait()
    flat_outs[0].start()
    flat_outs[3].start()

    def tick_body(tick, carry):
        step, sub = tick // SLICES, lax.rem(tick, SLICES)
        for way in range(2):
            last = (sub < SLICES // 2) if way == 0 else (sub >= SLICES // 2)

            @pl.when((step < reach - 1) | last)
            def _():
                ring_copy(way, sub, step + 1).wait_recv()
                pair_copy(way, sub, step + 1).start()

            @pl.when((step < reach - 2) | ((step == reach - 2) & last))
            def _():
                ring_copy(way, sub, step + 2).start()

        @pl.when((step == 0) & (sub == 0))
        def _():
            own_copy().wait_recv()

        @pl.when((step > 0) & (sub == 0))
        def _():
            for piece in range(SLICES):
                pair_copy(0, piece, step).wait_recv()

        @pl.when(sub == 0)
        def _():
            for which in range(2):
                block_out(at(-step, which)).start()

        spread = reach * SLICES // pairs

        @pl.when(lax.rem(tick, spread) == 0)
        def _():
            pair = tick // spread
            value = project(dy_ref, wo_s, do_ref, pair)
            dot_ref[pl.ds(pl.multiple_of(pair * 256, 256), 256), :] = value.T

        def near_tile(item, inner):
            side = item // tiles
            tile = lax.rem(item, tiles)

            @pl.when((chip >= step) & ((step > 0) | ((core == 1) & (side == 0))))
            def _():
                blk = 2 * (chip - step) + side
                forward_update(kv_heads, group, scale2, tile, q_ref, kv_all_ref, blk, stats,
                               start_ref[tile] + (me - blk) * tok)
            return inner

        share = 2 * tiles // SLICES
        lax.fori_loop(sub * share, (sub + 1) * share, near_tile, 0)
        return carry

    lax.fori_loop(0, reach * SLICES, tick_body, 0)
    flat_outs[1].start()
    flat_outs[2].start()
    for way in range(2):
        for sub in range(SLICES):
            for hop in range(1, reach + 1):
                if hop < reach or (sub < SLICES // 2) == (way == 0):
                    if way == 1 or hop == reach:
                        pair_copy(way, sub, hop).wait_recv()
                    pair_copy(way, sub, hop).wait_send()
                    ring_copy(way, sub, hop).wait_send()
    for offset in range(1, chips - reach + 1):
        for which in range(2):
            block_out(at(offset, which)).start()
    own_copy().wait_send()
    for step in range(1, n):
        seg_copy(step).wait_send()
    for copy in flat_outs:
        copy.wait()
    for blk in range(n):
        block_out(blk).wait()


def reduce_kernel(n, scale, kv_width, dkv_ref, o_hbm, dq_hbm, x_hbm, dy_hbm, wkv_hbm, wq_ref, wo_ref,
                  y_ref, dx_ref, dwo_ref, dwq_ref, dwk_ref, dwv_ref,
                  o_ref, dq_ref, x_ref, dy_ref, wkv_ref, xt_ref, dyt_ref, xtp_ref, dytp_ref,
                  own_s, mate_s, slot1_s, stage1_s, grad_s, grad_mate_s, o_mate_s, dq_mate_s, slot2_s, stage2_s,
                  wq_s, wo_s, load_sem, block_sem, mate_send, mate_recv, ring_send, ring_recv, extra_send, extra_recv):
    me, chips, core, chip, at = places(n)
    mate = at(0, 1 - core)
    ring = (at(1, core), at(-1, core))
    tok = o_ref.shape[0]
    quarter = tok // 4
    heads, out_rows, head_dim = dwo_ref.shape
    loads = [pltpu.make_async_copy(src, dst, load_sem.at[index]) for index, (src, dst) in enumerate(
        ((o_hbm, o_ref), (dq_hbm, dq_ref), (x_hbm, x_ref), (dy_hbm, dy_ref), (wo_ref, wo_s), (wq_ref, wq_s),
         (wkv_hbm, wkv_ref)))]
    order = []
    for step in range(1, chips):
        for offset in (-step, step):
            if offset % chips not in order:
                order.append(offset % chips)
    order.append(0)
    own_loads = [pltpu.make_async_copy(dkv_ref.at[at(offset, core)], own_s.at[index], block_sem.at[index])
                 for index, offset in enumerate(order)]
    for load in own_loads:
        load.start()
    for load in loads:
        load.start()
    greet([ring[0], ring[1], mate])
    mate_copies = [remote(dkv_ref.at[at(offset, 1 - core)], mate_s.at[index], mate_send.at[index], mate_recv.at[index], mate)
                   for index, offset in enumerate(order)]
    extras = [remote(o_hbm, o_mate_s, extra_send.at[0], extra_recv.at[0], mate),
              remote(dq_hbm, dq_mate_s, extra_send.at[1], extra_recv.at[1], mate),
              remote(grad_s, grad_mate_s, extra_send.at[2], extra_recv.at[2], mate),
              remote(xt_ref, xtp_ref, extra_send.at[3], extra_recv.at[3], mate),
              remote(dyt_ref, dytp_ref, extra_send.at[4], extra_recv.at[4], mate)]
    for index, copy in enumerate(mate_copies):
        copy.start()
        if index == 3:
            extras[0].start()
            extras[1].start()

    ready = set()

    def need(position):
        if position not in ready:
            ready.add(position)
            own_loads[position].wait()
            mate_copies[position].wait_recv()

    def ring_copy(job, way, sub, step):
        slots, stage = (slot1_s, stage1_s) if job == 0 else (slot2_s, stage2_s)
        src = stage.at[way, sub] if step == 0 else slots.at[way, sub, step - 1]
        return remote(src, slots.at[way, sub, step], ring_send.at[job, way, sub, step], ring_recv.at[job, way, sub, step],
                      ring[way])

    started = []

    def send(job, way, sub, step):
        started.append(ring_copy(job, way, sub, step))
        started[-1].start()

    def contrib1(way, sub, step):
        offset = (-(1 + step) if way == 0 else 1 + step) % chips
        position = order.index(offset)
        need(position)
        span = slice((2 * way + sub) * quarter, (2 * way + sub + 1) * quarter)
        return own_s[position, span, :] + mate_s[position, span, :]

    cut = 7 * head_dim

    def contrib2(way, sub, step):
        offset = -(1 + step) if way == 0 else 1 + step
        first_row = pl.multiple_of(at(offset % chips, core) * out_rows, 32)
        take = pl.ds(first_row, out_rows)
        lhs, lhs_mate = (dyt_ref, dytp_ref) if way == 0 else (xt_ref, xtp_ref)
        rhs, rhs_mate = (o_ref, o_mate_s) if way == 0 else (dq_ref, dq_mate_s)
        if sub == 0:
            return (dot32(lhs[take, :], rhs[:, 0:cut], NN) + dot32(lhs_mate[take, :], rhs_mate[:, 0:cut], NN))
        main = dot32(lhs[take, :], rhs[:, cut:], NN) + dot32(lhs_mate[take, :], rhs_mate[:, cut:], NN)
        cols = slice(way * kv_width, (way + 1) * kv_width)
        side = dot32(xt_ref[take, :], grad_s[:, cols], NN) + dot32(xtp_ref[take, :], grad_mate_s[:, cols], NN)
        return jnp.concatenate([main, side], axis=1)

    strip = 256
    strips = y_ref.shape[1] // strip

    def rows_out(part):
        return pl.ds(pl.multiple_of(part * strip, strip), strip)

    def times_weight(src_ref, w_s, part):
        total = None
        for pair in range(heads // 2):
            w_pair = jnp.concatenate([w_s[2 * pair, rows_out(part), :], w_s[2 * pair + 1, rows_out(part), :]], axis=1)
            piece = dot32(src_ref[:, pair * 256:(pair + 1) * 256], w_pair, NT)
            total = piece if total is None else total + piece
        return total

    def y_strip(part, carry):
        y_ref[:, rows_out(part)] = times_weight(o_ref, wo_s, part).astype(jnp.bfloat16)
        return carry

    def flip_strip(part, carry):
        xt_ref[rows_out(part), :] = x_ref[:, rows_out(part)].T
        dyt_ref[rows_out(part), :] = dy_ref[:, rows_out(part)].T
        return carry

    def dx_strip(part, carry):
        wide = times_weight(dq_ref, wq_s, part) + dot32(grad_s[...], wkv_ref[rows_out(part), :], NT)
        dx_ref[:, rows_out(part)] = wide.astype(jnp.bfloat16)
        return carry

    steps = chips - 1
    both = [(sub, way) for sub in range(2) for way in range(2)]
    for sub, way in both:
        stage1_s[way, sub] = contrib1(way, sub, 0)
        send(0, way, sub, 0)
    for load in loads:
        load.wait()
    for step in range(steps):
        if step == 0:
            lax.fori_loop(0, strips, y_strip, 0)
        if step == 1:
            lax.fori_loop(0, strips, flip_strip, 0)
        if step == 4:
            extras[3].start()
            extras[4].start()
        if step == steps - 1:
            for index in (0, 1, 3, 4):
                extras[index].wait_recv()
            for way in range(2):
                stage2_s[way, 0] = contrib2(way, 0, 0)
                send(1, way, 0, 0)
        for sub, way in both:
            part = contrib1(way, sub, step + 1)
            ring_copy(0, way, sub, step).wait_recv()
            if step < steps - 1:
                slot1_s[way, sub, step] = slot1_s[way, sub, step] + part
                send(0, way, sub, step + 1)
            else:
                span = slice((2 * way + sub) * quarter, (2 * way + sub + 1) * quarter)
                total = slot1_s[way, sub, step] + part
                grad_s[span, 0:kv_width] = (total[:, 0:kv_width] * scale).astype(jnp.bfloat16)
                grad_s[span, kv_width:] = total[:, kv_width:].astype(jnp.bfloat16)
    extras[2].start()
    extras[2].wait_recv()
    for way in range(2):
        stage2_s[way, 1] = contrib2(way, 1, 0)
        send(1, way, 1, 0)
    for step in range(steps):
        if step == 0:
            lax.fori_loop(0, strips, dx_strip, 0)
        for sub, way in both:
            part = contrib2(way, sub, step + 1)
            ring_copy(1, way, sub, step).wait_recv()
            if step < steps - 1:
                slot2_s[way, sub, step] = slot2_s[way, sub, step] + part
                send(1, way, sub, step + 1)
            else:
                total = slot2_s[way, sub, step] + part
                out_ref = dwo_ref if way == 0 else dwq_ref
                base = 0 if sub == 0 else cut // head_dim
                for index in range(cut // head_dim if sub == 0 else heads - cut // head_dim):
                    out_ref[base + index] = total[:, index * head_dim:(index + 1) * head_dim]
                if sub == 1:
                    side_ref = dwk_ref if way == 0 else dwv_ref
                    for index in range(kv_width // head_dim):
                        base = heads * head_dim - cut + index * head_dim
                        side_ref[:, index, :] = total[:, base:base + head_dim]
    for copy in started + mate_copies + extras:
        copy.wait_send()


VMEM_SPEC = pl.BlockSpec(memory_space=pltpu.VMEM)
ANY_SPEC = pl.BlockSpec(memory_space=pl.ANY)
VMEM_LIMIT = 60 * 1024 * 1024
REDUCE_LIMIT = 67043328


def solution(mesh):
    group_count = mesh.shape['cp']
    row_spec = P(('dp', 'cp'), None)
    tok_spec = P(('dp', 'cp'))
    weight_spec = P(None, None, None)
    grad_spec = P(('dp', 'cp'), None, None)

    def local_step(x_act, seg_ids, w_q, w_k, w_v, w_o, dy_act):
        tok = x_act.shape[0]
        model_dim, q_heads, head_dim = w_q.shape
        kv_heads = w_k.shape[1]
        group = q_heads // kv_heads
        q_width = q_heads * head_dim
        kv_width = kv_heads * head_dim
        tiles = tok // QT
        scale = head_dim ** -0.5
        bf16 = jnp.bfloat16

        w_kv = jnp.concatenate([w_k.reshape(model_dim, kv_width), w_v.reshape(model_dim, kv_width)], axis=1)
        seg_rows = seg_ids.reshape(tok // 128, 128)
        wq_heads = w_q.transpose(1, 0, 2)
        wo_heads = w_o.transpose(1, 0, 2)

        slots = kv_heads * tiles
        width = group * QT
        chips = group_count // 2
        reach = chips // 2
        dma = pltpu.SemaphoreType.DMA
        f32 = jnp.float32
        shape = jax.ShapeDtypeStruct
        flat = shape((tok, q_width), bf16)
        row32 = shape((tiles, 1, width), f32)
        wide32 = shape((tiles, head_dim, width), f32)
        kv_all, wkv_kept, seg_all, q_loc, do_loc, do_turned, *kept = pl.pallas_call(
            functools.partial(gather_kernel, group_count, kv_heads, group, scale * LOG2E),
            out_shape=(shape((group_count, tok, 2 * kv_width), bf16), shape((model_dim, 2 * kv_width), bf16),
                       shape((group_count, tok // 128, 128), jnp.int32),
                       flat, flat, shape((q_width, tok), bf16), shape((tiles, 1, width), jnp.int32),
                       row32, row32, row32, row32, wide32, wide32),
            in_specs=[VMEM_SPEC] * 4 + [ANY_SPEC] * 2,
            out_specs=(ANY_SPEC, ANY_SPEC, VMEM_SPEC) + (ANY_SPEC,) * 3 + (VMEM_SPEC,) * 7,
            scratch_shapes=[pltpu.VMEM((group_count, tok, 2 * kv_width), bf16), pltpu.VMEM((tok, q_width), bf16),
                            pltpu.VMEM((tok, q_width), bf16), pltpu.VMEM((q_width, tok), bf16),
                            dma((4,)), dma((group_count,)), pltpu.VMEM((tok, 2 * kv_width), bf16), pltpu.VMEM((q_heads, model_dim, head_dim), bf16),
                            pltpu.VMEM((q_heads, model_dim, head_dim), bf16),
                            dma((2,)), dma((group_count - 1,)), dma((group_count - 1,)),
                            dma((2, SLICES, reach)), dma((2, SLICES, reach)), dma((2, SLICES, reach)), dma((2, SLICES, reach)), dma((1,)), dma((1,))],
            compiler_params=pltpu.CompilerParams(collective_id=0, has_side_effects=True, vmem_limit_bytes=VMEM_LIMIT),
            cost_estimate=pl.CostEstimate(flops=8 * tok * model_dim * q_width, bytes_accessed=2**24, transcendentals=0),
            name='gather_keys',
        )(seg_rows, x_act, dy_act, w_kv, wq_heads, wo_heads)

        o_loc, dq_loc, dkv_all = pl.pallas_call(
            functools.partial(attention_kernel, kv_heads, group, scale),
            out_shape=(flat, flat, shape((group_count, tok, 2 * kv_width), f32)),
            in_specs=[VMEM_SPEC] * 5 + [ANY_SPEC] + [VMEM_SPEC] * 7,
            out_specs=(VMEM_SPEC, VMEM_SPEC, ANY_SPEC),
            scratch_shapes=[pltpu.VMEM((tiles, 1, width), f32)] * 4
                           + [pltpu.VMEM((slots, 1, width), f32)] + [pltpu.VMEM((tiles, head_dim, width), f32)] * 2
                           + [pltpu.VMEM((group_count, tok, 2 * kv_width), f32),
                            pltpu.VMEM((tok, 2 * kv_width), f32), dma((group_count,)),
                            pltpu.VMEM((group_count, tok, 2 * kv_width), bf16), dma((group_count,))],
            compiler_params=pltpu.CompilerParams(vmem_limit_bytes=VMEM_LIMIT),
            cost_estimate=pl.CostEstimate(flops=16 * 14 * tok * tok * q_width, bytes_accessed=2**25, transcendentals=0),
            name='attend',
        )(seg_rows, seg_all, q_loc, do_loc, do_turned, kv_all, *kept)

        out_rows = model_dim // group_count
        blk = (tok, 2 * kv_width)
        cols2 = (q_width + kv_width) // 2
        steps = chips - 1
        head_grad = shape((q_heads, out_rows, head_dim), f32)
        y_out, dx_out, dwo, dwq, dwk, dwv = pl.pallas_call(
            functools.partial(reduce_kernel, group_count, scale, kv_width),
            out_shape=(shape((tok, model_dim), bf16), shape((tok, model_dim), bf16), head_grad, head_grad,
                       shape((out_rows, kv_heads, head_dim), f32), shape((out_rows, kv_heads, head_dim), f32)),
            in_specs=[ANY_SPEC] * 8,
            out_specs=(VMEM_SPEC,) * 6,
            scratch_shapes=[pltpu.VMEM((tok, q_width), bf16), pltpu.VMEM((tok, q_width), bf16),
                            pltpu.VMEM((tok, model_dim), bf16), pltpu.VMEM((tok, model_dim), bf16),
                            pltpu.VMEM((model_dim, 2 * kv_width), bf16),
                            pltpu.VMEM((model_dim, tok), bf16), pltpu.VMEM((model_dim, tok), bf16),
                            pltpu.VMEM((model_dim, tok), bf16), pltpu.VMEM((model_dim, tok), bf16),
                            pltpu.VMEM((chips,) + blk, f32), pltpu.VMEM((chips,) + blk, f32),
                            pltpu.VMEM((2, 2, steps, tok // 4, 2 * kv_width), f32), pltpu.VMEM((2, 2, tok // 4, 2 * kv_width), f32),
                            pltpu.VMEM(blk, bf16), pltpu.VMEM(blk, bf16),
                            pltpu.VMEM((tok, q_width), bf16), pltpu.VMEM((tok, q_width), bf16),
                            pltpu.VMEM((2, 2, steps, out_rows, cols2), f32), pltpu.VMEM((2, 2, out_rows, cols2), f32),
                            pltpu.VMEM((q_heads, model_dim, head_dim), bf16), pltpu.VMEM((q_heads, model_dim, head_dim), bf16),
                            dma((7,)), dma((chips,)), dma((chips,)), dma((chips,)),
                            dma((2, 2, 2, steps)), dma((2, 2, 2, steps)), dma((5,)), dma((5,))],
            compiler_params=pltpu.CompilerParams(collective_id=1, has_side_effects=True, vmem_limit_bytes=REDUCE_LIMIT),
            cost_estimate=pl.CostEstimate(flops=16 * tok * model_dim * q_width, bytes_accessed=2**25, transcendentals=0),
            name='reduce_grads',
        )(dkv_all, o_loc, dq_loc, x_act, dy_act, wkv_kept, wq_heads, wo_heads)
        return y_out, dx_out, dwq.transpose(1, 0, 2), dwk, dwv, dwo.transpose(1, 0, 2)

    return jax.shard_map(local_step, mesh=mesh,
                         in_specs=(row_spec, tok_spec, weight_spec, weight_spec, weight_spec, weight_spec, row_spec),
                         out_specs=(row_spec, row_spec, grad_spec, grad_spec, grad_spec, grad_spec),
                         check_vma=False)
```

```python
import functools

import jax
import jax.numpy as jnp
from jax import lax
from jax.experimental import pallas as pl
from jax.experimental.pallas import tpu as pltpu
from jax.sharding import PartitionSpec as P

QT = 128
SLICES = 3
LOG2E = 1.4426950408889634
NEG_INF = float('-inf')
NT = (((1,), (1,)), ((), ()))
TN = (((0,), (0,)), ((), ()))
NN = (((1,), (0,)), ((), ()))


def dot32(left_arg, right_arg, dims):
    return lax.dot_general(left_arg, right_arg, dims, preferred_element_type=jnp.float32)


def stack_heads(ref, tile, head, group):
    rows = pl.ds(pl.multiple_of(tile * QT, QT), QT)
    return jnp.concatenate(
        [ref[rows, (head * group + member) * 128:(head * group + member + 1) * 128] for member in range(group)], axis=0)


def member_rows(ref, tile, head, group, chunk):
    rows = pl.ds(pl.multiple_of(tile * QT, QT), QT)
    first = (head * group + 2 * chunk) * 128
    return jnp.concatenate([ref[rows, first:first + 128], ref[rows, first + 128:first + 256]], axis=0)


def forward_update(kv_heads, group, scale2, tile, q_ref, kv_ref, blk, stats, mask_row, keys=None, diag=False):
    keys = kv_ref.shape[1] if keys is None else keys
    chains = [(head, chunk) for chunk in range(group // 2) for head in range(kv_heads)]
    k_blks = [kv_ref[blk, 0:keys, head * 128:(head + 1) * 128] for head in range(kv_heads)]
    v_turned = [kv_ref[blk, 0:keys, (kv_heads + head) * 128:(kv_heads + head + 1) * 128].T for head in range(kv_heads)]
    old = [None if diag else (stats[head][0][tile], stats[head][1][tile]) for head in range(kv_heads)]
    new_rows = [([], []) for head in range(kv_heads)]

    def score(chain):
        head, chunk = chain
        return dot32(k_blks[head], member_rows(q_ref, tile, head, group, chunk), NT)

    pending = [score(chain) for chain in chains[:6]]
    for index, (head, chunk) in enumerate(chains):
        scores = pending.pop(0)
        if index + 6 < len(chains):
            pending.append(score(chains[index + 6]))
        cols = slice(chunk * 256, (chunk + 1) * 256)
        if mask_row is not None:
            key_pos = lax.broadcasted_iota(jnp.int32, (keys, 256), 0)
            allowed = key_pos >= mask_row[:, cols]
            if diag:
                query_pos = lax.rem(lax.broadcasted_iota(jnp.int32, (1, 256), 1), QT) + tile * QT
                allowed = allowed & (key_pos <= query_pos)
            scores = jnp.where(allowed, scores, NEG_INF)
        new_max = jnp.max(scores, axis=0, keepdims=True) * scale2
        if not diag:
            old_max = old[head][0][:, cols]
            new_max = jnp.maximum(old_max, new_max)
        weights = jnp.exp2(scores * scale2 - new_max)
        total = jnp.sum(weights, axis=0, keepdims=True)
        part = dot32(v_turned[head], weights.astype(jnp.bfloat16), NN)
        acc = stats[head][2]
        if diag:
            acc[tile, :, cols] = part
        else:
            factor = jnp.exp2(old_max - new_max)
            total = old[head][1][:, cols] * factor + total
            acc[tile, :, cols] = acc[tile, :, cols] * factor + part
        new_rows[head][0].append(new_max)
        new_rows[head][1].append(total)
    for head in range(kv_heads):
        stats[head][0][tile] = jnp.concatenate(new_rows[head][0], axis=1)
        stats[head][1][tile] = jnp.concatenate(new_rows[head][1], axis=1)


def attention_kernel(kv_heads, group, scale, seg_ref, seg_all_ref, q_ref, do_ref, dot_ref, kv_hbm, start_s,
                     max0_ref, max1_ref, sum0_ref, sum1_ref, acc0_ref, acc1_ref,
                     o_ref, dq_ref, dkv_ref, max0_s, max1_s, sum0_s, sum1_s, delta_s, acc0_s, acc1_s,
                     grad_s, zero_s, out_sem,
                     kv_ref, in_sem):
    tok = q_ref.shape[0]
    blocks = kv_ref.shape[0]
    tiles = tok // QT
    width = group * QT
    scale2 = scale * LOG2E
    max_s, sum_s, acc_s = (max0_s, max1_s), (sum0_s, sum1_s), (acc0_s, acc1_s)
    stats = [(max_s[head], sum_s[head], acc_s[head]) for head in range(kv_heads)]
    me = lax.axis_index('cp')
    near_first = jnp.maximum(2 * (me // 2 - (blocks // 4 - 1)), 0)
    for kept_ref, kept_s in ((max0_ref, max0_s), (max1_ref, max1_s), (sum0_ref, sum0_s), (sum1_ref, sum1_s),
                             (acc0_ref, acc0_s), (acc1_ref, acc1_s)):
        kept_s[...] = kept_ref[...]
    zero_s[...] = jnp.zeros(zero_s.shape, jnp.float32)

    seg_own = seg_ref[...]
    first_seg = jnp.min(seg_own)
    head_count = jnp.sum((seg_own == first_seg).astype(jnp.int32))
    shard_index = lax.broadcasted_iota(jnp.int32, seg_all_ref.shape, 0)
    earlier = (shard_index < me) & (seg_all_ref[...] < first_seg)
    doc_start = jnp.sum(earlier.astype(jnp.int32))
    first = doc_start // tok
    has_prev = doc_start < me * tok
    tiles_prev = jnp.where(has_prev, (head_count + QT - 1) // QT, 0)
    full_tiles = head_count // QT

    def key_copy(blk):
        return pltpu.make_async_copy(kv_hbm.at[blk], kv_ref.at[blk], in_sem.at[blk])

    def key_body(blk, carry):
        key_copy(blk).start()
        return carry

    lax.fori_loop(first, me + 1, key_body, 0)

    def zero_copy(blk):
        return pltpu.make_async_copy(zero_s, dkv_ref.at[blk], out_sem.at[blk])

    def grad_copy(blk):
        return pltpu.make_async_copy(grad_s.at[blk], dkv_ref.at[blk], out_sem.at[blk])

    def clear_body(blk, carry):
        zero_copy(blk).start()
        return carry

    lax.fori_loop(0, first, clear_body, 0)
    lax.fori_loop(me + 1, blocks, clear_body, 0)

    def k_cols(head):
        return slice(head * 128, (head + 1) * 128)

    def v_cols(head):
        return slice((kv_heads + head) * 128, (kv_heads + head + 1) * 128)

    def diag_mask(tile, keys):
        key_pos = lax.broadcasted_iota(jnp.int32, (keys, width), 0)
        query_pos = lax.rem(lax.broadcasted_iota(jnp.int32, (1, width), 1), QT) + tile * QT
        return (key_pos <= query_pos) & (key_pos >= start_s[tile])

    def off_mask(tile, blk):
        key_pos = lax.broadcasted_iota(jnp.int32, (tok, width), 0)
        return key_pos >= start_s[tile] + (me - blk) * tok

    def over_tiles(body, blk):
        def tile_body(tile, carry):
            masked = (blk == first) | (tile >= full_tiles)
            pl.when(masked)(functools.partial(body, tile, True, blk))
            pl.when(jnp.logical_not(masked))(functools.partial(body, tile, False, blk))
            return carry
        lax.fori_loop(0, tiles_prev, tile_body, 0)

    def forward_body(tile, masked, blk):
        row = start_s[tile] + (me - blk) * tok if masked else None
        forward_update(kv_heads, group, scale2, tile, q_ref, kv_ref, blk, stats, row)

    def forward_blocks(blk, carry):
        key_copy(blk).wait()
        over_tiles(forward_body, blk)
        return carry

    lax.fori_loop(first, jnp.maximum(first, near_first), forward_blocks, 0)

    unit = (lax.broadcasted_iota(jnp.int32, (128, 128), 0)
            == lax.broadcasted_iota(jnp.int32, (128, 128), 1)).astype(jnp.bfloat16)

    def turned(block_t):
        return dot32(unit, block_t, NT).astype(jnp.bfloat16)

    for tile in range(tiles):
        for head in range(kv_heads):
            slot = head * tiles + tile
            total = sum_s[head][tile]
            max_s[head][tile] = max_s[head][tile] + jnp.log2(total)
            out_t = (acc_s[head][tile] / total).astype(jnp.bfloat16)
            first_col = head * group * 128
            do_t = jnp.concatenate(
                [dot_ref[first_col + member * 128:first_col + (member + 1) * 128, tile * QT:(tile + 1) * QT]
                 for member in range(group)], axis=1)
            delta_s[slot] = jnp.sum(do_t.astype(jnp.float32) * out_t.astype(jnp.float32), axis=0, keepdims=True)
            for member in range(group):
                col = first_col + member * 128
                o_ref[tile * QT:(tile + 1) * QT, col:col + 128] = turned(out_t[:, member * QT:(member + 1) * QT])

    def grads(tile, head, blk, keys, mask_fn):
        slot = head * tiles + tile
        q_tile = stack_heads(q_ref, tile, head, group)
        do_tile = stack_heads(do_ref, tile, head, group)
        k_blk = kv_ref[blk, 0:keys, k_cols(head)]
        v_blk = kv_ref[blk, 0:keys, v_cols(head)]
        scores = dot32(k_blk, q_tile, NT) * scale2
        if mask_fn is not None:
            scores = jnp.where(mask_fn(), scores, NEG_INF)
        prob = jnp.exp2(scores - max_s[head][tile])
        dprob = dot32(v_blk, do_tile, NT)
        dscore = (prob * (dprob - delta_s[slot])).astype(jnp.bfloat16)
        dv_part = dot32(prob.astype(jnp.bfloat16), do_tile, NN)
        dk_part = dot32(dscore, q_tile, NN)
        dq_part = dot32(k_blk, dscore, TN)
        return dq_part, dk_part, dv_part

    key_copy(me).wait()
    for tile in reversed(range(tiles)):
        keys = QT * (tile + 1)
        for head in range(kv_heads):
            dq_part, dk_part, dv_part = grads(tile, head, me, keys, functools.partial(diag_mask, tile, keys))
            acc_s[head][tile] = dq_part
            if tile == tiles - 1:
                grad_s[me, 0:keys, k_cols(head)] = dk_part
                grad_s[me, 0:keys, v_cols(head)] = dv_part
            else:
                grad_s[me, 0:keys, k_cols(head)] = grad_s[me, 0:keys, k_cols(head)] + dk_part
                grad_s[me, 0:keys, v_cols(head)] = grad_s[me, 0:keys, v_cols(head)] + dv_part
    grad_copy(me).start()

    def backward_body(tile, masked, blk):
        for head in range(kv_heads):
            slot = head * tiles + tile
            dq_part, dk_part, dv_part = grads(tile, head, blk, tok, functools.partial(off_mask, tile, blk) if masked else None)
            acc_s[head][tile] = acc_s[head][tile] + dq_part
            grad_s[blk, :, k_cols(head)] = grad_s[blk, :, k_cols(head)] + dk_part
            grad_s[blk, :, v_cols(head)] = grad_s[blk, :, v_cols(head)] + dv_part

    def backward_blocks(blk, carry):
        pl.when(blk >= near_first)(lambda: key_copy(blk).wait())
        grad_s[blk] = jnp.zeros(zero_s.shape, jnp.float32)
        over_tiles(backward_body, blk)
        grad_copy(blk).start()
        return carry

    lax.fori_loop(first, me, backward_blocks, 0)

    for tile in range(tiles):
        for head in range(kv_heads):
            grad_t = (acc_s[head][tile] * scale).astype(jnp.bfloat16)
            for member in range(group):
                col = (head * group + member) * 128
                dq_ref[tile * QT:(tile + 1) * QT, col:col + 128] = turned(grad_t[:, member * QT:(member + 1) * QT])

    def wait_body(blk, carry):
        zero_copy(blk).wait()
        return carry

    lax.fori_loop(0, blocks, wait_body, 0)


def places(n):
    me = lax.axis_index('cp')
    chips = n // 2
    core = lax.rem(me, 2)
    chip = me // 2

    def at(offset, which):
        return lax.rem(chip + offset + chips, chips) * 2 + which

    return me, chips, core, chip, at


def remote(src, dst, send_sem, recv_sem, target):
    return pltpu.make_async_remote_copy(src_ref=src, dst_ref=dst, send_sem=send_sem, recv_sem=recv_sem,
                                        device_id={'cp': target}, device_id_type=pl.DeviceIdType.MESH)


def greet(targets):
    barrier = pltpu.get_barrier_semaphore()
    for target in targets:
        pl.semaphore_signal(barrier, inc=1, device_id={'cp': target}, device_id_type=pl.DeviceIdType.MESH)
    pl.semaphore_wait(barrier, len(targets))


def gather_kernel(n, kv_heads, group, scale2, seg_ref, x_ref, dy_ref, wk_ref, wv_ref, wq_ref, wo_ref,
                  kv_out, wk_out, wv_out, seg_all_ref, q_out, do_out, dot_out, start_ref,
                  max0_ref, max1_ref, sum0_ref, sum1_ref, acc0_ref, acc1_ref,
                  kv_all_ref, q_ref, do_ref, dot_ref, flat_sem, block_sem, kv_s, wq_s, wo_s, load_sem, seg_send, seg_recv, ring_send, ring_recv, pair_send, pair_recv,
                  mate_send, mate_recv):
    me, chips, core, chip, at = places(n)
    mate = at(0, 1 - core)
    tok = kv_s.shape[0]
    tiles = tok // QT
    slice_rows = tok // SLICES
    reach = chips // 2
    stats = [(max0_ref, sum0_ref, acc0_ref), (max1_ref, sum1_ref, acc1_ref)]
    load_q = pltpu.make_async_copy(wq_ref, wq_s, load_sem.at[0])
    load_o = pltpu.make_async_copy(wo_ref, wo_s, load_sem.at[1])
    load_q.start()
    load_o.start()
    kv_own = jnp.concatenate([dot32(x_ref[...], wk_ref[...], NN), dot32(x_ref[...], wv_ref[...], NN)], axis=1).astype(jnp.bfloat16)
    kv_s[...] = kv_own
    kv_all_ref[me] = kv_own
    seg_all_ref[me] = seg_ref[...]
    greet([lax.rem(me + step, n) for step in range(1, n)])

    flat_outs = [pltpu.make_async_copy(src, dst, flat_sem.at[index]) for index, (src, dst) in enumerate(
        ((q_ref, q_out), (do_ref, do_out), (dot_ref, dot_out), (wk_ref, wk_out), (wv_ref, wv_out)))]

    def block_out(blk):
        return pltpu.make_async_copy(kv_all_ref.at[blk], kv_out.at[blk], block_sem.at[blk])

    def rows(sub):
        return pl.ds(pl.multiple_of(sub * slice_rows, slice_rows), slice_rows)

    def ring_copy(way, sub, hop):
        offset = 1 - hop if way == 0 else hop - 1
        spot = kv_all_ref.at[at(offset, core), rows(sub)]
        return remote(spot, spot, ring_send.at[way, sub, hop - 1], ring_recv.at[way, sub, hop - 1],
                      at(1 if way == 0 else -1, core))

    def pair_copy(way, sub, hop):
        spot = kv_all_ref.at[at(-hop if way == 0 else hop, core), rows(sub)]
        return remote(spot, spot, pair_send.at[way, sub, hop - 1], pair_recv.at[way, sub, hop - 1], mate)

    def seg_copy(step):
        return remote(seg_ref, seg_all_ref.at[me], seg_send.at[step - 1], seg_recv.at[step - 1], lax.rem(me + step, n))

    def own_copy():
        return remote(kv_s, kv_all_ref.at[me], mate_send.at[0], mate_recv.at[0], mate)

    for sub in range(SLICES):
        for way in range(2):
            ring_copy(way, sub, 1).start()
    own_copy().start()
    for step in range(1, n):
        seg_copy(step).start()

    pairs = wq_s.shape[0] // 2

    def project(src_ref, w_s, dst_ref, pair):
        w_pair = jnp.concatenate([w_s[2 * pair], w_s[2 * pair + 1]], axis=1)
        cols = pl.ds(pl.multiple_of(pair * 256, 256), 256)
        value = dot32(src_ref[...], w_pair, NN).astype(jnp.bfloat16)
        dst_ref[:, cols] = value
        return value

    def query_pair(pair, carry):
        project(x_ref, wq_s, q_ref, pair)
        return carry

    load_q.wait()
    lax.fori_loop(0, pairs, query_pair, 0)

    for step in range(1, n):
        seg_copy(step).wait_recv()
    seg_own = seg_ref[...]
    first_seg = jnp.min(seg_own)
    shard_index = lax.broadcasted_iota(jnp.int32, seg_all_ref.shape, 0)
    earlier = (shard_index < me) & (seg_all_ref[...] < first_seg)
    doc_start = jnp.sum(earlier.astype(jnp.int32))
    seg_wide = seg_own.astype(jnp.float32)
    columns = [jnp.broadcast_to(seg_wide[part:part + 1, :], (128, 128)).T for part in range(tok // 128)]
    for tile in range(tiles):
        count = sum(jnp.sum((column < seg_wide[tile:tile + 1, :]).astype(jnp.int32), axis=0, keepdims=True)
                    for column in columns)
        row = jnp.where(count == 0, doc_start - me * tok, count)
        start_ref[tile] = jnp.concatenate([row] * group, axis=1)

    for tile in range(tiles):
        forward_update(kv_heads, group, scale2, tile, q_ref, kv_all_ref, me, stats, start_ref[tile], QT * (tile + 1), True)
    load_o.wait()
    flat_outs[0].start()
    flat_outs[3].start()
    flat_outs[4].start()

    def tick_body(tick, carry):
        step, sub = tick // SLICES, lax.rem(tick, SLICES)
        for way in range(2):
            last = (sub < SLICES // 2) if way == 0 else (sub >= SLICES // 2)

            @pl.when((step < reach - 1) | last)
            def _():
                ring_copy(way, sub, step + 1).wait_recv()
                pair_copy(way, sub, step + 1).start()

            @pl.when((step < reach - 2) | ((step == reach - 2) & last))
            def _():
                ring_copy(way, sub, step + 2).start()

        @pl.when((step == 0) & (sub == 0))
        def _():
            own_copy().wait_recv()

        @pl.when((step > 0) & (sub == 0))
        def _():
            for piece in range(SLICES):
                pair_copy(0, piece, step).wait_recv()

        @pl.when(sub == 0)
        def _():
            for which in range(2):
                block_out(at(-step, which)).start()

        spread = reach * SLICES // pairs

        @pl.when(lax.rem(tick, spread) == 0)
        def _():
            pair = tick // spread
            value = project(dy_ref, wo_s, do_ref, pair)
            dot_ref[pl.ds(pl.multiple_of(pair * 256, 256), 256), :] = value.T

        def near_tile(item, inner):
            side = item // tiles
            tile = lax.rem(item, tiles)

            @pl.when((chip >= step) & ((step > 0) | ((core == 1) & (side == 0))))
            def _():
                blk = 2 * (chip - step) + side
                forward_update(kv_heads, group, scale2, tile, q_ref, kv_all_ref, blk, stats,
                               start_ref[tile] + (me - blk) * tok)
            return inner

        share = 2 * tiles // SLICES
        lax.fori_loop(sub * share, (sub + 1) * share, near_tile, 0)
        return carry

    lax.fori_loop(0, reach * SLICES, tick_body, 0)
    flat_outs[1].start()
    flat_outs[2].start()
    for way in range(2):
        for sub in range(SLICES):
            for hop in range(1, reach + 1):
                if hop < reach or (sub < SLICES // 2) == (way == 0):
                    if way == 1 or hop == reach:
                        pair_copy(way, sub, hop).wait_recv()
                    pair_copy(way, sub, hop).wait_send()
                    ring_copy(way, sub, hop).wait_send()
    for offset in range(1, chips - reach + 1):
        for which in range(2):
            block_out(at(offset, which)).start()
    own_copy().wait_send()
    for step in range(1, n):
        seg_copy(step).wait_send()
    for copy in flat_outs:
        copy.wait()
    for blk in range(n):
        block_out(blk).wait()


def reduce_kernel(n, scale, kv_width, dkv_ref, o_hbm, dq_hbm, x_hbm, dy_hbm, wk_hbm, wv_hbm, wq_ref, wo_ref,
                  y_ref, dx_ref, dwo_ref, dwq_ref, dwk_ref, dwv_ref,
                  o_ref, dq_ref, x_ref, dy_ref, wkv_ref, xt_ref, dyt_ref, xtp_ref, dytp_ref,
                  own_s, mate_s, slot1_s, stage1_s, grad_s, grad_mate_s, o_mate_s, dq_mate_s, slot2_s, stage2_s,
                  wq_s, wo_s, load_sem, block_sem, mate_send, mate_recv, ring_send, ring_recv, extra_send, extra_recv):
    me, chips, core, chip, at = places(n)
    mate = at(0, 1 - core)
    ring = (at(1, core), at(-1, core))
    tok = o_ref.shape[0]
    quarter = tok // 4
    heads, out_rows, head_dim = dwo_ref.shape
    loads = [pltpu.make_async_copy(src, dst, load_sem.at[index]) for index, (src, dst) in enumerate(
        ((o_hbm, o_ref), (dq_hbm, dq_ref), (x_hbm, x_ref), (dy_hbm, dy_ref), (wo_ref, wo_s), (wq_ref, wq_s),
         (wk_hbm, wkv_ref.at[:, 0:kv_width]), (wv_hbm, wkv_ref.at[:, kv_width:2 * kv_width])))]
    order = []
    for step in range(1, chips):
        for offset in (-step, step):
            if offset % chips not in order:
                order.append(offset % chips)
    order.append(0)
    own_loads = [pltpu.make_async_copy(dkv_ref.at[at(offset, core)], own_s.at[index], block_sem.at[index])
                 for index, offset in enumerate(order)]
    for load in own_loads:
        load.start()
    for load in loads:
        load.start()
    greet([ring[0], ring[1], mate])
    halves = [pl.ds(way * (tok // 2), tok // 2) for way in range(2)]
    mate_copies = [[remote(dkv_ref.at[at(offset, 1 - core), halves[way]], mate_s.at[index, halves[way]],
                           mate_send.at[index, way], mate_recv.at[index, way], mate) for way in range(2)]
                   for index, offset in enumerate(order)]
    extras = [remote(o_hbm, o_mate_s, extra_send.at[0], extra_recv.at[0], mate),
              remote(dq_hbm, dq_mate_s, extra_send.at[1], extra_recv.at[1], mate),
              remote(grad_s, grad_mate_s, extra_send.at[2], extra_recv.at[2], mate),
              remote(xt_ref, xtp_ref, extra_send.at[3], extra_recv.at[3], mate),
              remote(dyt_ref, dytp_ref, extra_send.at[4], extra_recv.at[4], mate)]
    mate_copies[0][0].start()
    mate_copies[1][1].start()
    mate_copies[0][1].start()
    mate_copies[1][0].start()
    for index in range(2, len(order)):
        for copy in mate_copies[index]:
            copy.start()
        if index == 3:
            extras[0].start()
            extras[1].start()

    ready = set()

    def need(position, way):
        if position not in ready:
            ready.add(position)
            own_loads[position].wait()
        mate_copies[position][way].wait_recv()

    def ring_copy(job, way, sub, step):
        slots, stage = (slot1_s, stage1_s) if job == 0 else (slot2_s, stage2_s)
        src = stage.at[way, sub] if step == 0 else slots.at[way, sub, step - 1]
        return remote(src, slots.at[way, sub, step], ring_send.at[job, way, sub, step], ring_recv.at[job, way, sub, step],
                      ring[way])

    started = []

    def send(job, way, sub, step):
        started.append(ring_copy(job, way, sub, step))
        started[-1].start()

    def contrib1(way, sub, step):
        offset = (-(1 + step) if way == 0 else 1 + step) % chips
        position = order.index(offset)
        if sub == 0:
            need(position, way)
        span = slice((2 * way + sub) * quarter, (2 * way + sub + 1) * quarter)
        return own_s[position, span, :] + mate_s[position, span, :]

    cut = 7 * head_dim

    def contrib2(way, sub, step):
        offset = -(1 + step) if way == 0 else 1 + step
        first_row = pl.multiple_of(at(offset % chips, core) * out_rows, 32)
        take = pl.ds(first_row, out_rows)
        lhs, lhs_mate = (dyt_ref, dytp_ref) if way == 0 else (xt_ref, xtp_ref)
        rhs, rhs_mate = (o_ref, o_mate_s) if way == 0 else (dq_ref, dq_mate_s)
        if sub == 0:
            return (dot32(lhs[take, :], rhs[:, 0:cut], NN) + dot32(lhs_mate[take, :], rhs_mate[:, 0:cut], NN))
        main = dot32(lhs[take, :], rhs[:, cut:], NN) + dot32(lhs_mate[take, :], rhs_mate[:, cut:], NN)
        cols = slice(way * kv_width, (way + 1) * kv_width)
        side = dot32(xt_ref[take, :], grad_s[:, cols], NN) + dot32(xtp_ref[take, :], grad_mate_s[:, cols], NN)
        return jnp.concatenate([main, side], axis=1)

    strip = 256
    strips = y_ref.shape[1] // strip

    def rows_out(part):
        return pl.ds(pl.multiple_of(part * strip, strip), strip)

    def times_weight(src_ref, w_s, part):
        total = None
        for pair in range(heads // 2):
            w_pair = jnp.concatenate([w_s[2 * pair, rows_out(part), :], w_s[2 * pair + 1, rows_out(part), :]], axis=1)
            piece = dot32(src_ref[:, pair * 256:(pair + 1) * 256], w_pair, NT)
            total = piece if total is None else total + piece
        return total

    def y_strip(part, carry):
        y_ref[:, rows_out(part)] = times_weight(o_ref, wo_s, part).astype(jnp.bfloat16)
        return carry

    def flip_strip(part, carry):
        xt_ref[rows_out(part), :] = x_ref[:, rows_out(part)].T
        dyt_ref[rows_out(part), :] = dy_ref[:, rows_out(part)].T
        return carry

    def dx_strip(part, carry):
        wide = times_weight(dq_ref, wq_s, part) + dot32(grad_s[...], wkv_ref[rows_out(part), :], NT)
        dx_ref[:, rows_out(part)] = wide.astype(jnp.bfloat16)
        return carry

    steps = chips - 1
    both = [(sub, way) for sub in range(2) for way in range(2)]
    for sub, way in both:
        stage1_s[way, sub] = contrib1(way, sub, 0)
        send(0, way, sub, 0)
    for load in loads:
        load.wait()
    for step in range(steps):
        if step == 0:
            lax.fori_loop(0, strips, y_strip, 0)
        if step == 1:
            lax.fori_loop(0, strips, flip_strip, 0)
        if step == 4:
            extras[3].start()
            extras[4].start()
        if step == steps - 1:
            for index in (0, 1, 3, 4):
                extras[index].wait_recv()
            for way in range(2):
                stage2_s[way, 0] = contrib2(way, 0, 0)
                send(1, way, 0, 0)
        for sub, way in both:
            part = contrib1(way, sub, step + 1)
            ring_copy(0, way, sub, step).wait_recv()
            if step < steps - 1:
                slot1_s[way, sub, step] = slot1_s[way, sub, step] + part
                send(0, way, sub, step + 1)
            else:
                span = slice((2 * way + sub) * quarter, (2 * way + sub + 1) * quarter)
                total = slot1_s[way, sub, step] + part
                grad_s[span, 0:kv_width] = (total[:, 0:kv_width] * scale).astype(jnp.bfloat16)
                grad_s[span, kv_width:] = total[:, kv_width:].astype(jnp.bfloat16)
    extras[2].start()
    extras[2].wait_recv()
    for way in range(2):
        stage2_s[way, 1] = contrib2(way, 1, 0)
        send(1, way, 1, 0)
    for step in range(steps):
        if step == 0:
            lax.fori_loop(0, strips, dx_strip, 0)
        for sub, way in both:
            part = contrib2(way, sub, step + 1)
            ring_copy(1, way, sub, step).wait_recv()
            if step < steps - 1:
                slot2_s[way, sub, step] = slot2_s[way, sub, step] + part
                send(1, way, sub, step + 1)
            else:
                total = slot2_s[way, sub, step] + part
                out_ref = dwo_ref if way == 0 else dwq_ref
                base = 0 if sub == 0 else cut // head_dim
                for index in range(cut // head_dim if sub == 0 else heads - cut // head_dim):
                    out_ref[base + index] = total[:, index * head_dim:(index + 1) * head_dim]
                if sub == 1:
                    side_ref = dwk_ref if way == 0 else dwv_ref
                    for index in range(kv_width // head_dim):
                        base = heads * head_dim - cut + index * head_dim
                        side_ref[:, index, :] = total[:, base:base + head_dim]
    for copy in started + mate_copies[0] + sum(mate_copies[1:], []) + extras:
        copy.wait_send()


VMEM_SPEC = pl.BlockSpec(memory_space=pltpu.VMEM)
ANY_SPEC = pl.BlockSpec(memory_space=pl.ANY)
VMEM_LIMIT = 60 * 1024 * 1024
REDUCE_LIMIT = 67043328


def solution(mesh):
    group_count = mesh.shape['cp']
    row_spec = P(('dp', 'cp'), None)
    tok_spec = P(('dp', 'cp'))
    weight_spec = P(None, None, None)
    grad_spec = P(('dp', 'cp'), None, None)

    def local_step(x_act, seg_ids, w_q, w_k, w_v, w_o, dy_act):
        tok = x_act.shape[0]
        model_dim, q_heads, head_dim = w_q.shape
        kv_heads = w_k.shape[1]
        group = q_heads // kv_heads
        q_width = q_heads * head_dim
        kv_width = kv_heads * head_dim
        tiles = tok // QT
        scale = head_dim ** -0.5
        bf16 = jnp.bfloat16

        wk_flat, wv_flat = w_k.reshape(model_dim, kv_width), w_v.reshape(model_dim, kv_width)
        seg_rows = seg_ids.reshape(tok // 128, 128)
        wq_heads = w_q.transpose(1, 0, 2)
        wo_heads = w_o.transpose(1, 0, 2)

        slots = kv_heads * tiles
        width = group * QT
        chips = group_count // 2
        reach = chips // 2
        dma = pltpu.SemaphoreType.DMA
        f32 = jnp.float32
        shape = jax.ShapeDtypeStruct
        flat = shape((tok, q_width), bf16)
        row32 = shape((tiles, 1, width), f32)
        wide32 = shape((tiles, head_dim, width), f32)
        kv_all, wk_kept, wv_kept, seg_all, q_loc, do_loc, do_turned, *kept = pl.pallas_call(
            functools.partial(gather_kernel, group_count, kv_heads, group, scale * LOG2E),
            out_shape=(shape((group_count, tok, 2 * kv_width), bf16), shape((model_dim, kv_width), bf16), shape((model_dim, kv_width), bf16),
                       shape((group_count, tok // 128, 128), jnp.int32),
                       flat, flat, shape((q_width, tok), bf16), shape((tiles, 1, width), jnp.int32),
                       row32, row32, row32, row32, wide32, wide32),
            in_specs=[VMEM_SPEC] * 5 + [ANY_SPEC] * 2,
            out_specs=(ANY_SPEC, ANY_SPEC, ANY_SPEC, VMEM_SPEC) + (ANY_SPEC,) * 3 + (VMEM_SPEC,) * 7,
            scratch_shapes=[pltpu.VMEM((group_count, tok, 2 * kv_width), bf16), pltpu.VMEM((tok, q_width), bf16),
                            pltpu.VMEM((tok, q_width), bf16), pltpu.VMEM((q_width, tok), bf16),
                            dma((5,)), dma((group_count,)), pltpu.VMEM((tok, 2 * kv_width), bf16), pltpu.VMEM((q_heads, model_dim, head_dim), bf16),
                            pltpu.VMEM((q_heads, model_dim, head_dim), bf16),
                            dma((2,)), dma((group_count - 1,)), dma((group_count - 1,)),
                            dma((2, SLICES, reach)), dma((2, SLICES, reach)), dma((2, SLICES, reach)), dma((2, SLICES, reach)), dma((1,)), dma((1,))],
            compiler_params=pltpu.CompilerParams(collective_id=0, has_side_effects=True, vmem_limit_bytes=VMEM_LIMIT),
            cost_estimate=pl.CostEstimate(flops=8 * tok * model_dim * q_width, bytes_accessed=2**24, transcendentals=0),
            name='gather_keys',
        )(seg_rows, x_act, dy_act, wk_flat, wv_flat, wq_heads, wo_heads)

        o_loc, dq_loc, dkv_all = pl.pallas_call(
            functools.partial(attention_kernel, kv_heads, group, scale),
            out_shape=(flat, flat, shape((group_count, tok, 2 * kv_width), f32)),
            in_specs=[VMEM_SPEC] * 5 + [ANY_SPEC] + [VMEM_SPEC] * 7,
            out_specs=(VMEM_SPEC, VMEM_SPEC, ANY_SPEC),
            scratch_shapes=[pltpu.VMEM((tiles, 1, width), f32)] * 4
                           + [pltpu.VMEM((slots, 1, width), f32)] + [pltpu.VMEM((tiles, head_dim, width), f32)] * 2
                           + [pltpu.VMEM((group_count, tok, 2 * kv_width), f32),
                            pltpu.VMEM((tok, 2 * kv_width), f32), dma((group_count,)),
                            pltpu.VMEM((group_count, tok, 2 * kv_width), bf16), dma((group_count,))],
            compiler_params=pltpu.CompilerParams(vmem_limit_bytes=VMEM_LIMIT),
            cost_estimate=pl.CostEstimate(flops=16 * 14 * tok * tok * q_width, bytes_accessed=2**25, transcendentals=0),
            name='attend',
        )(seg_rows, seg_all, q_loc, do_loc, do_turned, kv_all, *kept)

        out_rows = model_dim // group_count
        blk = (tok, 2 * kv_width)
        cols2 = (q_width + kv_width) // 2
        steps = chips - 1
        head_grad = shape((q_heads, out_rows, head_dim), f32)
        y_out, dx_out, dwo, dwq, dwk, dwv = pl.pallas_call(
            functools.partial(reduce_kernel, group_count, scale, kv_width),
            out_shape=(shape((tok, model_dim), bf16), shape((tok, model_dim), bf16), head_grad, head_grad,
                       shape((out_rows, kv_heads, head_dim), f32), shape((out_rows, kv_heads, head_dim), f32)),
            in_specs=[ANY_SPEC] * 9,
            out_specs=(VMEM_SPEC,) * 6,
            scratch_shapes=[pltpu.VMEM((tok, q_width), bf16), pltpu.VMEM((tok, q_width), bf16),
                            pltpu.VMEM((tok, model_dim), bf16), pltpu.VMEM((tok, model_dim), bf16),
                            pltpu.VMEM((model_dim, 2 * kv_width), bf16),
                            pltpu.VMEM((model_dim, tok), bf16), pltpu.VMEM((model_dim, tok), bf16),
                            pltpu.VMEM((model_dim, tok), bf16), pltpu.VMEM((model_dim, tok), bf16),
                            pltpu.VMEM((chips,) + blk, f32), pltpu.VMEM((chips,) + blk, f32),
                            pltpu.VMEM((2, 2, steps, tok // 4, 2 * kv_width), f32), pltpu.VMEM((2, 2, tok // 4, 2 * kv_width), f32),
                            pltpu.VMEM(blk, bf16), pltpu.VMEM(blk, bf16),
                            pltpu.VMEM((tok, q_width), bf16), pltpu.VMEM((tok, q_width), bf16),
                            pltpu.VMEM((2, 2, steps, out_rows, cols2), f32), pltpu.VMEM((2, 2, out_rows, cols2), f32),
                            pltpu.VMEM((q_heads, model_dim, head_dim), bf16), pltpu.VMEM((q_heads, model_dim, head_dim), bf16),
                            dma((8,)), dma((chips,)), dma((chips, 2)), dma((chips, 2)),
                            dma((2, 2, 2, steps)), dma((2, 2, 2, steps)), dma((5,)), dma((5,))],
            compiler_params=pltpu.CompilerParams(collective_id=1, has_side_effects=True, vmem_limit_bytes=REDUCE_LIMIT),
            cost_estimate=pl.CostEstimate(flops=16 * tok * model_dim * q_width, bytes_accessed=2**25, transcendentals=0),
            name='reduce_grads',
        )(dkv_all, o_loc, dq_loc, x_act, dy_act, wk_kept, wv_kept, wq_heads, wo_heads)
        return y_out, dx_out, dwq.transpose(1, 0, 2), dwk, dwv, dwo.transpose(1, 0, 2)

    return jax.shard_map(local_step, mesh=mesh,
                         in_specs=(row_spec, tok_spec, weight_spec, weight_spec, weight_spec, weight_spec, row_spec),
                         out_specs=(row_spec, row_spec, grad_spec, grad_spec, grad_spec, grad_spec),
                         check_vma=False)
```

```python
import functools

import jax
import jax.numpy as jnp
from jax import lax
from jax.experimental import pallas as pl
from jax.experimental.pallas import tpu as pltpu
from jax.sharding import PartitionSpec as P

QT = 128
SLICES = 3
LOG2E = 1.4426950408889634
NEG_INF = float('-inf')
NT = (((1,), (1,)), ((), ()))
TN = (((0,), (0,)), ((), ()))
NN = (((1,), (0,)), ((), ()))


def dot32(left_arg, right_arg, dims):
    return lax.dot_general(left_arg, right_arg, dims, preferred_element_type=jnp.float32)


def stack_heads(ref, tile, head, group):
    rows = pl.ds(pl.multiple_of(tile * QT, QT), QT)
    return jnp.concatenate(
        [ref[rows, (head * group + member) * 128:(head * group + member + 1) * 128] for member in range(group)], axis=0)


def member_rows(ref, tile, head, group, chunk):
    rows = pl.ds(pl.multiple_of(tile * QT, QT), QT)
    first = (head * group + 2 * chunk) * 128
    return jnp.concatenate([ref[rows, first:first + 128], ref[rows, first + 128:first + 256]], axis=0)


def forward_update(kv_heads, group, scale2, tile, q_ref, kv_ref, blk, stats, mask_row, keys=None, diag=False):
    keys = kv_ref.shape[1] if keys is None else keys
    chains = [(head, chunk) for chunk in range(group // 2) for head in range(kv_heads)]
    k_blks = [kv_ref[blk, 0:keys, head * 128:(head + 1) * 128] for head in range(kv_heads)]
    v_turned = [kv_ref[blk, 0:keys, (kv_heads + head) * 128:(kv_heads + head + 1) * 128].T for head in range(kv_heads)]
    old = [None if diag else (stats[head][0][tile], stats[head][1][tile]) for head in range(kv_heads)]
    new_rows = [([], []) for head in range(kv_heads)]

    def score(chain):
        head, chunk = chain
        return dot32(k_blks[head], member_rows(q_ref, tile, head, group, chunk), NT)

    pending = [score(chain) for chain in chains[:6]]
    for index, (head, chunk) in enumerate(chains):
        scores = pending.pop(0)
        if index + 6 < len(chains):
            pending.append(score(chains[index + 6]))
        cols = slice(chunk * 256, (chunk + 1) * 256)
        if mask_row is not None:
            key_pos = lax.broadcasted_iota(jnp.int32, (keys, 256), 0)
            allowed = key_pos >= mask_row[:, cols]
            if diag:
                query_pos = lax.rem(lax.broadcasted_iota(jnp.int32, (1, 256), 1), QT) + tile * QT
                allowed = allowed & (key_pos <= query_pos)
            scores = jnp.where(allowed, scores, NEG_INF)
        new_max = jnp.max(scores, axis=0, keepdims=True) * scale2
        if not diag:
            old_max = old[head][0][:, cols]
            new_max = jnp.maximum(old_max, new_max)
        weights = jnp.exp2(scores * scale2 - new_max)
        total = jnp.sum(weights, axis=0, keepdims=True)
        part = dot32(v_turned[head], weights.astype(jnp.bfloat16), NN)
        acc = stats[head][2]
        if diag:
            acc[tile, :, cols] = part
        else:
            factor = jnp.exp2(old_max - new_max)
            total = old[head][1][:, cols] * factor + total
            acc[tile, :, cols] = acc[tile, :, cols] * factor + part
        new_rows[head][0].append(new_max)
        new_rows[head][1].append(total)
    for head in range(kv_heads):
        stats[head][0][tile] = jnp.concatenate(new_rows[head][0], axis=1)
        stats[head][1][tile] = jnp.concatenate(new_rows[head][1], axis=1)


def attention_kernel(kv_heads, group, scale, seg_ref, seg_all_ref, q_ref, do_ref, dot_ref, kv_hbm, start_s,
                     max0_ref, max1_ref, sum0_ref, sum1_ref, acc0_ref, acc1_ref,
                     o_ref, dq_ref, dkv_ref, max0_s, max1_s, sum0_s, sum1_s, delta_s, acc0_s, acc1_s,
                     grad_s, zero_s, out_sem,
                     kv_ref, in_sem):
    tok = q_ref.shape[0]
    blocks = kv_ref.shape[0]
    tiles = tok // QT
    width = group * QT
    scale2 = scale * LOG2E
    max_s, sum_s, acc_s = (max0_s, max1_s), (sum0_s, sum1_s), (acc0_s, acc1_s)
    stats = [(max_s[head], sum_s[head], acc_s[head]) for head in range(kv_heads)]
    me = lax.axis_index('cp')
    near_first = jnp.maximum(2 * (me // 2 - (blocks // 4 - 1)), 0)
    for kept_ref, kept_s in ((max0_ref, max0_s), (max1_ref, max1_s), (sum0_ref, sum0_s), (sum1_ref, sum1_s),
                             (acc0_ref, acc0_s), (acc1_ref, acc1_s)):
        kept_s[...] = kept_ref[...]
    zero_s[...] = jnp.zeros(zero_s.shape, jnp.float32)

    seg_own = seg_ref[...]
    first_seg = jnp.min(seg_own)
    head_count = jnp.sum((seg_own == first_seg).astype(jnp.int32))
    shard_index = lax.broadcasted_iota(jnp.int32, seg_all_ref.shape, 0)
    earlier = (shard_index < me) & (seg_all_ref[...] < first_seg)
    doc_start = jnp.sum(earlier.astype(jnp.int32))
    first = doc_start // tok
    has_prev = doc_start < me * tok
    tiles_prev = jnp.where(has_prev, (head_count + QT - 1) // QT, 0)
    full_tiles = head_count // QT

    def key_copy(blk):
        return pltpu.make_async_copy(kv_hbm.at[blk], kv_ref.at[blk], in_sem.at[blk])

    def key_body(blk, carry):
        key_copy(blk).start()
        return carry

    lax.fori_loop(first, me + 1, key_body, 0)

    def zero_copy(blk):
        return pltpu.make_async_copy(zero_s, dkv_ref.at[blk], out_sem.at[blk])

    def grad_copy(blk):
        return pltpu.make_async_copy(grad_s.at[blk], dkv_ref.at[blk], out_sem.at[blk])

    def clear_body(blk, carry):
        zero_copy(blk).start()
        return carry

    lax.fori_loop(0, first, clear_body, 0)
    lax.fori_loop(me + 1, blocks, clear_body, 0)

    def k_cols(head):
        return slice(head * 128, (head + 1) * 128)

    def v_cols(head):
        return slice((kv_heads + head) * 128, (kv_heads + head + 1) * 128)

    def diag_mask(tile, keys):
        key_pos = lax.broadcasted_iota(jnp.int32, (keys, width), 0)
        query_pos = lax.rem(lax.broadcasted_iota(jnp.int32, (1, width), 1), QT) + tile * QT
        return (key_pos <= query_pos) & (key_pos >= start_s[tile])

    def off_mask(tile, blk):
        key_pos = lax.broadcasted_iota(jnp.int32, (tok, width), 0)
        return key_pos >= start_s[tile] + (me - blk) * tok

    def over_tiles(body, blk):
        def tile_body(tile, carry):
            masked = (blk == first) | (tile >= full_tiles)
            pl.when(masked)(functools.partial(body, tile, True, blk))
            pl.when(jnp.logical_not(masked))(functools.partial(body, tile, False, blk))
            return carry
        lax.fori_loop(0, tiles_prev, tile_body, 0)

    def forward_body(tile, masked, blk):
        row = start_s[tile] + (me - blk) * tok if masked else None
        forward_update(kv_heads, group, scale2, tile, q_ref, kv_ref, blk, stats, row)

    def forward_blocks(blk, carry):
        key_copy(blk).wait()
        over_tiles(forward_body, blk)
        return carry

    lax.fori_loop(first, jnp.maximum(first, near_first), forward_blocks, 0)

    unit = (lax.broadcasted_iota(jnp.int32, (128, 128), 0)
            == lax.broadcasted_iota(jnp.int32, (128, 128), 1)).astype(jnp.bfloat16)

    def turned(block_t):
        return dot32(unit, block_t, NT).astype(jnp.bfloat16)

    for tile in range(tiles):
        for head in range(kv_heads):
            slot = head * tiles + tile
            total = sum_s[head][tile]
            max_s[head][tile] = max_s[head][tile] + jnp.log2(total)
            out_t = (acc_s[head][tile] / total).astype(jnp.bfloat16)
            first_col = head * group * 128
            do_t = jnp.concatenate(
                [dot_ref[first_col + member * 128:first_col + (member + 1) * 128, tile * QT:(tile + 1) * QT]
                 for member in range(group)], axis=1)
            delta_s[slot] = jnp.sum(do_t.astype(jnp.float32) * out_t.astype(jnp.float32), axis=0, keepdims=True)
            for member in range(group):
                col = first_col + member * 128
                o_ref[tile * QT:(tile + 1) * QT, col:col + 128] = turned(out_t[:, member * QT:(member + 1) * QT])

    def grads(tile, head, blk, keys, mask_fn):
        slot = head * tiles + tile
        q_tile = stack_heads(q_ref, tile, head, group)
        do_tile = stack_heads(do_ref, tile, head, group)
        k_blk = kv_ref[blk, 0:keys, k_cols(head)]
        v_blk = kv_ref[blk, 0:keys, v_cols(head)]
        scores = dot32(k_blk, q_tile, NT) * scale2
        if mask_fn is not None:
            scores = jnp.where(mask_fn(), scores, NEG_INF)
        prob = jnp.exp2(scores - max_s[head][tile])
        dprob = dot32(v_blk, do_tile, NT)
        dscore = (prob * (dprob - delta_s[slot])).astype(jnp.bfloat16)
        dv_part = dot32(prob.astype(jnp.bfloat16), do_tile, NN)
        dk_part = dot32(dscore, q_tile, NN)
        dq_part = dot32(k_blk, dscore, TN)
        return dq_part, dk_part, dv_part

    key_copy(me).wait()
    for tile in reversed(range(tiles)):
        keys = QT * (tile + 1)
        for head in range(kv_heads):
            dq_part, dk_part, dv_part = grads(tile, head, me, keys, functools.partial(diag_mask, tile, keys))
            acc_s[head][tile] = dq_part
            if tile == tiles - 1:
                grad_s[me, 0:keys, k_cols(head)] = dk_part
                grad_s[me, 0:keys, v_cols(head)] = dv_part
            else:
                grad_s[me, 0:keys, k_cols(head)] = grad_s[me, 0:keys, k_cols(head)] + dk_part
                grad_s[me, 0:keys, v_cols(head)] = grad_s[me, 0:keys, v_cols(head)] + dv_part
    grad_copy(me).start()

    def backward_body(tile, masked, blk):
        for head in range(kv_heads):
            slot = head * tiles + tile
            dq_part, dk_part, dv_part = grads(tile, head, blk, tok, functools.partial(off_mask, tile, blk) if masked else None)
            acc_s[head][tile] = acc_s[head][tile] + dq_part
            grad_s[blk, :, k_cols(head)] = grad_s[blk, :, k_cols(head)] + dk_part
            grad_s[blk, :, v_cols(head)] = grad_s[blk, :, v_cols(head)] + dv_part

    def backward_blocks(blk, carry):
        pl.when(blk >= near_first)(lambda: key_copy(blk).wait())
        grad_s[blk] = jnp.zeros(zero_s.shape, jnp.float32)
        over_tiles(backward_body, blk)
        grad_copy(blk).start()
        return carry

    lax.fori_loop(first, me, backward_blocks, 0)

    for tile in range(tiles):
        for head in range(kv_heads):
            grad_t = (acc_s[head][tile] * scale).astype(jnp.bfloat16)
            for member in range(group):
                col = (head * group + member) * 128
                dq_ref[tile * QT:(tile + 1) * QT, col:col + 128] = turned(grad_t[:, member * QT:(member + 1) * QT])

    def wait_body(blk, carry):
        zero_copy(blk).wait()
        return carry

    lax.fori_loop(0, blocks, wait_body, 0)


def places(n):
    me = lax.axis_index('cp')
    chips = n // 2
    core = lax.rem(me, 2)
    chip = me // 2

    def at(offset, which):
        return lax.rem(chip + offset + chips, chips) * 2 + which

    return me, chips, core, chip, at


def remote(src, dst, send_sem, recv_sem, target):
    return pltpu.make_async_remote_copy(src_ref=src, dst_ref=dst, send_sem=send_sem, recv_sem=recv_sem,
                                        device_id={'cp': target}, device_id_type=pl.DeviceIdType.MESH)


def greet(targets):
    barrier = pltpu.get_barrier_semaphore()
    for target in targets:
        pl.semaphore_signal(barrier, inc=1, device_id={'cp': target}, device_id_type=pl.DeviceIdType.MESH)
    pl.semaphore_wait(barrier, len(targets))


def gather_kernel(n, kv_heads, group, scale2, seg_ref, x_ref, dy_ref, wk_ref, wv_ref, wq_ref, wo_ref,
                  kv_out, wk_out, wv_out, seg_all_ref, q_out, do_out, dot_out, start_ref,
                  max0_ref, max1_ref, sum0_ref, sum1_ref, acc0_ref, acc1_ref,
                  kv_all_ref, q_ref, do_ref, dot_ref, flat_sem, block_sem, kv_s, wq_s, wo_s, load_sem, seg_send, seg_recv, ring_send, ring_recv, pair_send, pair_recv,
                  mate_send, mate_recv):
    me, chips, core, chip, at = places(n)
    mate = at(0, 1 - core)
    tok = kv_s.shape[0]
    tiles = tok // QT
    slice_rows = tok // SLICES
    reach = chips // 2
    stats = [(max0_ref, sum0_ref, acc0_ref), (max1_ref, sum1_ref, acc1_ref)]
    load_q = pltpu.make_async_copy(wq_ref, wq_s, load_sem.at[0])
    load_o = pltpu.make_async_copy(wo_ref, wo_s, load_sem.at[1])
    load_q.start()
    load_o.start()
    kv_own = jnp.concatenate([dot32(x_ref[...], wk_ref[...], NN), dot32(x_ref[...], wv_ref[...], NN)], axis=1).astype(jnp.bfloat16)
    kv_s[...] = kv_own
    kv_all_ref[me] = kv_own
    seg_all_ref[me] = seg_ref[...]
    greet([lax.rem(me + step, n) for step in range(1, n)])

    flat_outs = [pltpu.make_async_copy(src, dst, flat_sem.at[index]) for index, (src, dst) in enumerate(
        ((q_ref, q_out), (do_ref, do_out), (dot_ref, dot_out), (wk_ref, wk_out), (wv_ref, wv_out)))]

    def block_out(blk):
        return pltpu.make_async_copy(kv_all_ref.at[blk], kv_out.at[blk], block_sem.at[blk])

    def rows(sub):
        return pl.ds(pl.multiple_of(sub * slice_rows, slice_rows), slice_rows)

    def ring_copy(way, sub, hop):
        offset = 1 - hop if way == 0 else hop - 1
        spot = kv_all_ref.at[at(offset, core), rows(sub)]
        return remote(spot, spot, ring_send.at[way, sub, hop - 1], ring_recv.at[way, sub, hop - 1],
                      at(1 if way == 0 else -1, core))

    def pair_copy(way, sub, hop):
        spot = kv_all_ref.at[at(-hop if way == 0 else hop, core), rows(sub)]
        return remote(spot, spot, pair_send.at[way, sub, hop - 1], pair_recv.at[way, sub, hop - 1], mate)

    def seg_copy(step):
        return remote(seg_ref, seg_all_ref.at[me], seg_send.at[step - 1], seg_recv.at[step - 1], lax.rem(me + step, n))

    def own_copy():
        return remote(kv_s, kv_all_ref.at[me], mate_send.at[0], mate_recv.at[0], mate)

    for sub in range(SLICES):
        for way in range(2):
            ring_copy(way, sub, 1).start()
    own_copy().start()
    for step in range(1, n):
        seg_copy(step).start()

    pairs = wq_s.shape[0] // 2

    def project(src_ref, w_s, dst_ref, pair):
        w_pair = jnp.concatenate([w_s[2 * pair], w_s[2 * pair + 1]], axis=1)
        cols = pl.ds(pl.multiple_of(pair * 256, 256), 256)
        value = dot32(src_ref[...], w_pair, NN).astype(jnp.bfloat16)
        dst_ref[:, cols] = value
        return value

    def query_pair(pair, carry):
        project(x_ref, wq_s, q_ref, pair)
        return carry

    load_q.wait()
    lax.fori_loop(0, pairs, query_pair, 0)

    for step in range(1, n):
        seg_copy(step).wait_recv()
    seg_own = seg_ref[...]
    first_seg = jnp.min(seg_own)
    shard_index = lax.broadcasted_iota(jnp.int32, seg_all_ref.shape, 0)
    earlier = (shard_index < me) & (seg_all_ref[...] < first_seg)
    doc_start = jnp.sum(earlier.astype(jnp.int32))
    seg_wide = seg_own.astype(jnp.float32)
    columns = [jnp.broadcast_to(seg_wide[part:part + 1, :], (128, 128)).T for part in range(tok // 128)]
    for tile in range(tiles):
        count = sum(jnp.sum((column < seg_wide[tile:tile + 1, :]).astype(jnp.int32), axis=0, keepdims=True)
                    for column in columns)
        row = jnp.where(count == 0, doc_start - me * tok, count)
        start_ref[tile] = jnp.concatenate([row] * group, axis=1)

    for tile in range(tiles):
        forward_update(kv_heads, group, scale2, tile, q_ref, kv_all_ref, me, stats, start_ref[tile], QT * (tile + 1), True)
    load_o.wait()
    flat_outs[0].start()
    flat_outs[3].start()
    flat_outs[4].start()

    def tick_body(tick, carry):
        step, sub = tick // SLICES, lax.rem(tick, SLICES)
        for way in range(2):
            last = (sub < SLICES // 2) if way == 0 else (sub >= SLICES // 2)

            @pl.when((step < reach - 1) | last)
            def _():
                ring_copy(way, sub, step + 1).wait_recv()
                pair_copy(way, sub, step + 1).start()

            @pl.when((step < reach - 2) | ((step == reach - 2) & last))
            def _():
                ring_copy(way, sub, step + 2).start()

        @pl.when((step == 0) & (sub == 0))
        def _():
            own_copy().wait_recv()

        @pl.when((step > 0) & (sub == 0))
        def _():
            for piece in range(SLICES):
                pair_copy(0, piece, step).wait_recv()

        @pl.when(sub == 0)
        def _():
            for which in range(2):
                block_out(at(-step, which)).start()

        spread = reach * SLICES // pairs

        @pl.when(lax.rem(tick, spread) == 0)
        def _():
            pair = tick // spread
            value = project(dy_ref, wo_s, do_ref, pair)
            unit = (lax.broadcasted_iota(jnp.int32, (256, 256), 0)
                    == lax.broadcasted_iota(jnp.int32, (256, 256), 1)).astype(jnp.bfloat16)
            dot_ref[pl.ds(pl.multiple_of(pair * 256, 256), 256), :] = dot32(unit, value, NT).astype(jnp.bfloat16)

        def near_tile(item, inner):
            side = item // tiles
            tile = lax.rem(item, tiles)

            @pl.when((chip >= step) & ((step > 0) | ((core == 1) & (side == 0))))
            def _():
                blk = 2 * (chip - step) + side
                forward_update(kv_heads, group, scale2, tile, q_ref, kv_all_ref, blk, stats,
                               start_ref[tile] + (me - blk) * tok)
            return inner

        share = 2 * tiles // SLICES
        lax.fori_loop(sub * share, (sub + 1) * share, near_tile, 0)
        return carry

    lax.fori_loop(0, reach * SLICES, tick_body, 0)
    flat_outs[1].start()
    flat_outs[2].start()
    for way in range(2):
        for sub in range(SLICES):
            for hop in range(1, reach + 1):
                if hop < reach or (sub < SLICES // 2) == (way == 0):
                    if way == 1 or hop == reach:
                        pair_copy(way, sub, hop).wait_recv()
                    pair_copy(way, sub, hop).wait_send()
                    ring_copy(way, sub, hop).wait_send()
    for offset in range(1, chips - reach + 1):
        for which in range(2):
            block_out(at(offset, which)).start()
    own_copy().wait_send()
    for step in range(1, n):
        seg_copy(step).wait_send()
    for copy in flat_outs:
        copy.wait()
    for blk in range(n):
        block_out(blk).wait()


def reduce_kernel(n, scale, kv_width, dkv_ref, o_hbm, dq_hbm, x_hbm, dy_hbm, wk_hbm, wv_hbm, wq_ref, wo_ref,
                  y_ref, dx_ref, dwo_ref, dwq_ref, dwk_ref, dwv_ref,
                  o_ref, dq_ref, x_ref, dy_ref, wkv_ref, xt_ref, dyt_ref, xtp_ref, dytp_ref,
                  own_s, mate_s, slot1_s, stage1_s, grad_s, grad_mate_s, o_mate_s, dq_mate_s, slot2_s, stage2_s,
                  wq_s, wo_s, load_sem, block_sem, mate_send, mate_recv, ring_send, ring_recv, extra_send, extra_recv):
    me, chips, core, chip, at = places(n)
    mate = at(0, 1 - core)
    ring = (at(1, core), at(-1, core))
    tok = o_ref.shape[0]
    quarter = tok // 4
    heads, out_rows, head_dim = dwo_ref.shape
    loads = [pltpu.make_async_copy(src, dst, load_sem.at[index]) for index, (src, dst) in enumerate(
        ((o_hbm, o_ref), (dq_hbm, dq_ref), (x_hbm, x_ref), (dy_hbm, dy_ref), (wo_ref, wo_s), (wq_ref, wq_s),
         (wk_hbm, wkv_ref.at[:, 0:kv_width]), (wv_hbm, wkv_ref.at[:, kv_width:2 * kv_width])))]
    order = []
    for step in range(1, chips):
        for offset in (-step, step):
            if offset % chips not in order:
                order.append(offset % chips)
    order.append(0)
    own_loads = [pltpu.make_async_copy(dkv_ref.at[at(offset, core)], own_s.at[index], block_sem.at[index])
                 for index, offset in enumerate(order)]
    for load in own_loads:
        load.start()
    for load in loads:
        load.start()
    greet([ring[0], ring[1], mate])
    halves = [pl.ds(way * (tok // 2), tok // 2) for way in range(2)]
    mate_copies = [[remote(dkv_ref.at[at(offset, 1 - core), halves[way]], mate_s.at[index, halves[way]],
                           mate_send.at[index, way], mate_recv.at[index, way], mate) for way in range(2)]
                   for index, offset in enumerate(order)]
    extras = [remote(o_hbm, o_mate_s, extra_send.at[0], extra_recv.at[0], mate),
              remote(dq_hbm, dq_mate_s, extra_send.at[1], extra_recv.at[1], mate),
              remote(grad_s, grad_mate_s, extra_send.at[2], extra_recv.at[2], mate),
              remote(xt_ref, xtp_ref, extra_send.at[3], extra_recv.at[3], mate),
              remote(dyt_ref, dytp_ref, extra_send.at[4], extra_recv.at[4], mate)]
    mate_copies[0][0].start()
    mate_copies[1][1].start()
    mate_copies[0][1].start()
    mate_copies[1][0].start()
    for index in range(2, len(order)):
        for copy in mate_copies[index]:
            copy.start()
        if index == 3:
            extras[0].start()
            extras[1].start()

    ready = set()

    def need(position, way):
        if position not in ready:
            ready.add(position)
            own_loads[position].wait()
        mate_copies[position][way].wait_recv()

    def ring_copy(job, way, sub, step):
        slots, stage = (slot1_s, stage1_s) if job == 0 else (slot2_s, stage2_s)
        src = stage.at[way, sub] if step == 0 else slots.at[way, sub, step - 1]
        return remote(src, slots.at[way, sub, step], ring_send.at[job, way, sub, step], ring_recv.at[job, way, sub, step],
                      ring[way])

    started = []

    def send(job, way, sub, step):
        started.append(ring_copy(job, way, sub, step))
        started[-1].start()

    def contrib1(way, sub, step):
        offset = (-(1 + step) if way == 0 else 1 + step) % chips
        position = order.index(offset)
        if sub == 0:
            need(position, way)
        span = slice((2 * way + sub) * quarter, (2 * way + sub + 1) * quarter)
        return own_s[position, span, :] + mate_s[position, span, :]

    cut = 7 * head_dim

    def contrib2(way, sub, step):
        offset = -(1 + step) if way == 0 else 1 + step
        first_row = pl.multiple_of(at(offset % chips, core) * out_rows, 32)
        take = pl.ds(first_row, out_rows)
        lhs, lhs_mate = (dyt_ref, dytp_ref) if way == 0 else (xt_ref, xtp_ref)
        rhs, rhs_mate = (o_ref, o_mate_s) if way == 0 else (dq_ref, dq_mate_s)
        if sub == 0:
            return (dot32(lhs[take, :], rhs[:, 0:cut], NN) + dot32(lhs_mate[take, :], rhs_mate[:, 0:cut], NN))
        main = dot32(lhs[take, :], rhs[:, cut:], NN) + dot32(lhs_mate[take, :], rhs_mate[:, cut:], NN)
        cols = slice(way * kv_width, (way + 1) * kv_width)
        side = dot32(xt_ref[take, :], grad_s[:, cols], NN) + dot32(xtp_ref[take, :], grad_mate_s[:, cols], NN)
        return jnp.concatenate([main, side], axis=1)

    strip = 256
    strips = y_ref.shape[1] // strip

    def rows_out(part):
        return pl.ds(pl.multiple_of(part * strip, strip), strip)

    def times_weight(src_ref, w_s, part):
        total = None
        for pair in range(heads // 2):
            w_pair = jnp.concatenate([w_s[2 * pair, rows_out(part), :], w_s[2 * pair + 1, rows_out(part), :]], axis=1)
            piece = dot32(src_ref[:, pair * 256:(pair + 1) * 256], w_pair, NT)
            total = piece if total is None else total + piece
        return total

    def y_strip(part, carry):
        y_ref[:, rows_out(part)] = times_weight(o_ref, wo_s, part).astype(jnp.bfloat16)
        return carry

    def flip_strip(part, carry):
        xt_ref[rows_out(part), :] = x_ref[:, rows_out(part)].T
        dyt_ref[rows_out(part), :] = dy_ref[:, rows_out(part)].T
        return carry

    def dx_strip(part, carry):
        wide = times_weight(dq_ref, wq_s, part) + dot32(grad_s[...], wkv_ref[rows_out(part), :], NT)
        dx_ref[:, rows_out(part)] = wide.astype(jnp.bfloat16)
        return carry

    steps = chips - 1
    both = [(sub, way) for sub in range(2) for way in range(2)]
    for sub, way in both:
        stage1_s[way, sub] = contrib1(way, sub, 0)
        send(0, way, sub, 0)
    for load in loads:
        load.wait()
    for step in range(steps):
        if step == 0:
            lax.fori_loop(0, strips, y_strip, 0)
        if step == 1:
            lax.fori_loop(0, strips, flip_strip, 0)
        if step == 4:
            extras[3].start()
            extras[4].start()
        if step == steps - 1:
            for index in (0, 1, 3, 4):
                extras[index].wait_recv()
            for way in range(2):
                stage2_s[way, 0] = contrib2(way, 0, 0)
                send(1, way, 0, 0)
        for sub, way in both:
            part = contrib1(way, sub, step + 1)
            ring_copy(0, way, sub, step).wait_recv()
            if step < steps - 1:
                slot1_s[way, sub, step] = slot1_s[way, sub, step] + part
                send(0, way, sub, step + 1)
            else:
                span = slice((2 * way + sub) * quarter, (2 * way + sub + 1) * quarter)
                total = slot1_s[way, sub, step] + part
                grad_s[span, 0:kv_width] = (total[:, 0:kv_width] * scale).astype(jnp.bfloat16)
                grad_s[span, kv_width:] = total[:, kv_width:].astype(jnp.bfloat16)
    extras[2].start()
    extras[2].wait_recv()
    for way in range(2):
        stage2_s[way, 1] = contrib2(way, 1, 0)
        send(1, way, 1, 0)
    for step in range(steps):
        if step == 0:
            lax.fori_loop(0, strips, dx_strip, 0)
        for sub, way in both:
            part = contrib2(way, sub, step + 1)
            ring_copy(1, way, sub, step).wait_recv()
            if step < steps - 1:
                slot2_s[way, sub, step] = slot2_s[way, sub, step] + part
                send(1, way, sub, step + 1)
            else:
                total = slot2_s[way, sub, step] + part
                out_ref = dwo_ref if way == 0 else dwq_ref
                base = 0 if sub == 0 else cut // head_dim
                for index in range(cut // head_dim if sub == 0 else heads - cut // head_dim):
                    out_ref[base + index] = total[:, index * head_dim:(index + 1) * head_dim]
                if sub == 1:
                    side_ref = dwk_ref if way == 0 else dwv_ref
                    for index in range(kv_width // head_dim):
                        base = heads * head_dim - cut + index * head_dim
                        side_ref[:, index, :] = total[:, base:base + head_dim]
    for copy in started + mate_copies[0] + sum(mate_copies[1:], []) + extras:
        copy.wait_send()


VMEM_SPEC = pl.BlockSpec(memory_space=pltpu.VMEM)
ANY_SPEC = pl.BlockSpec(memory_space=pl.ANY)
VMEM_LIMIT = 60 * 1024 * 1024
REDUCE_LIMIT = 67043328


def solution(mesh):
    group_count = mesh.shape['cp']
    row_spec = P(('dp', 'cp'), None)
    tok_spec = P(('dp', 'cp'))
    weight_spec = P(None, None, None)
    grad_spec = P(('dp', 'cp'), None, None)

    def local_step(x_act, seg_ids, w_q, w_k, w_v, w_o, dy_act):
        tok = x_act.shape[0]
        model_dim, q_heads, head_dim = w_q.shape
        kv_heads = w_k.shape[1]
        group = q_heads // kv_heads
        q_width = q_heads * head_dim
        kv_width = kv_heads * head_dim
        tiles = tok // QT
        scale = head_dim ** -0.5
        bf16 = jnp.bfloat16

        wk_flat, wv_flat = w_k.reshape(model_dim, kv_width), w_v.reshape(model_dim, kv_width)
        seg_rows = seg_ids.reshape(tok // 128, 128)
        wq_heads = w_q.transpose(1, 0, 2)
        wo_heads = w_o.transpose(1, 0, 2)

        slots = kv_heads * tiles
        width = group * QT
        chips = group_count // 2
        reach = chips // 2
        dma = pltpu.SemaphoreType.DMA
        f32 = jnp.float32
        shape = jax.ShapeDtypeStruct
        flat = shape((tok, q_width), bf16)
        row32 = shape((tiles, 1, width), f32)
        wide32 = shape((tiles, head_dim, width), f32)
        kv_all, wk_kept, wv_kept, seg_all, q_loc, do_loc, do_turned, *kept = pl.pallas_call(
            functools.partial(gather_kernel, group_count, kv_heads, group, scale * LOG2E),
            out_shape=(shape((group_count, tok, 2 * kv_width), bf16), shape((model_dim, kv_width), bf16), shape((model_dim, kv_width), bf16),
                       shape((group_count, tok // 128, 128), jnp.int32),
                       flat, flat, shape((q_width, tok), bf16), shape((tiles, 1, width), jnp.int32),
                       row32, row32, row32, row32, wide32, wide32),
            in_specs=[VMEM_SPEC] * 5 + [ANY_SPEC] * 2,
            out_specs=(ANY_SPEC, ANY_SPEC, ANY_SPEC, VMEM_SPEC) + (ANY_SPEC,) * 3 + (VMEM_SPEC,) * 7,
            scratch_shapes=[pltpu.VMEM((group_count, tok, 2 * kv_width), bf16), pltpu.VMEM((tok, q_width), bf16),
                            pltpu.VMEM((tok, q_width), bf16), pltpu.VMEM((q_width, tok), bf16),
                            dma((5,)), dma((group_count,)), pltpu.VMEM((tok, 2 * kv_width), bf16), pltpu.VMEM((q_heads, model_dim, head_dim), bf16),
                            pltpu.VMEM((q_heads, model_dim, head_dim), bf16),
                            dma((2,)), dma((group_count - 1,)), dma((group_count - 1,)),
                            dma((2, SLICES, reach)), dma((2, SLICES, reach)), dma((2, SLICES, reach)), dma((2, SLICES, reach)), dma((1,)), dma((1,))],
            compiler_params=pltpu.CompilerParams(collective_id=0, has_side_effects=True, vmem_limit_bytes=VMEM_LIMIT),
            cost_estimate=pl.CostEstimate(flops=8 * tok * model_dim * q_width, bytes_accessed=2**24, transcendentals=0),
            name='gather_keys',
        )(seg_rows, x_act, dy_act, wk_flat, wv_flat, wq_heads, wo_heads)

        o_loc, dq_loc, dkv_all = pl.pallas_call(
            functools.partial(attention_kernel, kv_heads, group, scale),
            out_shape=(flat, flat, shape((group_count, tok, 2 * kv_width), f32)),
            in_specs=[VMEM_SPEC] * 5 + [ANY_SPEC] + [VMEM_SPEC] * 7,
            out_specs=(VMEM_SPEC, VMEM_SPEC, ANY_SPEC),
            scratch_shapes=[pltpu.VMEM((tiles, 1, width), f32)] * 4
                           + [pltpu.VMEM((slots, 1, width), f32)] + [pltpu.VMEM((tiles, head_dim, width), f32)] * 2
                           + [pltpu.VMEM((group_count, tok, 2 * kv_width), f32),
                            pltpu.VMEM((tok, 2 * kv_width), f32), dma((group_count,)),
                            pltpu.VMEM((group_count, tok, 2 * kv_width), bf16), dma((group_count,))],
            compiler_params=pltpu.CompilerParams(vmem_limit_bytes=VMEM_LIMIT),
            cost_estimate=pl.CostEstimate(flops=16 * 14 * tok * tok * q_width, bytes_accessed=2**25, transcendentals=0),
            name='attend',
        )(seg_rows, seg_all, q_loc, do_loc, do_turned, kv_all, *kept)

        out_rows = model_dim // group_count
        blk = (tok, 2 * kv_width)
        cols2 = (q_width + kv_width) // 2
        steps = chips - 1
        head_grad = shape((q_heads, out_rows, head_dim), f32)
        y_out, dx_out, dwo, dwq, dwk, dwv = pl.pallas_call(
            functools.partial(reduce_kernel, group_count, scale, kv_width),
            out_shape=(shape((tok, model_dim), bf16), shape((tok, model_dim), bf16), head_grad, head_grad,
                       shape((out_rows, kv_heads, head_dim), f32), shape((out_rows, kv_heads, head_dim), f32)),
            in_specs=[ANY_SPEC] * 9,
            out_specs=(VMEM_SPEC,) * 6,
            scratch_shapes=[pltpu.VMEM((tok, q_width), bf16), pltpu.VMEM((tok, q_width), bf16),
                            pltpu.VMEM((tok, model_dim), bf16), pltpu.VMEM((tok, model_dim), bf16),
                            pltpu.VMEM((model_dim, 2 * kv_width), bf16),
                            pltpu.VMEM((model_dim, tok), bf16), pltpu.VMEM((model_dim, tok), bf16),
                            pltpu.VMEM((model_dim, tok), bf16), pltpu.VMEM((model_dim, tok), bf16),
                            pltpu.VMEM((chips,) + blk, f32), pltpu.VMEM((chips,) + blk, f32),
                            pltpu.VMEM((2, 2, steps, tok // 4, 2 * kv_width), f32), pltpu.VMEM((2, 2, tok // 4, 2 * kv_width), f32),
                            pltpu.VMEM(blk, bf16), pltpu.VMEM(blk, bf16),
                            pltpu.VMEM((tok, q_width), bf16), pltpu.VMEM((tok, q_width), bf16),
                            pltpu.VMEM((2, 2, steps, out_rows, cols2), f32), pltpu.VMEM((2, 2, out_rows, cols2), f32),
                            pltpu.VMEM((q_heads, model_dim, head_dim), bf16), pltpu.VMEM((q_heads, model_dim, head_dim), bf16),
                            dma((8,)), dma((chips,)), dma((chips, 2)), dma((chips, 2)),
                            dma((2, 2, 2, steps)), dma((2, 2, 2, steps)), dma((5,)), dma((5,))],
            compiler_params=pltpu.CompilerParams(collective_id=1, has_side_effects=True, vmem_limit_bytes=REDUCE_LIMIT),
            cost_estimate=pl.CostEstimate(flops=16 * tok * model_dim * q_width, bytes_accessed=2**25, transcendentals=0),
            name='reduce_grads',
        )(dkv_all, o_loc, dq_loc, x_act, dy_act, wk_kept, wv_kept, wq_heads, wo_heads)
        return y_out, dx_out, dwq.transpose(1, 0, 2), dwk, dwv, dwo.transpose(1, 0, 2)

    return jax.shard_map(local_step, mesh=mesh,
                         in_specs=(row_spec, tok_spec, weight_spec, weight_spec, weight_spec, weight_spec, row_spec),
                         out_specs=(row_spec, row_spec, grad_spec, grad_spec, grad_spec, grad_spec),
                         check_vma=False)
```
